128 devices in a mesh: zg: 2 (over x_lo), xy: 64 (over x_hi, y, z, core).
Axes of the slice: x: 4 (x_hi: 2, x_lo: 2; x = x_hi * 2 + x_lo), y: 4, z: 4, core: 2. Of those that a mesh axis runs over, the one named last changes fastest.
Arguments:
- charges: float32 [262144], P(('zg', 'xy')), may hold values from -12 to 12
- cells: int32 [8, 262144], P(None, ('zg', 'xy')), may hold values from 0 to 786431
- splines: float32 [8, 262144], P(None, ('zg', 'xy')), may hold values from 0.05 to 1
- counts: int32 [128], P(('zg', 'xy')), may hold values from 1024 to 2048, as said below
- green: bfloat16 [512, 4, 384, 384], P(('zg', 'xy')), may hold values from -0.3125 to 0.3125
Outputs:
- potential: float32 [384, 512, 512], P(('zg', 'xy'))
The draws below stay inside these ranges and needn't reach their ends.
Inputs may be any that keep to these rules, and one draw needn't show every extreme that they name: `counts`: some device has all 2048 slots live in every draw.
All inputs are finite; a program needn't handle non-finite values.
Results may differ from the reference program's by a relative error of at most 0.0041.
Values may be sent and summed in bfloat16 or wider, within the bound.
No kernel may reach another device: no remote copies, remote signals or barrier semaphores. Data moves between devices by JAX's collectives and lax.ppermute only.
A program may use at most 64 MiB of HBM per device.

```python
import jax
import jax.numpy as jnp
from jax import lax

NX = 512
NY = 512
NZ = 384
KYB = 4
SPREAD = 8
PART_DEV = 2048
ZDEV = 3
PARTICLES = 262144
N_ZG = 2
N_XY = 64
DEVICES = 128


def draw_counts(key, part):
    first = jax.random.fold_in(key, 11)
    second = jax.random.fold_in(key, 23)
    values = jax.random.randint(first, (DEVICES,), PART_DEV // 2, PART_DEV + 1, dtype=jnp.int32)
    chosen = jax.random.randint(second, (), 0, DEVICES, dtype=jnp.int32)
    places = jnp.arange(DEVICES, dtype=jnp.int32)
    return jnp.where(places == chosen, PART_DEV, values).astype(jnp.int32)


def plant(entries, stream_key, low, top_value):
    index_at = [jax.random.randint(jax.random.fold_in(stream_key, axis), (), 0, length) for axis, length in enumerate(entries.shape)]
    longest = entries.shape.index(max(entries.shape))
    next_to = index_at[:longest] + [(index_at[longest] + 1) % entries.shape[longest]] + index_at[longest + 1:]
    return entries.at[tuple(index_at)].set(low).at[tuple(next_to)].set(top_value)


def steps_of(stream_key, shape, split, smallest, high):
    def one(axis_at, blocks):
        heights = jax.random.uniform(jax.random.fold_in(jax.random.fold_in(stream_key, 6), axis_at), (blocks,), jnp.float32, smallest / len(split), high / len(split))
        return jnp.repeat(jnp.exp(heights), shape[axis_at] // blocks).reshape((-1,) + (1,) * (len(shape) - axis_at - 1))

    level = one(*split[0])
    for cut in split[1:]:
        level = level * one(*cut)
    return level


def normal_values(key, dims, spread, reach, pieces=(), kind=jnp.bfloat16):
    result = spread * jax.random.normal(key, dims, jnp.float32)
    if pieces:
        result = result * steps_of(key, dims, pieces, -0.22, 0.18)
    return jnp.clip(result, -reach, reach).astype(kind)


def setup_inputs(seed: int = 0) -> dict:
    key_list = jax.random.split(jax.random.key(seed), 6)
    charges = normal_values(key_list[0], (PARTICLES,), 2.0, 12.0, ((0, 128),), jnp.float32)
    cells = plant(jax.random.randint(key_list[1], (SPREAD, PARTICLES), 0, ZDEV * NX * NY), jax.random.fold_in(key_list[1], 1), 0, (ZDEV * NX * NY) - 1).astype(jnp.int32)
    splines = jnp.clip(0.05 + 0.95 * jax.random.uniform(key_list[2], (SPREAD, PARTICLES), jnp.float32) ** steps_of(key_list[2], (SPREAD, PARTICLES), ((1, 128),), -0.2, 0.2), 0.05, 1.0)
    counts = draw_counts(jax.random.fold_in(key_list[5], 71), 0)
    green = normal_values(key_list[4], (NX, KYB, NZ, NZ), NZ ** -0.5, 0.3125, ((0, 128),))
    return {"charges": charges, "cells": cells, "splines": splines, "counts": counts, "green": green}


def reference(charges, cells, splines, counts, green):
    devices = N_ZG * N_XY
    slab = NZ // devices
    slots = jnp.arange(devices * PART_DEV, dtype=jnp.int32)
    owner = slots // PART_DEV
    rank = slots - owner * PART_DEV
    live = (rank < counts[owner]).astype(jnp.float32)
    values = splines * (charges * live)[None, :]
    offsets = cells + (owner * (slab * NX * NY))[None, :]
    density = jnp.zeros((NZ * NX * NY,), jnp.float32).at[offsets.reshape(-1)].add(values.reshape(-1))
    density = density.reshape(NZ, NX, NY)
    norm = jnp.sqrt(jnp.float32(NX * NY))
    transformed = jnp.fft.fft2(density, axes=(1, 2)) / norm
    spectrum = jnp.stack([jnp.real(transformed), jnp.imag(transformed)], axis=1).astype(jnp.bfloat16)

    def one_column(pair):
        matrices, plane = pair
        blocks = plane.astype(jnp.float32).reshape(NZ, 2, KYB, NY // KYB)
        mixed = jnp.einsum('bzw,wcbj->zcbj', matrices.astype(jnp.float32), blocks)
        return mixed.reshape(NZ, 2, NY).astype(jnp.bfloat16)
    columns = lax.map(one_column, (green, jnp.moveaxis(spectrum, 2, 0)))
    mixed = jnp.moveaxis(columns, 0, 2).astype(jnp.float32)
    complex_hat = lax.complex(mixed[:, 0], mixed[:, 1])
    potential = jnp.real(jnp.fft.ifft2(complex_hat, axes=(1, 2))) * norm
    return potential.astype(jnp.float32)
```

```python
import jax
import jax.numpy as jnp
import numpy as np
from jax import lax
from jax.experimental import pallas as pl
from jax.experimental.pallas import tpu as pltpu
from jax.sharding import PartitionSpec as P

NX = 512
NY = 512
NZ = 384
KYB = 4
AXES = ("zg", "xy")
DEV = 128
ZD = 3
NU = NX // DEV
HALF = NY // 2
LANE = 128
SLOTS = 2048
SPREAD = 8
TILES = SLOTS // LANE
ROWS = ZD * NX * NY // LANE
F32 = jnp.float32
BF16 = jnp.bfloat16


def split(table):
    high = table.astype(BF16)
    return high, (table - high.astype(np.float64)).astype(BF16)


def angles(left, right):
    return (np.outer(left, right) % NX) * (2.0 * np.pi / NX)


def tables():
    y = np.arange(NY)
    v = np.arange(HALF)
    scale = 1.0 / 512.0
    alternating = np.where(y % 2 == 0, 1.0, -1.0)
    forward_y = np.concatenate([np.cos(angles(y, v)), -np.sin(angles(y, v))], axis=1)
    forward_y[:, HALF] = alternating
    inverse_y = np.concatenate([np.cos(angles(v, y)), np.sin(angles(v, y))], axis=0)
    inverse_y[HALF] = -alternating
    x = np.arange(NX)
    a = angles(np.arange(NX), x).reshape(DEV, NU, NX)
    cos, sin = np.cos(a), np.sin(a)
    plain = np.stack([cos, -sin], axis=1).reshape(2 * NX, NX)
    turned = np.stack([sin, cos], axis=1).reshape(2 * NX, NX)
    return (
        *split(forward_y * scale),
        *split(plain),
        *split(turned),
        plain.T.astype(BF16),
        (inverse_y * scale).astype(BF16),
    )


def dot(a, b):
    return jnp.dot(a, b, preferred_element_type=F32)


def front_kernel(
    rows_hbm, cells, splines, charges, counts, yh_hbm, yl_hbm, ph_hbm, pl_hbm, th_hbm, tl_hbm, out, *scratch
):
    bins = scratch[:SPREAD]
    spikes = scratch[8:10]
    lanes, values, dens_hi, dens_lo, along_hi, along_lo = scratch[10:16]
    tabs = scratch[16:22]
    row_sem, tab_sem = scratch[22:24]
    row_of = scratch[24:]
    row_copies = [
        pltpu.make_async_copy(rows_hbm.at[pl.ds(t * 1024, 1024)], row_of[t], row_sem.at[t]) for t in range(TILES)
    ]
    for copy in row_copies:
        copy.start()
    sources = (yh_hbm, yl_hbm, ph_hbm, pl_hbm, th_hbm, tl_hbm)
    tab_copies = [pltpu.make_async_copy(s, d, tab_sem.at[i]) for i, (s, d) in enumerate(zip(sources, tabs))]
    for copy in tab_copies:
        copy.start()
    slot = lax.broadcasted_iota(jnp.int32, (1, SLOTS), 1)
    live = (slot < counts[0]).astype(F32)
    value = splines[...] * (charges[...] * live)
    lane_of = cells[...] & (LANE - 1)
    for t in range(TILES):
        lanes[t] = lane_of[:, t * LANE : (t + 1) * LANE]
        values[t] = value[:, t * LANE : (t + 1) * LANE]
    zeros = jnp.zeros((256, LANE), F32)

    def clear(i, carry):
        for b in bins:
            b[pl.ds(i * 256, 256), :] = zeros
        return carry

    lax.fori_loop(0, ROWS // 256, clear, 0)
    lane = lax.broadcasted_iota(jnp.int32, (SPREAD, LANE), 1)

    def build(spike, g):
        pick = jnp.full((SPREAD, LANE), g, jnp.int32)
        for t in range(TILES):
            at = jnp.take_along_axis(lanes[t], pick, axis=1)
            amount = jnp.take_along_axis(values[t], pick, axis=1)
            spike[t * SPREAD : (t + 1) * SPREAD, :] = jnp.where(lane == at, amount, 0.0)

    def apply(spike, g):
        for t in range(TILES):
            rows = [row_of[t][g + k * LANE] for k in range(SPREAD)]
            sums = [bins[k][pl.ds(rows[k], 1), :] + spike[pl.ds(t * SPREAD + k, 1), :] for k in range(SPREAD)]
            for k in range(SPREAD):
                bins[k][pl.ds(rows[k], 1), :] = sums[k]

    build(spikes[0], 0)
    for copy in row_copies:
        copy.wait()

    def body(h, carry):
        build(spikes[1], 2 * h + 1)
        apply(spikes[0], 2 * h)
        build(spikes[0], jnp.minimum(2 * h + 2, LANE - 1))
        apply(spikes[1], 2 * h + 1)
        return carry

    lax.fori_loop(0, LANE // 2, body, 0)
    for copy in tab_copies:
        copy.wait()
    yh, yl, ph, plo, th, tl = tabs
    first = lax.broadcasted_iota(jnp.int32, (2 * NX, LANE), 1) == 0

    def plane(z, carry):
        for j in range(NY // LANE):
            for q in range(4):
                at = pl.ds(z * (NX * 4) + q * 512 + j, 128, stride=4)
                total = bins[0][at, :]
                for b in bins[1:]:
                    total = total + b[at, :]
                high = total.astype(BF16)
                dens_hi[q * 128 : (q + 1) * 128, j * LANE : (j + 1) * LANE] = high
                dens_lo[q * 128 : (q + 1) * 128, j * LANE : (j + 1) * LANE] = (total - high.astype(F32)).astype(BF16)
        along = dot(dens_hi[...], yh[...]) + dot(dens_lo[...], yh[...]) + dot(dens_hi[...], yl[...])
        high = along.astype(BF16)
        along_hi[...] = high
        along_lo[...] = (along - high.astype(F32)).astype(BF16)
        re_hi, re_lo = along_hi[:, :HALF], along_lo[:, :HALF]
        im_hi, im_lo = along_hi[:, HALF:], along_lo[:, HALF:]
        p = dot(ph[...], re_hi) + dot(ph[...], re_lo) + dot(plo[...], re_hi)
        q = dot(th[...], im_hi) + dot(th[...], im_lo) + dot(tl[...], im_hi)
        p0, p1, q0, q1 = p[:, :LANE], p[:, LANE:], q[:, :LANE], q[:, LANE:]
        minus0 = jnp.where(first, 0.0, p0) - q0
        minus1 = p1 - q1
        parts = (
            p0 + jnp.where(first, 0.0, q0),
            p1 + q1,
            jnp.where(first, minus1, minus0),
            jnp.where(first, minus0, minus1),
        )
        for j, part in enumerate(parts):
            out[:, z, :, j * LANE : (j + 1) * LANE] = part.astype(BF16).reshape(DEV, 2 * NU, LANE)
        return carry

    lax.fori_loop(0, ZD, plane, 0)


def front(charges, cells, splines, counts, tabs):
    vmem = pl.BlockSpec(memory_space=pltpu.VMEM)
    smem = pl.BlockSpec(memory_space=pltpu.SMEM)
    hbm = pl.BlockSpec(memory_space=pl.ANY)
    rows = lax.shift_right_logical(cells, 7).reshape(SPREAD, TILES, LANE).transpose(1, 0, 2).reshape(-1)
    return pl.pallas_call(
        front_kernel,
        out_shape=jax.ShapeDtypeStruct((DEV, ZD, 2 * NU, NY), BF16),
        in_specs=[hbm, vmem, vmem, vmem, smem] + [hbm] * 6,
        out_specs=vmem,
        scratch_shapes=[pltpu.VMEM((ROWS, LANE), F32)] * SPREAD
        + [pltpu.VMEM((LANE, LANE), F32)] * 2
        + [pltpu.VMEM((TILES, SPREAD, LANE), jnp.int32), pltpu.VMEM((TILES, SPREAD, LANE), F32)]
        + [pltpu.VMEM((NX, NY), BF16)] * 4
        + [pltpu.VMEM(t.shape, BF16) for t in tabs]
        + [pltpu.SemaphoreType.DMA((TILES,)), pltpu.SemaphoreType.DMA((6,))]
        + [pltpu.SMEM((SPREAD * LANE,), jnp.int32)] * TILES,
        name="front",
    )(rows, cells, splines, charges.reshape(1, SLOTS), counts, *tabs)


BLOCK = (0, 1, 3, 2)


def green_kernel(spectrum, green, out, flat, sums, *rhs):
    for j in range(KYB):
        flat[...] = spectrum[:, :, j * LANE : (j + 1) * LANE].astype(F32).reshape(NZ * 2 * NU, LANE)
        for ul in range(NU):
            for c in range(2):
                rows = flat[pl.ds(c * NU + ul, NZ, stride=2 * NU), :]
                rhs[ul][j, :, c * LANE : (c + 1) * LANE] = rows.astype(BF16)
    first = lax.broadcasted_iota(jnp.int32, (NZ, 2 * LANE), 1) % LANE == 0
    for ul in range(NU):
        m0, m1, m2, m3 = (dot(green[ul, BLOCK[j]], rhs[ul][j]) for j in range(KYB))
        s2 = jnp.where(first, m3, m2)
        s3 = jnp.where(first, m2, m3)
        t0 = m0 + jnp.where(first, 0.0, s2)
        d0 = jnp.where(first, 0.0, m0) - s2
        t1 = m1 + s3
        d1 = m1 - s3
        re = pl.ds(ul, NZ, stride=2 * NU)
        im = pl.ds(NU + ul, NZ, stride=2 * NU)
        sums[0, re, :] = t0[:, :LANE]
        sums[0, im, :] = t0[:, LANE:]
        sums[1, re, :] = t1[:, :LANE]
        sums[1, im, :] = t1[:, LANE:]
        sums[2, re, :] = -d0[:, LANE:]
        sums[2, im, :] = d0[:, :LANE]
        sums[3, re, :] = -d1[:, LANE:]
        sums[3, im, :] = d1[:, :LANE]
    for j in range(KYB):
        out[:, :, j * LANE : (j + 1) * LANE] = sums[j].astype(BF16).reshape(NZ, 2 * NU, LANE)


def mix(pencil, green):
    vmem = pl.BlockSpec(memory_space=pltpu.VMEM)
    return pl.pallas_call(
        green_kernel,
        out_shape=jax.ShapeDtypeStruct((NZ, 2 * NU, NY), BF16),
        in_specs=[vmem, vmem],
        out_specs=vmem,
        scratch_shapes=[pltpu.VMEM((NZ * 2 * NU, LANE), F32), pltpu.VMEM((KYB, NZ * 2 * NU, LANE), F32)]
        + [pltpu.VMEM((KYB, NZ, 2 * LANE), BF16)] * NU,
        name="mix",
    )(pencil.reshape(NZ, 2 * NU, NY), green)


def back_kernel(mixed, inverse_x, inverse_y, out):
    middle = dot(inverse_x[...], mixed[:, 0].reshape(2 * NX, NY))
    out[0] = dot(middle.astype(BF16), inverse_y[...])


def back(returned, inverse_x, inverse_y):
    return pl.pallas_call(
        back_kernel,
        grid=(ZD,),
        out_shape=jax.ShapeDtypeStruct((ZD, NX, NY), F32),
        in_specs=[
            pl.BlockSpec((DEV, 1, 2 * NU, NY), lambda z: (0, z, 0, 0)),
            pl.BlockSpec((NX, 2 * NX), lambda z: (0, 0)),
            pl.BlockSpec((NY, NY), lambda z: (0, 0)),
        ],
        out_specs=pl.BlockSpec((1, NX, NY), lambda z: (z, 0, 0)),
        name="back",
    )(returned, inverse_x, inverse_y)


def shards(charges, cells, splines, counts, green):
    *forward, inverse_x, inverse_y = (jnp.asarray(t) for t in tables())
    spectrum = front(charges, cells, splines, counts, forward)
    pencil = lax.all_to_all(spectrum, AXES, split_axis=0, concat_axis=0, tiled=True)
    mixed = mix(pencil, green).reshape(DEV, ZD, 2 * NU, NY)
    returned = lax.all_to_all(mixed, AXES, split_axis=0, concat_axis=0, tiled=True)
    return back(returned, inverse_x, inverse_y)


def solution(mesh):
    in_specs = (
        P(AXES),
        P(None, AXES),
        P(None, AXES),
        P(AXES),
        P(AXES, None, None, None),
    )
    return jax.shard_map(
        shards, mesh=mesh, in_specs=in_specs, out_specs=P(AXES, None, None), check_vma=False
    )
```

```python
import functools

import jax
import jax.numpy as jnp
import numpy as np
from jax import lax
from jax.experimental import pallas as pl
from jax.experimental.pallas import tpu as pltpu
from jax.sharding import PartitionSpec as P

NX = 512
NY = 512
NZ = 384
KYB = 4
AXES = ("zg", "xy")
DEV = 128
ZD = 3
NU = NX // DEV
HALF = NY // 2
LANE = 128
SLOTS = 2048
SPREAD = 8
TILES = SLOTS // LANE
ROWS = ZD * NX * NY // LANE
F32 = jnp.float32
BF16 = jnp.bfloat16


def split(table):
    high = table.astype(BF16)
    return high, (table - high.astype(np.float64)).astype(BF16)


def angles(left, right):
    return (np.outer(left, right) % NX) * (2.0 * np.pi / NX)


def tables():
    y = np.arange(NY)
    v = np.arange(HALF)
    scale = 1.0 / 512.0
    alternating = np.where(y % 2 == 0, 1.0, -1.0)
    forward_y = np.concatenate([np.cos(angles(y, v)), -np.sin(angles(y, v))], axis=1)
    forward_y[:, HALF] = alternating
    inverse_y = np.concatenate([np.cos(angles(v, y)), np.sin(angles(v, y))], axis=0)
    inverse_y[HALF] = -alternating
    x = np.arange(NX)
    a = angles(np.arange(NX), x).reshape(DEV, NU, NX)
    cos, sin = np.cos(a), np.sin(a)
    plain = np.stack([cos, -sin], axis=1).reshape(2 * NX, NX)
    return (
        *split(forward_y * scale),
        *split(plain),
        plain.T.astype(BF16),
        *((scale * inverse_y.reshape(2, 2, LANE, NY)[:, j].reshape(2 * LANE, NY)).astype(BF16) for j in range(2)),
    )


def dot(a, b):
    return jnp.dot(a, b, preferred_element_type=F32)


def turn(q):
    whole = q.reshape(DEV, 2 * NU, LANE)
    real = lax.broadcasted_iota(jnp.int32, whole.shape, 1) < NU
    swapped = pltpu.roll(whole, NU, 1)
    return jnp.where(real, -swapped, swapped).reshape(2 * NX, LANE)


def along_x(high, low, re, im):
    tab_hi, tab_lo = high[0], low[0]
    data_hi, data_lo = high[1], low[1]
    p, q = (
        dot(tab_hi[...], data_hi[:, c]) + dot(tab_hi[...], data_lo[:, c]) + dot(tab_lo[...], data_hi[:, c])
        for c in (re, im)
    )
    return p, turn(q)


def store(out, z, plus, minus):
    out[:, z, :, :LANE] = plus.astype(BF16).reshape(DEV, 2 * NU, LANE)
    out[:, z, :, LANE:] = minus.astype(BF16).reshape(DEV, 2 * NU, LANE)


def front_kernel(
    rows_hbm, cells, splines, charges, counts, yh_hbm, yl_hbm, ph_hbm, pl_hbm, out, rest_hi, rest_lo, *scratch
):
    bins = scratch[:SPREAD]
    spikes = scratch[8:10]
    lanes, values, dens_hi, dens_lo, along_hi, along_lo = scratch[10:16]
    tabs = scratch[16:20]
    row_sem, tab_sem = scratch[20:22]
    row_of = scratch[22:]
    row_copies = [
        pltpu.make_async_copy(rows_hbm.at[pl.ds(t * 1024, 1024)], row_of[t], row_sem.at[t]) for t in range(TILES)
    ]
    for copy in row_copies:
        copy.start()
    sources = (yh_hbm, yl_hbm, ph_hbm, pl_hbm)
    tab_copies = [pltpu.make_async_copy(s, d, tab_sem.at[i]) for i, (s, d) in enumerate(zip(sources, tabs))]
    for copy in tab_copies:
        copy.start()
    slot = lax.broadcasted_iota(jnp.int32, (1, SLOTS), 1)
    live = (slot < counts[0]).astype(F32)
    value = splines[...] * (charges[...] * live)
    lane_of = cells[...] & (LANE - 1)
    for t in range(TILES):
        lanes[t] = lane_of[:, t * LANE : (t + 1) * LANE]
        values[t] = value[:, t * LANE : (t + 1) * LANE]
    zeros = jnp.zeros((256, LANE), F32)

    def clear(i, carry):
        for b in bins:
            b[pl.ds(i * 256, 256), :] = zeros
        return carry

    lax.fori_loop(0, ROWS // 256, clear, 0)
    lane = lax.broadcasted_iota(jnp.int32, (SPREAD, LANE), 1)

    def build(spike, g):
        pick = jnp.full((SPREAD, LANE), g, jnp.int32)
        for t in range(TILES):
            at = jnp.take_along_axis(lanes[t], pick, axis=1)
            amount = jnp.take_along_axis(values[t], pick, axis=1)
            spike[t * SPREAD : (t + 1) * SPREAD, :] = jnp.where(lane == at, amount, 0.0)

    def apply(spike, g):
        for t in range(TILES):
            rows = [row_of[t][g + k * LANE] for k in range(SPREAD)]
            sums = [bins[k][pl.ds(rows[k], 1), :] + spike[pl.ds(t * SPREAD + k, 1), :] for k in range(SPREAD)]
            for k in range(SPREAD):
                bins[k][pl.ds(rows[k], 1), :] = sums[k]

    build(spikes[0], 0)
    for copy in row_copies:
        copy.wait()

    def body(h, carry):
        build(spikes[1], 2 * h + 1)
        apply(spikes[0], 2 * h)
        build(spikes[0], jnp.minimum(2 * h + 2, LANE - 1))
        apply(spikes[1], 2 * h + 1)
        return carry

    lax.fori_loop(0, LANE // 2, body, 0)
    for copy in tab_copies:
        copy.wait()
    yh, yl, ph, plo = tabs
    first = lax.broadcasted_iota(jnp.int32, (2 * NX, LANE), 1) == 0

    def plane(z, carry):
        for j in range(NY // LANE):
            for q in range(4):
                at = pl.ds(z * (NX * 4) + q * 512 + j, 128, stride=4)
                total = bins[0][at, :]
                for b in bins[1:]:
                    total = total + b[at, :]
                high = total.astype(BF16)
                dens_hi[q * 128 : (q + 1) * 128, j * LANE : (j + 1) * LANE] = high
                dens_lo[q * 128 : (q + 1) * 128, j * LANE : (j + 1) * LANE] = (total - high.astype(F32)).astype(BF16)
        along = dot(dens_hi[...], yh[...]) + dot(dens_lo[...], yh[...]) + dot(dens_hi[...], yl[...])
        high = along.astype(BF16)
        along_hi[...] = high
        along_lo[...] = (along - high.astype(F32)).astype(BF16)
        p, q = along_x((ph, along_hi), (plo, along_lo), slice(0, LANE), slice(HALF, HALF + LANE))
        store(out, z, p + jnp.where(first, 0.0, q), jnp.where(first, 0.0, p) - q)
        for c, at in enumerate((LANE, HALF + LANE)):
            rest_hi[z, :, c * LANE : (c + 1) * LANE] = along_hi[:, at : at + LANE]
            rest_lo[z, :, c * LANE : (c + 1) * LANE] = along_lo[:, at : at + LANE]
        return carry

    lax.fori_loop(0, ZD, plane, 0)


def rest_kernel(rest_hi, rest_lo, ph, plo, out):
    p, q = along_x((ph, rest_hi.at[0]), (plo, rest_lo.at[0]), slice(0, LANE), slice(LANE, 2 * LANE))
    store(out, 0, p + q, p - q)


def rest(rest_hi, rest_lo, ph, plo):
    plane = pl.BlockSpec((1, NX, 2 * LANE), lambda z: (z, 0, 0))
    table = pl.BlockSpec((2 * NX, NX), lambda z: (0, 0))
    return pl.pallas_call(
        rest_kernel,
        grid=(ZD,),
        out_shape=jax.ShapeDtypeStruct((DEV, ZD, 2 * NU, 2 * LANE), BF16),
        in_specs=[plane, plane, table, table],
        out_specs=pl.BlockSpec((DEV, 1, 2 * NU, 2 * LANE), lambda z: (0, z, 0, 0)),
        name="rest",
    )(rest_hi, rest_lo, ph, plo)


def front(charges, cells, splines, counts, tabs):
    vmem = pl.BlockSpec(memory_space=pltpu.VMEM)
    smem = pl.BlockSpec(memory_space=pltpu.SMEM)
    hbm = pl.BlockSpec(memory_space=pl.ANY)
    rows = lax.shift_right_logical(cells, 7).reshape(SPREAD, TILES, LANE).transpose(1, 0, 2).reshape(-1)
    return pl.pallas_call(
        front_kernel,
        out_shape=(
            jax.ShapeDtypeStruct((DEV, ZD, 2 * NU, 2 * LANE), BF16),
            jax.ShapeDtypeStruct((ZD, NX, 2 * LANE), BF16),
            jax.ShapeDtypeStruct((ZD, NX, 2 * LANE), BF16),
        ),
        in_specs=[hbm, vmem, vmem, vmem, smem] + [hbm] * 4,
        out_specs=(vmem, vmem, vmem),
        scratch_shapes=[pltpu.VMEM((ROWS, LANE), F32)] * SPREAD
        + [pltpu.VMEM((LANE, LANE), F32)] * 2
        + [pltpu.VMEM((TILES, SPREAD, LANE), jnp.int32), pltpu.VMEM((TILES, SPREAD, LANE), F32)]
        + [pltpu.VMEM((NX, NY), BF16)] * 4
        + [pltpu.VMEM(t.shape, BF16) for t in tabs]
        + [pltpu.SemaphoreType.DMA((TILES,)), pltpu.SemaphoreType.DMA((4,))]
        + [pltpu.SMEM((SPREAD * LANE,), jnp.int32)] * TILES,
        name="front",
    )(rows, cells, splines, charges.reshape(1, SLOTS), counts, *tabs)


def green_kernel(blocks, spectrum, green, out, flat, sums, *rhs):
    plus, minus, odd = blocks
    for j in range(2):
        flat[...] = spectrum[:, :, j * LANE : (j + 1) * LANE].astype(F32).reshape(NZ * 2 * NU, LANE)
        for ul in range(NU):
            for c in range(2):
                rows = flat[pl.ds(c * NU + ul, NZ, stride=2 * NU), :]
                rhs[ul][j, :, c * LANE : (c + 1) * LANE] = rows.astype(BF16)
    first = lax.broadcasted_iota(jnp.int32, (NZ, 2 * LANE), 1) % LANE == 0
    for ul in range(NU):
        m0 = dot(green[ul, plus], rhs[ul][0])
        m1 = jnp.where(first, dot(green[ul, odd], rhs[ul][1]), dot(green[ul, minus], rhs[ul][1]))
        if plus == 0:
            total = m0 + jnp.where(first, 0.0, m1)
            apart = jnp.where(first, 0.0, m0) - m1
        else:
            total = m0 + m1
            apart = m0 - m1
        re = pl.ds(ul, NZ, stride=2 * NU)
        im = pl.ds(NU + ul, NZ, stride=2 * NU)
        sums[0, re, :] = total[:, :LANE]
        sums[0, im, :] = total[:, LANE:]
        sums[1, re, :] = -apart[:, LANE:]
        sums[1, im, :] = apart[:, :LANE]
    for j in range(2):
        out[:, :, j * LANE : (j + 1) * LANE] = sums[j].astype(BF16).reshape(NZ, 2 * NU, LANE)


def mix(pencil, green, blocks):
    vmem = pl.BlockSpec(memory_space=pltpu.VMEM)
    return pl.pallas_call(
        functools.partial(green_kernel, blocks),
        out_shape=jax.ShapeDtypeStruct((NZ, 2 * NU, 2 * LANE), BF16),
        in_specs=[vmem, vmem],
        out_specs=vmem,
        scratch_shapes=[pltpu.VMEM((NZ * 2 * NU, LANE), F32), pltpu.VMEM((2, NZ * 2 * NU, LANE), F32)]
        + [pltpu.VMEM((2, NZ, 2 * LANE), BF16)] * NU,
        name=f"mix{blocks[0]}",
    )(pencil.reshape(NZ, 2 * NU, 2 * LANE), green).reshape(DEV, ZD, 2 * NU, 2 * LANE)


def back_kernel(mixed, inverse_x, inverse_y, *refs):
    middle = dot(inverse_x[...], mixed[:, 0].reshape(2 * NX, 2 * LANE))
    total = dot(middle.astype(BF16), inverse_y[...])
    refs[-1][0] = total if len(refs) == 1 else total + refs[0][0]


def back(returned, inverse_x, inverse_y, *before):
    plane = pl.BlockSpec((1, NX, NY), lambda z: (z, 0, 0))
    return pl.pallas_call(
        back_kernel,
        grid=(ZD,),
        out_shape=jax.ShapeDtypeStruct((ZD, NX, NY), F32),
        in_specs=[
            pl.BlockSpec((DEV, 1, 2 * NU, 2 * LANE), lambda z: (0, z, 0, 0)),
            pl.BlockSpec((NX, 2 * NX), lambda z: (0, 0)),
            pl.BlockSpec((2 * LANE, NY), lambda z: (0, 0)),
        ]
        + [plane] * len(before),
        out_specs=plane,
        name=f"back{len(before)}",
    )(returned, inverse_x, inverse_y, *before)


def exchange(chunk):
    return lax.all_to_all(chunk, AXES, split_axis=0, concat_axis=0, tiled=True)


def shards(charges, cells, splines, counts, green):
    yh, yl, ph, plo, inverse_x, inverse_a, inverse_b = (jnp.asarray(t) for t in tables())
    first, rest_hi, rest_lo = front(charges, cells, splines, counts, (yh, yl, ph, plo))
    pencil_a = exchange(first)
    pencil_b = exchange(rest(rest_hi, rest_lo, ph, plo))
    back_a = exchange(mix(pencil_a, green, (0, 3, 2)))
    back_b = exchange(mix(pencil_b, green, (1, 2, 3)))
    return back(back_b, inverse_x, inverse_b, back(back_a, inverse_x, inverse_a))


def solution(mesh):
    in_specs = (
        P(AXES),
        P(None, AXES),
        P(None, AXES),
        P(AXES),
        P(AXES, None, None, None),
    )
    return jax.shard_map(
        shards, mesh=mesh, in_specs=in_specs, out_specs=P(AXES, None, None), check_vma=False
    )
```

```python
import jax
import jax.numpy as jnp
import numpy as np
from jax import lax
from jax.experimental import pallas as pl
from jax.experimental.pallas import tpu as pltpu
from jax.sharding import PartitionSpec as P

NX = 512
NY = 512
NZ = 384
KYB = 4
AXES = ("zg", "xy")
DEV = 128
ZD = 3
NU = NX // DEV
HALF = NY // 2
LANE = 128
SLOTS = 2048
SPREAD = 8
TILES = SLOTS // LANE
ROWS = ZD * NX * NY // LANE
F32 = jnp.float32
BF16 = jnp.bfloat16


def split(table):
    high = table.astype(BF16)
    return high, (table - high.astype(np.float64)).astype(BF16)


def angles(left, right):
    return (np.outer(left, right) % NX) * (2.0 * np.pi / NX)


def waves():
    device = np.arange(DEV)[:, None, None]
    half = np.arange(2)[None, :, None]
    number = np.arange(NU // 2)[None, None, :]
    return device * NU + number * 2 + (half + device // (DEV // 2)) % 2


def forward_tables():
    y = np.arange(NY)
    v = np.arange(HALF)
    along_y = np.concatenate([np.cos(angles(y, v)), -np.sin(angles(y, v))], axis=1)
    along_y[:, HALF] = np.where(y % 2 == 0, 1.0, -1.0)
    x = np.arange(NX // 2)
    low = np.arange(DEV // 2)[:, None, None]
    number = np.arange(NU // 2)[None, None, :]
    out = [*split(along_y / 512.0)]
    for odd in range(2):
        which = (np.arange(2)[None, :, None] + odd) % 2
        a = angles(((low + which * (DEV // 2)) * NU + number * 2 + odd).reshape(-1), x).reshape(DEV // 2, NU, NX // 2)
        out += split(np.stack([np.cos(a), -np.sin(a)], axis=1).reshape(NX, NX // 2))
    return tuple(out)


def inverse_tables():
    wave = jnp.asarray(waves().reshape(DEV, 1, NU), jnp.int32)
    wave = jnp.broadcast_to(wave, (DEV, 2, NU)).reshape(1, 2 * NX)
    quarter = jnp.tile(jnp.repeat(jnp.arange(2, dtype=jnp.int32), NU), DEV)[None, :] * (NX // 4)
    x = lax.broadcasted_iota(jnp.int32, (NX, 2 * NX), 0)
    step = 2.0 * np.pi / NX
    along_x = jnp.cos(((x * wave + quarter) & (NX - 1)).astype(F32) * step)
    row = lax.broadcasted_iota(jnp.int32, (NY, NY), 0)
    y = lax.broadcasted_iota(jnp.int32, (NY, NY), 1)
    phase = (row & (HALF - 1)) * y - jnp.where(row < HALF, 0, NY // 4)
    phase = jnp.where(row == HALF, (y + 1) * (NY // 2), phase)
    along_y = jnp.cos((phase & (NY - 1)).astype(F32) * step) / 512.0
    return along_x.astype(BF16), along_y.astype(BF16)


def in_hbm(*arrays):
    return tuple(pltpu.with_memory_space_constraint(a, pltpu.HBM) for a in arrays)


def dot(a, b):
    return jnp.dot(a, b, preferred_element_type=F32)


def turn(q):
    whole = q.reshape(-1, 2 * NU, q.shape[1])
    real = lax.broadcasted_iota(jnp.int32, whole.shape, 1) < NU
    swapped = pltpu.roll(whole, NU, 1)
    return jnp.where(real, -swapped, swapped).reshape(q.shape)


def front_kernel(
    rows_hbm, cells_hbm, splines_hbm, charges_hbm, counts, yh_hbm, yl_hbm, eh_hbm, el_hbm, oh_hbm, ol_hbm, out_hbm, *scratch
):
    bins = scratch[:SPREAD]
    spikes = scratch[8:10]
    lanes, values, dens_hi, dens_lo, fold_hi, fold_lo = scratch[10:16]
    tabs = scratch[16:22]
    out, cells, splines, charges, row_sem, tab_sem, out_sem, slot_sem = scratch[22:30]
    row_of = scratch[30:]
    slot_copies = [
        pltpu.make_async_copy(s, d, slot_sem.at[i])
        for i, (s, d) in enumerate(((cells_hbm, cells), (splines_hbm, splines), (charges_hbm, charges)))
    ]
    for copy in slot_copies:
        copy.start()
    row_copies = [
        pltpu.make_async_copy(rows_hbm.at[pl.ds(t * 1024, 1024)], row_of[t], row_sem.at[t]) for t in range(TILES)
    ]
    for copy in row_copies:
        copy.start()
    sources = (yh_hbm, yl_hbm, eh_hbm, el_hbm, oh_hbm, ol_hbm)
    tab_copies = [pltpu.make_async_copy(s, d, tab_sem.at[i]) for i, (s, d) in enumerate(zip(sources, tabs))]
    for copy in tab_copies:
        copy.start()
    zeros = jnp.zeros((256, LANE), F32)

    def clear(i, carry):
        for b in bins:
            b[pl.ds(i * 256, 256), :] = zeros
        return carry

    lax.fori_loop(0, ROWS // 256, clear, 0)
    for copy in slot_copies:
        copy.wait()
    slot = lax.broadcasted_iota(jnp.int32, (1, SLOTS), 1)
    live = (slot < counts[0]).astype(F32)
    value = splines[...] * (charges[...] * live)
    lane_of = cells[...] & (LANE - 1)
    for t in range(TILES):
        lanes[t] = lane_of[:, t * LANE : (t + 1) * LANE]
        values[t] = value[:, t * LANE : (t + 1) * LANE]
    lane = lax.broadcasted_iota(jnp.int32, (SPREAD, LANE), 1)

    def build(spike, g):
        pick = jnp.full((SPREAD, LANE), g, jnp.int32)
        for t in range(TILES):
            at = jnp.take_along_axis(lanes[t], pick, axis=1)
            amount = jnp.take_along_axis(values[t], pick, axis=1)
            spike[t * SPREAD : (t + 1) * SPREAD, :] = jnp.where(lane == at, amount, 0.0)

    def apply(spike, g):
        for t in range(TILES):
            rows = [row_of[t][g + k * LANE] for k in range(SPREAD)]
            sums = [bins[k][pl.ds(rows[k], 1), :] + spike[pl.ds(t * SPREAD + k, 1), :] for k in range(SPREAD)]
            for k in range(SPREAD):
                bins[k][pl.ds(rows[k], 1), :] = sums[k]

    build(spikes[0], 0)
    for copy in row_copies:
        copy.wait()

    def body(h, carry):
        build(spikes[1], 2 * h + 1)
        apply(spikes[0], 2 * h)
        build(spikes[0], jnp.minimum(2 * h + 2, LANE - 1))
        apply(spikes[1], 2 * h + 1)
        return carry

    lax.fori_loop(0, LANE // 2, body, 0)
    for copy in tab_copies:
        copy.wait()
    yh, yl, *along_x = tabs
    first = lax.broadcasted_iota(jnp.int32, (NX, LANE), 1) == 0
    lower = lax.broadcasted_iota(jnp.int32, (NX, LANE), 0) % 4 < 2

    def plane(z, carry):
        for j in range(NY // LANE):
            for q in range(4):
                at = pl.ds(z * (NX * 4) + q * 512 + j, 128, stride=4)
                total = bins[0][at, :]
                for b in bins[1:]:
                    total = total + b[at, :]
                high = total.astype(BF16)
                dens_hi[q * 128 : (q + 1) * 128, j * LANE : (j + 1) * LANE] = high
                dens_lo[q * 128 : (q + 1) * 128, j * LANE : (j + 1) * LANE] = (total - high.astype(F32)).astype(BF16)
        along = dot(dens_hi[...], yh[...]) + dot(dens_lo[...], yh[...]) + dot(dens_hi[...], yl[...])
        near, far = along[: NX // 2], along[NX // 2 :]
        parts = []
        for h, folded in enumerate((near + far, near - far)):
            high = folded.astype(BF16)
            fold_hi[h] = high
            fold_lo[h] = (folded - high.astype(F32)).astype(BF16)
            tab_hi, tab_lo = along_x[2 * h], along_x[2 * h + 1]
            p, q = (
                dot(tab_hi[...], fold_hi[h, :, c]) + dot(tab_hi[...], fold_lo[h, :, c]) + dot(tab_lo[...], fold_hi[h, :, c])
                for c in (slice(0, HALF), slice(HALF, NY))
            )
            q = turn(q)
            p0, p1, q0, q1 = p[:, :LANE], p[:, LANE:], q[:, :LANE], q[:, LANE:]
            minus0 = jnp.where(first, 0.0, p0) - q0
            minus1 = p1 - q1
            parts.append(
                (
                    p0 + jnp.where(first, 0.0, q0),
                    p1 + q1,
                    jnp.where(first, minus1, minus0),
                    jnp.where(first, minus0, minus1),
                )
            )
        for j, (even, odd) in enumerate(zip(*parts)):
            at = slice(j * LANE, (j + 1) * LANE)
            shape = (DEV // 2, 2 * NU, LANE)
            out[z, : DEV // 2, :, at] = jnp.where(lower, even, odd).astype(BF16).reshape(shape)
            out[z, DEV // 2 :, :, at] = jnp.where(lower, odd, even).astype(BF16).reshape(shape)
        pltpu.make_async_copy(out.at[z], out_hbm.at[:, z], out_sem.at[z]).start()
        return carry

    lax.fori_loop(0, ZD, plane, 0)
    for z in range(ZD):
        pltpu.make_async_copy(out.at[z], out_hbm.at[:, z], out_sem.at[z]).wait()


def front(charges, cells, splines, counts, tabs):
    smem = pl.BlockSpec(memory_space=pltpu.SMEM)
    hbm = pl.BlockSpec(memory_space=pltpu.HBM)
    rows = lax.shift_right_logical(cells, 7).reshape(SPREAD, TILES, LANE).transpose(1, 0, 2).reshape(-1)
    return pl.pallas_call(
        front_kernel,
        out_shape=pltpu.HBM((DEV, ZD, 2 * NU, NY), BF16),
        in_specs=[hbm] * 4 + [smem] + [hbm] * 6,
        out_specs=hbm,
        scratch_shapes=[pltpu.VMEM((ROWS, LANE), F32)] * SPREAD
        + [pltpu.VMEM((LANE, LANE), F32)] * 2
        + [pltpu.VMEM((TILES, SPREAD, LANE), jnp.int32), pltpu.VMEM((TILES, SPREAD, LANE), F32)]
        + [pltpu.VMEM((NX, NY), BF16)] * 2
        + [pltpu.VMEM((2, NX // 2, NY), BF16)] * 2
        + [pltpu.VMEM(t.shape, BF16) for t in tabs]
        + [pltpu.VMEM((ZD, DEV, 2 * NU, NY), BF16)]
        + [pltpu.VMEM((SPREAD, SLOTS), jnp.int32), pltpu.VMEM((SPREAD, SLOTS), F32), pltpu.VMEM((1, SLOTS), F32)]
        + [pltpu.SemaphoreType.DMA((n,)) for n in (TILES, 6, ZD, 3)]
        + [pltpu.SMEM((SPREAD * LANE,), jnp.int32)] * TILES,
        compiler_params=pltpu.CompilerParams(vmem_limit_bytes=44 << 20),
        name="front",
    )(*in_hbm(rows, cells, splines, charges.reshape(1, SLOTS)), counts, *in_hbm(*tabs))


BLOCK = (0, 1, 3, 2)
PART = NZ // 2


def green_kernel(odd_first, spectrum, green_hbm, out_hbm, green, out, flat, sums, green_sem, out_sem, *rhs):
    waves_of = [2 * (ul % 2) + jnp.bitwise_xor(odd_first[0], ul // 2) for ul in range(NU)]
    fetches = [
        pltpu.make_async_copy(green_hbm.at[waves_of[ul]], green.at[ul], green_sem.at[ul]) for ul in range(NU)
    ]
    for fetch in fetches:
        fetch.start()
    for j in range(KYB):
        flat[...] = spectrum[:, :, j * LANE : (j + 1) * LANE].astype(F32).reshape(NZ * 2 * NU, LANE)
        for ul in range(NU):
            for c in range(2):
                rows = flat[pl.ds(c * NU + ul, NZ, stride=2 * NU), :]
                rhs[ul][j, :, c * LANE : (c + 1) * LANE] = rows.astype(BF16)
    first = lax.broadcasted_iota(jnp.int32, (PART, 2 * LANE), 1) % LANE == 0
    sends = []
    for part in range(2):
        planes = slice(part * PART, (part + 1) * PART)
        for ul in range(NU):
            if part == 0:
                fetches[ul].wait()
            m0, m1, m2, m3 = (dot(green[ul, BLOCK[j], planes, :], rhs[ul][j]) for j in range(KYB))
            s2 = jnp.where(first, m3, m2)
            s3 = jnp.where(first, m2, m3)
            t0 = m0 + jnp.where(first, 0.0, s2)
            d0 = jnp.where(first, 0.0, m0) - s2
            t1 = m1 + s3
            d1 = m1 - s3
            re = pl.ds(ul, PART, stride=2 * NU)
            im = pl.ds(NU + ul, PART, stride=2 * NU)
            sums[0, re, :] = t0[:, :LANE]
            sums[0, im, :] = t0[:, LANE:]
            sums[1, re, :] = t1[:, :LANE]
            sums[1, im, :] = t1[:, LANE:]
            sums[2, re, :] = -d0[:, LANE:]
            sums[2, im, :] = d0[:, :LANE]
            sums[3, re, :] = -d1[:, LANE:]
            sums[3, im, :] = d1[:, :LANE]
        for j in range(KYB):
            out[planes, :, j * LANE : (j + 1) * LANE] = sums[j].astype(BF16).reshape(PART, 2 * NU, LANE)
        send = pltpu.make_async_copy(out.at[planes], out_hbm.at[planes], out_sem.at[part])
        send.start()
        sends.append(send)
    for send in sends:
        send.wait()


def mix(pencil, green):
    vmem = pl.BlockSpec(memory_space=pltpu.VMEM)
    hbm = pl.BlockSpec(memory_space=pltpu.HBM)
    return pl.pallas_call(
        green_kernel,
        out_shape=pltpu.HBM((NZ, 2 * NU, NY), BF16),
        in_specs=[pl.BlockSpec(memory_space=pltpu.SMEM), vmem, hbm],
        out_specs=hbm,
        compiler_params=pltpu.CompilerParams(vmem_limit_bytes=36 << 20),
        scratch_shapes=[
            pltpu.VMEM((NU, KYB, NZ, NZ), BF16),
            pltpu.VMEM((NZ, 2 * NU, NY), BF16),
            pltpu.VMEM((NZ * 2 * NU, LANE), F32),
            pltpu.VMEM((KYB, PART * 2 * NU, LANE), F32),
            pltpu.SemaphoreType.DMA((NU,)),
            pltpu.SemaphoreType.DMA((2,)),
        ]
        + [pltpu.VMEM((KYB, NZ, 2 * LANE), BF16)] * NU,
        name="mix",
    )(lax.axis_index("zg").astype(jnp.int32).reshape(1), pencil.reshape(NZ, 2 * NU, NY), *in_hbm(green))


def back_kernel(mixed, x_hbm, y_hbm, out_hbm, along_x, along_y, out, tab_sem, out_sem):
    fetches = [
        pltpu.make_async_copy(x_hbm.at[pl.ds(0, HALF)], along_x.at[pl.ds(0, HALF)], tab_sem.at[0]),
        pltpu.make_async_copy(y_hbm, along_y, tab_sem.at[1]),
        pltpu.make_async_copy(x_hbm.at[pl.ds(HALF, HALF)], along_x.at[pl.ds(HALF, HALF)], tab_sem.at[2]),
    ]
    for fetch in fetches:
        fetch.start()
    sends = []
    for z in range(ZD):
        waves = mixed[:, z].reshape(2 * NX, NY)
        for h in range(2):
            rows = pl.ds(h * HALF, HALF)
            if z == 0:
                fetches[2 * h].wait()
            middle = dot(along_x[rows, :], waves).astype(BF16)
            if z == 0 and h == 0:
                fetches[1].wait()
            out[z, rows, :] = dot(middle, along_y[...])
            send = pltpu.make_async_copy(out.at[z, rows], out_hbm.at[z, rows], out_sem.at[2 * z + h])
            send.start()
            sends.append(send)
    for send in sends:
        send.wait()


def back(returned, inverse_x, inverse_y):
    vmem = pl.BlockSpec(memory_space=pltpu.VMEM)
    hbm = pl.BlockSpec(memory_space=pltpu.HBM)
    return pl.pallas_call(
        back_kernel,
        out_shape=jax.ShapeDtypeStruct((ZD, NX, NY), F32),
        in_specs=[vmem, hbm, hbm],
        out_specs=hbm,
        compiler_params=pltpu.CompilerParams(vmem_limit_bytes=24 << 20),
        scratch_shapes=[
            pltpu.VMEM((NX, 2 * NX), BF16),
            pltpu.VMEM((NY, NY), BF16),
            pltpu.VMEM((ZD, NX, NY), F32),
            pltpu.SemaphoreType.DMA((3,)),
            pltpu.SemaphoreType.DMA((2 * ZD,)),
        ],
        name="back",
    )(returned, *in_hbm(inverse_x, inverse_y))


def shards(charges, cells, splines, counts, green):
    forward = tuple(jnp.asarray(t) for t in forward_tables())
    inverse_x, inverse_y = inverse_tables()
    spectrum = front(charges, cells, splines, counts, forward)
    pencil = lax.all_to_all(spectrum, AXES, split_axis=0, concat_axis=0, tiled=True)
    mixed = mix(pencil, green).reshape(DEV, ZD, 2 * NU, NY)
    returned = lax.all_to_all(mixed, AXES, split_axis=0, concat_axis=0, tiled=True)
    return back(returned, inverse_x, inverse_y)


def solution(mesh):
    in_specs = (
        P(AXES),
        P(None, AXES),
        P(None, AXES),
        P(AXES),
        P(AXES, None, None, None),
    )
    return jax.shard_map(
        shards, mesh=mesh, in_specs=in_specs, out_specs=P(AXES, None, None), check_vma=False
    )
```

```python
import jax
import jax.numpy as jnp
import numpy as np
from jax import lax
from jax.experimental import pallas as pl
from jax.experimental.pallas import tpu as pltpu
from jax.sharding import PartitionSpec as P

NX = 512
NY = 512
NZ = 384
KYB = 4
AXES = ("zg", "xy")
DEV = 128
ZD = 3
NU = NX // DEV
HALF = NY // 2
LANE = 128
WIDE = 3 * LANE
SLOTS = 2048
SPREAD = 8
TILES = SLOTS // LANE
ROWS = ZD * NX * NY // LANE
F32 = jnp.float32
BF16 = jnp.bfloat16


def split(table):
    high = table.astype(BF16)
    return high, (table - high.astype(np.float64)).astype(BF16)


def angles(left, right):
    return (np.outer(left, right) % NX) * (2.0 * np.pi / NX)


def waves():
    device = np.arange(DEV)[:, None]
    offset = np.array([[0, 2, 1, -1], [1, -1, 0, 2]])[device[:, 0] // (DEV // 2)]
    return np.where(offset < 0, -1, device * NU + offset)


def forward_tables():
    y = np.arange(NY)
    v = np.arange(HALF)
    along_y = np.concatenate([np.cos(angles(y, v)), -np.sin(angles(y, v))], axis=1)
    along_y[:, HALF] = np.where(y % 2 == 0, 1.0, -1.0)
    x = np.arange(NX // 2)
    near, far = waves()[: DEV // 2], waves()[DEV // 2 :]
    out = [*split(along_y / 512.0)]
    for wave in (np.concatenate([near[:, :2], far[:, 2:]], axis=1), np.concatenate([far[:, :2], near[:, 2:]], axis=1)):
        a = angles(wave.reshape(-1), x).reshape(DEV // 2, NU, NX // 2)
        used = (wave >= 0)[:, :, None]
        out += split(np.stack([np.cos(a) * used, -np.sin(a) * used], axis=1).reshape(NX, NX // 2))
    return tuple(out)


def inverse_tables():
    wave = waves().reshape(DEV, 1, NU).repeat(2, axis=1).reshape(1, 2 * NX)
    used = jnp.asarray(wave >= 0, F32)
    wave = jnp.asarray(wave, jnp.int32)
    quarter = jnp.tile(jnp.repeat(jnp.arange(2, dtype=jnp.int32), NU), DEV)[None, :] * (NX // 4)
    x = lax.broadcasted_iota(jnp.int32, (NX, 2 * NX), 0)
    step = 2.0 * np.pi / NX
    along_x = jnp.cos(((x * wave + quarter) & (NX - 1)).astype(F32) * step) * used
    row = lax.broadcasted_iota(jnp.int32, (NY, NY), 0)
    y = lax.broadcasted_iota(jnp.int32, (NY, NY), 1)
    phase = (row & (HALF - 1)) * y - jnp.where(row < HALF, 0, NY // 4)
    phase = jnp.where(row == HALF, (y + 1) * (NY // 2), phase)
    along_y = jnp.cos((phase & (NY - 1)).astype(F32) * step) / 512.0
    return along_x.astype(BF16), along_y.astype(BF16)


def in_hbm(*arrays):
    return tuple(pltpu.with_memory_space_constraint(a, pltpu.HBM) for a in arrays)


def dot(a, b):
    return jnp.dot(a, b, preferred_element_type=F32)


def turn(q):
    whole = q.reshape(-1, 2 * NU, q.shape[1])
    real = lax.broadcasted_iota(jnp.int32, whole.shape, 1) < NU
    swapped = pltpu.roll(whole, NU, 1)
    return jnp.where(real, -swapped, swapped).reshape(q.shape)


def front_kernel(
    rows_hbm, cells_hbm, splines_hbm, charges_hbm, counts, yh_hbm, yl_hbm, eh_hbm, el_hbm, oh_hbm, ol_hbm, out_hbm, *scratch
):
    bins = scratch[:SPREAD]
    spikes = scratch[8:10]
    lanes, values, dens_hi, dens_lo, fold_hi, fold_lo = scratch[10:16]
    tabs = scratch[16:22]
    out, cells, splines, charges, row_sem, tab_sem, out_sem, slot_sem = scratch[22:30]
    row_of = scratch[30:]
    slot_copies = [
        pltpu.make_async_copy(s, d, slot_sem.at[i])
        for i, (s, d) in enumerate(((cells_hbm, cells), (splines_hbm, splines), (charges_hbm, charges)))
    ]
    for copy in slot_copies:
        copy.start()
    row_copies = [
        pltpu.make_async_copy(rows_hbm.at[pl.ds(t * 1024, 1024)], row_of[t], row_sem.at[t]) for t in range(TILES)
    ]
    for copy in row_copies:
        copy.start()
    sources = (yh_hbm, yl_hbm, eh_hbm, el_hbm, oh_hbm, ol_hbm)
    tab_copies = [pltpu.make_async_copy(s, d, tab_sem.at[i]) for i, (s, d) in enumerate(zip(sources, tabs))]
    for copy in tab_copies:
        copy.start()
    zeros = jnp.zeros((256, LANE), F32)

    def clear(i, carry):
        for b in bins:
            b[pl.ds(i * 256, 256), :] = zeros
        return carry

    lax.fori_loop(0, ROWS // 256, clear, 0)
    for copy in slot_copies:
        copy.wait()
    slot = lax.broadcasted_iota(jnp.int32, (1, SLOTS), 1)
    live = (slot < counts[0]).astype(F32)
    value = splines[...] * (charges[...] * live)
    lane_of = cells[...] & (LANE - 1)
    for t in range(TILES):
        lanes[t] = lane_of[:, t * LANE : (t + 1) * LANE]
        values[t] = value[:, t * LANE : (t + 1) * LANE]
    lane = lax.broadcasted_iota(jnp.int32, (SPREAD, LANE), 1)

    def build(spike, g):
        pick = jnp.full((SPREAD, LANE), g, jnp.int32)
        for t in range(TILES):
            at = jnp.take_along_axis(lanes[t], pick, axis=1)
            amount = jnp.take_along_axis(values[t], pick, axis=1)
            spike[t * SPREAD : (t + 1) * SPREAD, :] = jnp.where(lane == at, amount, 0.0)

    def apply(spike, g):
        for t in range(TILES):
            rows = [row_of[t][g + k * LANE] for k in range(SPREAD)]
            sums = [bins[k][pl.ds(rows[k], 1), :] + spike[pl.ds(t * SPREAD + k, 1), :] for k in range(SPREAD)]
            for k in range(SPREAD):
                bins[k][pl.ds(rows[k], 1), :] = sums[k]

    build(spikes[0], 0)
    for copy in row_copies:
        copy.wait()

    def body(h, carry):
        build(spikes[1], 2 * h + 1)
        apply(spikes[0], 2 * h)
        build(spikes[0], jnp.minimum(2 * h + 2, LANE - 1))
        apply(spikes[1], 2 * h + 1)
        return carry

    lax.fori_loop(0, LANE // 2, body, 0)
    for copy in tab_copies:
        copy.wait()
    yh, yl, *along_x = tabs
    first = lax.broadcasted_iota(jnp.int32, (NX, LANE), 1) == 0
    lower = lax.broadcasted_iota(jnp.int32, (NX, LANE), 0) % NU < 2
    row_of_tile = lax.broadcasted_iota(jnp.int32, (DEV // 2, 2 * NU, LANE), 1) % NU

    def plane(z, carry):
        for j in range(NY // LANE):
            for q in range(4):
                at = pl.ds(z * (NX * 4) + q * 512 + j, 128, stride=4)
                total = bins[0][at, :]
                for b in bins[1:]:
                    total = total + b[at, :]
                high = total.astype(BF16)
                dens_hi[q * 128 : (q + 1) * 128, j * LANE : (j + 1) * LANE] = high
                dens_lo[q * 128 : (q + 1) * 128, j * LANE : (j + 1) * LANE] = (total - high.astype(F32)).astype(BF16)
        along = dot(dens_hi[...], yh[...]) + dot(dens_lo[...], yh[...]) + dot(dens_hi[...], yl[...])
        near, far = along[: NX // 2], along[NX // 2 :]
        parts = []
        for h, folded in enumerate((near + far, near - far)):
            high = folded.astype(BF16)
            fold_hi[h] = high
            fold_lo[h] = (folded - high.astype(F32)).astype(BF16)
            tab_hi, tab_lo = along_x[2 * h], along_x[2 * h + 1]
            p, q = (
                dot(tab_hi[...], fold_hi[h, :, c]) + dot(tab_hi[...], fold_lo[h, :, c]) + dot(tab_lo[...], fold_hi[h, :, c])
                for c in (slice(0, HALF), slice(HALF, NY))
            )
            q = turn(q)
            p0, p1, q0, q1 = p[:, :LANE], p[:, LANE:], q[:, :LANE], q[:, LANE:]
            minus0 = jnp.where(first, 0.0, p0) - q0
            minus1 = p1 - q1
            parts.append(
                (
                    p0 + jnp.where(first, 0.0, q0),
                    p1 + q1,
                    jnp.where(first, minus1, minus0),
                    jnp.where(first, minus0, minus1),
                )
            )
        near = [jnp.where(lower, even, odd) for even, odd in zip(*parts)]
        far = [jnp.where(lower, odd, even) for even, odd in zip(*parts)]
        for side, (groups, spare) in enumerate(((near, 3), (far, 1))):
            shape = (DEV // 2, 2 * NU, LANE)
            last = groups[3].reshape(shape)
            for j in range(3):
                moved = pltpu.roll(last, (spare - (j ^ 2 * side)) % 8, 1)
                out[z, side * (DEV // 2) : (side + 1) * (DEV // 2), :, j * LANE : (j + 1) * LANE] = jnp.where(
                    row_of_tile == spare, moved, groups[j].reshape(shape)
                ).astype(BF16)
        pltpu.make_async_copy(out.at[z], out_hbm.at[:, z], out_sem.at[z]).start()
        return carry

    lax.fori_loop(0, ZD, plane, 0)
    for z in range(ZD):
        pltpu.make_async_copy(out.at[z], out_hbm.at[:, z], out_sem.at[z]).wait()


def front(charges, cells, splines, counts, tabs):
    smem = pl.BlockSpec(memory_space=pltpu.SMEM)
    hbm = pl.BlockSpec(memory_space=pltpu.HBM)
    rows = lax.shift_right_logical(cells, 7).reshape(SPREAD, TILES, LANE).transpose(1, 0, 2).reshape(-1)
    return pl.pallas_call(
        front_kernel,
        out_shape=pltpu.HBM((DEV, ZD, 2 * NU, WIDE), BF16),
        in_specs=[hbm] * 4 + [smem] + [hbm] * 6,
        out_specs=hbm,
        scratch_shapes=[pltpu.VMEM((ROWS, LANE), F32)] * SPREAD
        + [pltpu.VMEM((LANE, LANE), F32)] * 2
        + [pltpu.VMEM((TILES, SPREAD, LANE), jnp.int32), pltpu.VMEM((TILES, SPREAD, LANE), F32)]
        + [pltpu.VMEM((NX, NY), BF16)] * 2
        + [pltpu.VMEM((2, NX // 2, NY), BF16)] * 2
        + [pltpu.VMEM(t.shape, BF16) for t in tabs]
        + [pltpu.VMEM((ZD, DEV, 2 * NU, WIDE), BF16)]
        + [pltpu.VMEM((SPREAD, SLOTS), jnp.int32), pltpu.VMEM((SPREAD, SLOTS), F32), pltpu.VMEM((1, SLOTS), F32)]
        + [pltpu.SemaphoreType.DMA((n,)) for n in (TILES, 6, ZD, 3)]
        + [pltpu.SMEM((SPREAD * LANE,), jnp.int32)] * TILES,
        compiler_params=pltpu.CompilerParams(vmem_limit_bytes=44 << 20),
        name="front",
    )(*in_hbm(rows, cells, splines, charges.reshape(1, SLOTS)), counts, *in_hbm(*tabs))


WAVE = (0, 2, 1)
BLOCK = (0, 1, 3, 2)
MIRROR = (3, 2, 0, 1)
SWAP = (1, 3, 0, 2)
PART = NZ // 2


def green_kernel(far, spectrum, green_hbm, mirror_hbm, out_hbm, green, out, flat, sums, swapped, green_sem, out_sem, *rhs):
    sources = [green_hbm.at[w] for w in WAVE] + [mirror_hbm]
    fetches = [pltpu.make_async_copy(s, green.at[i], green_sem.at[i]) for i, s in enumerate(sources)]
    for fetch in fetches:
        fetch.start()
    at = [jnp.bitwise_xor(row, 2 * far[0]) for row in range(NU)]
    for j in range(3):
        flat[...] = spectrum[:, :, j * LANE : (j + 1) * LANE].astype(F32).reshape(NZ * 2 * NU, LANE)
        for row in range(NU):
            for c in range(2):
                values = flat[pl.ds(c * NU + at[row], NZ, stride=2 * NU), :].astype(BF16)
                to, group = (rhs[row], j) if row < 3 else (rhs[j], 3)
                to[group, :, c * LANE : (c + 1) * LANE] = values
    first = lax.broadcasted_iota(jnp.int32, (NZ, 2 * LANE), 1) % LANE == 0
    for j in range(KYB):
        swapped[j] = jnp.where(first, rhs[2][SWAP[j]], rhs[2][j])
    first = first[:PART]
    sends = []
    for part in range(2):
        planes = slice(part * PART, (part + 1) * PART)
        for row in range(3):
            if part == 0:
                fetches[row].wait()
            m = [dot(green[row, BLOCK[j], planes, :], rhs[row][j]) for j in range(KYB)]
            if row == 2:
                if part == 0:
                    fetches[3].wait()
                other = [dot(green[3, MIRROR[j], planes, :], swapped[j]) for j in range(KYB)]
                m = [m[j] + jnp.where(first, other[SWAP.index(j)], other[j]) for j in range(KYB)]
            s2 = jnp.where(first, m[3], m[2])
            s3 = jnp.where(first, m[2], m[3])
            t0 = m[0] + jnp.where(first, 0.0, s2)
            d0 = jnp.where(first, 0.0, m[0]) - s2
            t1 = m[1] + s3
            d1 = m[1] - s3
            groups = (
                (t0[:, :LANE], t0[:, LANE:]),
                (t1[:, :LANE], t1[:, LANE:]),
                (-d0[:, LANE:], d0[:, :LANE]),
                (-d1[:, LANE:], d1[:, :LANE]),
            )
            for j, group in enumerate(groups):
                for c in range(2):
                    to, slot = (j, row) if j < 3 else (row, 3)
                    sums[to, pl.ds(c * NU + at[slot], PART, stride=2 * NU), :] = group[c]
        for j in range(3):
            out[planes, :, j * LANE : (j + 1) * LANE] = sums[j].astype(BF16).reshape(PART, 2 * NU, LANE)
        send = pltpu.make_async_copy(out.at[planes], out_hbm.at[planes], out_sem.at[part])
        send.start()
        sends.append(send)
    for send in sends:
        send.wait()


def mix(pencil, green, mirror):
    vmem = pl.BlockSpec(memory_space=pltpu.VMEM)
    hbm = pl.BlockSpec(memory_space=pltpu.HBM)
    return pl.pallas_call(
        green_kernel,
        out_shape=pltpu.HBM((NZ, 2 * NU, WIDE), BF16),
        in_specs=[pl.BlockSpec(memory_space=pltpu.SMEM), vmem, hbm, hbm],
        out_specs=hbm,
        compiler_params=pltpu.CompilerParams(vmem_limit_bytes=36 << 20),
        scratch_shapes=[
            pltpu.VMEM((NU, KYB, NZ, NZ), BF16),
            pltpu.VMEM((NZ, 2 * NU, WIDE), BF16),
            pltpu.VMEM((NZ * 2 * NU, LANE), F32),
            pltpu.VMEM((3, PART * 2 * NU, LANE), F32),
            pltpu.VMEM((KYB, NZ, 2 * LANE), BF16),
            pltpu.SemaphoreType.DMA((NU,)),
            pltpu.SemaphoreType.DMA((2,)),
        ]
        + [pltpu.VMEM((KYB, NZ, 2 * LANE), BF16)] * 3,
        name="mix",
    )(lax.axis_index("zg").astype(jnp.int32).reshape(1), pencil.reshape(NZ, 2 * NU, WIDE), *in_hbm(green, mirror))


def back_kernel(mixed, x_hbm, y_hbm, out_hbm, along_x, along_y, out, rest, tab_sem, out_sem):
    fetches = [
        pltpu.make_async_copy(x_hbm.at[pl.ds(0, HALF)], along_x.at[pl.ds(0, HALF)], tab_sem.at[0]),
        pltpu.make_async_copy(y_hbm, along_y, tab_sem.at[1]),
        pltpu.make_async_copy(x_hbm.at[pl.ds(HALF, HALF)], along_x.at[pl.ds(HALF, HALF)], tab_sem.at[2]),
    ]
    for fetch in fetches:
        fetch.start()
    row_of_tile = lax.broadcasted_iota(jnp.int32, (DEV // 2, 2 * NU, LANE), 1) % NU
    sends = []
    for z in range(ZD):
        for side in range(2):
            devices = slice(side * (DEV // 2), (side + 1) * (DEV // 2))
            spare = 3 - 2 * side
            last = None
            for j in range(3):
                group = mixed[devices, z, :, j * LANE : (j + 1) * LANE].astype(F32)
                moved = pltpu.roll(group, ((j ^ 2 * side) - spare) % 8, 1)
                last = moved if last is None else jnp.where(row_of_tile == (j ^ 2 * side), moved, last)
            rest[devices, :, LANE:] = last.astype(BF16)
        rest[:, :, :LANE] = mixed[:, z, :, 2 * LANE :]
        for h in range(2):
            rows = pl.ds(h * HALF, HALF)
            if z == 0:
                fetches[2 * h].wait()
            front = dot(along_x[rows, :], mixed[:, z, :, : 2 * LANE].reshape(2 * NX, 2 * LANE)).astype(BF16)
            tail = dot(along_x[rows, :], rest[...].reshape(2 * NX, 2 * LANE)).astype(BF16)
            if z == 0 and h == 0:
                fetches[1].wait()
            out[z, rows, :] = dot(front, along_y[: 2 * LANE, :]) + dot(tail, along_y[2 * LANE :, :])
            send = pltpu.make_async_copy(out.at[z, rows], out_hbm.at[z, rows], out_sem.at[2 * z + h])
            send.start()
            sends.append(send)
    for send in sends:
        send.wait()


def back(returned, inverse_x, inverse_y):
    vmem = pl.BlockSpec(memory_space=pltpu.VMEM)
    hbm = pl.BlockSpec(memory_space=pltpu.HBM)
    return pl.pallas_call(
        back_kernel,
        out_shape=jax.ShapeDtypeStruct((ZD, NX, NY), F32),
        in_specs=[vmem, hbm, hbm],
        out_specs=hbm,
        compiler_params=pltpu.CompilerParams(vmem_limit_bytes=24 << 20),
        scratch_shapes=[
            pltpu.VMEM((NX, 2 * NX), BF16),
            pltpu.VMEM((NY, NY), BF16),
            pltpu.VMEM((ZD, NX, NY), F32),
            pltpu.VMEM((DEV, 2 * NU, 2 * LANE), BF16),
            pltpu.SemaphoreType.DMA((3,)),
            pltpu.SemaphoreType.DMA((2 * ZD,)),
        ],
        name="back",
    )(returned, *in_hbm(inverse_x, inverse_y))


def steps(charges, cells, splines, counts, green):
    forward = tuple(jnp.asarray(t) for t in forward_tables())
    inverse_x, inverse_y = inverse_tables()
    mirror = lax.ppermute(green[NU - 1], AXES, [(d, DEV - 1 - d) for d in range(DEV)])
    spectrum = front(charges, cells, splines, counts, forward)
    pencil = lax.all_to_all(spectrum, AXES, split_axis=0, concat_axis=0, tiled=True)
    mixed = mix(pencil, green, mirror).reshape(DEV, ZD, 2 * NU, WIDE)
    returned = lax.all_to_all(mixed, AXES, split_axis=0, concat_axis=0, tiled=True)
    return back(returned, inverse_x, inverse_y)


def solution(mesh):
    in_specs = (
        P(AXES),
        P(None, AXES),
        P(None, AXES),
        P(AXES),
        P(AXES, None, None, None),
    )
    return jax.shard_map(steps, mesh=mesh, in_specs=in_specs, out_specs=P(AXES, None, None), check_vma=False)
```

```python
import jax
import jax.numpy as jnp
import numpy as np
from jax import lax
from jax.experimental import pallas as pl
from jax.experimental.pallas import tpu as pltpu
from jax.sharding import PartitionSpec as P

NX = 512
NY = 512
NZ = 384
KYB = 4
AXES = ("zg", "xy")
DEV = 128
ZD = 3
NU = NX // DEV
HALF = NY // 2
LANE = 128
WIDE = 3 * LANE
SLOTS = 2048
SPREAD = 8
TILES = SLOTS // LANE
ROWS = ZD * NX * NY // LANE
F32 = jnp.float32
BF16 = jnp.bfloat16


def split(table):
    high = table.astype(BF16)
    return high, (table - high.astype(np.float64)).astype(BF16)


def angles(left, right):
    return (np.outer(left, right) % NX) * (2.0 * np.pi / NX)


def waves():
    device = np.arange(DEV)[:, None]
    offset = np.array([[0, 2, 1, -1], [1, -1, 0, 2]])[device[:, 0] // (DEV // 2)]
    return np.where(offset < 0, -1, device * NU + offset)


def forward_tables():
    y = np.arange(NY)
    v = np.arange(HALF)
    along_y = np.concatenate([np.cos(angles(y, v)), -np.sin(angles(y, v))], axis=1)
    along_y[:, HALF] = np.where(y % 2 == 0, 1.0, -1.0)
    x = np.arange(NX // 2)
    near, far = waves()[: DEV // 2], waves()[DEV // 2 :]
    out = [*split(along_y / 512.0)]
    for wave in (np.concatenate([near[:, :2], far[:, 2:]], axis=1), np.concatenate([far[:, :2], near[:, 2:]], axis=1)):
        a = angles(wave.reshape(-1), x).reshape(DEV // 2, NU, NX // 2)
        used = (wave >= 0)[:, :, None]
        out += split(np.stack([np.cos(a) * used, -np.sin(a) * used], axis=1).reshape(NX, NX // 2))
    return tuple(out)


def inverse_tables():
    wave = waves().reshape(DEV, 1, NU).repeat(2, axis=1).reshape(1, 2 * NX)
    used = jnp.asarray(wave >= 0, F32)
    wave = jnp.asarray(wave, jnp.int32)
    quarter = jnp.tile(jnp.repeat(jnp.arange(2, dtype=jnp.int32), NU), DEV)[None, :] * (NX // 4)
    x = lax.broadcasted_iota(jnp.int32, (NX, 2 * NX), 0)
    step = 2.0 * np.pi / NX
    along_x = jnp.cos(((x * wave + quarter) & (NX - 1)).astype(F32) * step) * used
    row = lax.broadcasted_iota(jnp.int32, (NY, NY), 0)
    y = lax.broadcasted_iota(jnp.int32, (NY, NY), 1)
    phase = (row & (HALF - 1)) * y - jnp.where(row < HALF, 0, NY // 4)
    phase = jnp.where(row == HALF, (y + 1) * (NY // 2), phase)
    along_y = jnp.cos((phase & (NY - 1)).astype(F32) * step) / 512.0
    return along_x.astype(BF16), along_y.astype(BF16)


def in_hbm(*arrays):
    return tuple(pltpu.with_memory_space_constraint(a, pltpu.HBM) for a in arrays)


def dot(a, b):
    return jnp.dot(a, b, preferred_element_type=F32)


def turn(q):
    whole = q.reshape(-1, 2 * NU, q.shape[1])
    real = lax.broadcasted_iota(jnp.int32, whole.shape, 1) < NU
    swapped = pltpu.roll(whole, NU, 1)
    return jnp.where(real, -swapped, swapped).reshape(q.shape)


def front_kernel(
    cells_hbm, splines_hbm, charges_hbm, counts, yh_hbm, yl_hbm, eh_hbm, el_hbm, oh_hbm, ol_hbm, out_hbm, *scratch
):
    bins = scratch[:SPREAD]
    spikes = scratch[8:10]
    lanes, values, dens_hi, dens_lo, fold_hi, fold_lo = scratch[10:16]
    tabs = scratch[16:22]
    out, cells, splines, charges, row_table, row_sem, tab_sem, out_sem, slot_sem = scratch[22:31]
    row_of = scratch[31:]
    slot_copies = [
        pltpu.make_async_copy(s, d, slot_sem.at[i])
        for i, (s, d) in enumerate(((cells_hbm, cells), (splines_hbm, splines), (charges_hbm, charges)))
    ]
    for copy in slot_copies:
        copy.start()
    sources = (yh_hbm, yl_hbm, eh_hbm, el_hbm, oh_hbm, ol_hbm)
    tab_copies = [pltpu.make_async_copy(s, d, tab_sem.at[i]) for i, (s, d) in enumerate(zip(sources, tabs))]
    for copy in tab_copies:
        copy.start()
    zeros = jnp.zeros((256, LANE), F32)

    def clear(i, carry):
        for b in bins:
            b[pl.ds(i * 256, 256), :] = zeros
        return carry

    lax.fori_loop(0, ROWS // 512, clear, 0)
    slot_copies[0].wait()
    for t in range(TILES):
        row_table[t] = lax.shift_right_logical(cells[:, t * LANE : (t + 1) * LANE], 7)
    row_copies = [pltpu.make_async_copy(row_table.at[t], row_of[t], row_sem.at[t]) for t in range(TILES)]
    for copy in row_copies:
        copy.start()
    lax.fori_loop(ROWS // 512, ROWS // 256, clear, 0)
    for copy in slot_copies[1:]:
        copy.wait()
    slot = lax.broadcasted_iota(jnp.int32, (1, SLOTS), 1)
    live = (slot < counts[0]).astype(F32)
    value = splines[...] * (charges[...] * live)
    lane_of = cells[...] & (LANE - 1)
    for t in range(TILES):
        lanes[t] = lane_of[:, t * LANE : (t + 1) * LANE]
        values[t] = value[:, t * LANE : (t + 1) * LANE]
    lane = lax.broadcasted_iota(jnp.int32, (SPREAD, LANE), 1)

    def build(spike, g):
        pick = jnp.full((SPREAD, LANE), g, jnp.int32)
        for t in range(TILES):
            at = jnp.take_along_axis(lanes[t], pick, axis=1)
            amount = jnp.take_along_axis(values[t], pick, axis=1)
            spike[t * SPREAD : (t + 1) * SPREAD, :] = jnp.where(lane == at, amount, 0.0)

    def apply(spike, g):
        for t in range(TILES):
            rows = [row_of[t][k, g] for k in range(SPREAD)]
            sums = [bins[k][pl.ds(rows[k], 1), :] + spike[pl.ds(t * SPREAD + k, 1), :] for k in range(SPREAD)]
            for k in range(SPREAD):
                bins[k][pl.ds(rows[k], 1), :] = sums[k]

    build(spikes[0], 0)
    for copy in row_copies:
        copy.wait()

    def body(h, carry):
        build(spikes[1], 2 * h + 1)
        apply(spikes[0], 2 * h)
        build(spikes[0], jnp.minimum(2 * h + 2, LANE - 1))
        apply(spikes[1], 2 * h + 1)
        return carry

    lax.fori_loop(0, LANE // 2, body, 0)
    for copy in tab_copies:
        copy.wait()
    yh, yl, *along_x = tabs
    first = lax.broadcasted_iota(jnp.int32, (NX, LANE), 1) == 0
    lower = lax.broadcasted_iota(jnp.int32, (NX, LANE), 0) % NU < 2
    row_of_tile = lax.broadcasted_iota(jnp.int32, (DEV // 2, 2 * NU, LANE), 1) % NU

    def plane(z, carry):
        for j in range(NY // LANE):
            for q in range(4):
                at = pl.ds(z * (NX * 4) + q * 512 + j, 128, stride=4)
                total = bins[0][at, :]
                for b in bins[1:]:
                    total = total + b[at, :]
                high = total.astype(BF16)
                dens_hi[q * 128 : (q + 1) * 128, j * LANE : (j + 1) * LANE] = high
                dens_lo[q * 128 : (q + 1) * 128, j * LANE : (j + 1) * LANE] = (total - high.astype(F32)).astype(BF16)
        along = dot(dens_hi[...], yh[...]) + dot(dens_lo[...], yh[...]) + dot(dens_hi[...], yl[...])
        near, far = along[: NX // 2], along[NX // 2 :]
        parts = []
        for h, folded in enumerate((near + far, near - far)):
            high = folded.astype(BF16)
            fold_hi[h] = high
            fold_lo[h] = (folded - high.astype(F32)).astype(BF16)
            tab_hi, tab_lo = along_x[2 * h], along_x[2 * h + 1]
            p, q = (
                dot(tab_hi[...], fold_hi[h, :, c]) + dot(tab_hi[...], fold_lo[h, :, c]) + dot(tab_lo[...], fold_hi[h, :, c])
                for c in (slice(0, HALF), slice(HALF, NY))
            )
            q = turn(q)
            p0, p1, q0, q1 = p[:, :LANE], p[:, LANE:], q[:, :LANE], q[:, LANE:]
            minus0 = jnp.where(first, 0.0, p0) - q0
            minus1 = p1 - q1
            parts.append(
                (
                    p0 + jnp.where(first, 0.0, q0),
                    p1 + q1,
                    jnp.where(first, minus1, minus0),
                    jnp.where(first, minus0, minus1),
                )
            )
        near = [jnp.where(lower, even, odd) for even, odd in zip(*parts)]
        far = [jnp.where(lower, odd, even) for even, odd in zip(*parts)]
        for side, (groups, spare) in enumerate(((near, 3), (far, 1))):
            shape = (DEV // 2, 2 * NU, LANE)
            last = groups[3].reshape(shape)
            for j in range(3):
                moved = pltpu.roll(last, (spare - (j ^ 2 * side)) % 8, 1)
                out[z, side * (DEV // 2) : (side + 1) * (DEV // 2), :, j * LANE : (j + 1) * LANE] = jnp.where(
                    row_of_tile == spare, moved, groups[j].reshape(shape)
                ).astype(BF16)
        pltpu.make_async_copy(out.at[z], out_hbm.at[:, z], out_sem.at[z]).start()
        return carry

    lax.fori_loop(0, ZD, plane, 0)
    for z in range(ZD):
        pltpu.make_async_copy(out.at[z], out_hbm.at[:, z], out_sem.at[z]).wait()


def front(charges, cells, splines, counts, tabs):
    smem = pl.BlockSpec(memory_space=pltpu.SMEM)
    hbm = pl.BlockSpec(memory_space=pltpu.HBM)
    return pl.pallas_call(
        front_kernel,
        out_shape=pltpu.HBM((DEV, ZD, 2 * NU, WIDE), BF16),
        in_specs=[hbm] * 3 + [smem] + [hbm] * 6,
        out_specs=hbm,
        scratch_shapes=[pltpu.VMEM((ROWS, LANE), F32)] * SPREAD
        + [pltpu.VMEM((LANE, LANE), F32)] * 2
        + [pltpu.VMEM((TILES, SPREAD, LANE), jnp.int32), pltpu.VMEM((TILES, SPREAD, LANE), F32)]
        + [pltpu.VMEM((NX, NY), BF16)] * 2
        + [pltpu.VMEM((2, NX // 2, NY), BF16)] * 2
        + [pltpu.VMEM(t.shape, BF16) for t in tabs]
        + [pltpu.VMEM((ZD, DEV, 2 * NU, WIDE), BF16)]
        + [pltpu.VMEM((SPREAD, SLOTS), jnp.int32), pltpu.VMEM((SPREAD, SLOTS), F32), pltpu.VMEM((1, SLOTS), F32)]
        + [pltpu.VMEM((TILES, SPREAD, LANE), jnp.int32)]
        + [pltpu.SemaphoreType.DMA((n,)) for n in (TILES, 6, ZD, 3)]
        + [pltpu.SMEM((SPREAD, LANE), jnp.int32)] * TILES,
        compiler_params=pltpu.CompilerParams(vmem_limit_bytes=44 << 20),
        name="front",
    )(*in_hbm(cells, splines, charges.reshape(1, SLOTS)), counts, *in_hbm(*tabs))


WAVE = (0, 2, 1)
BLOCK = (0, 1, 3, 2)
MIRROR = (3, 2, 0, 1)
SWAP = (1, 3, 0, 2)
PART = NZ // 2


def green_kernel(far, spectrum, green_hbm, mirror_hbm, out_hbm, green, out, sums, swapped, green_sem, out_sem, *rhs):
    sources = [green_hbm.at[w] for w in WAVE] + [mirror_hbm]
    fetches = [pltpu.make_async_copy(s, green.at[i], green_sem.at[i]) for i, s in enumerate(sources)]
    for fetch in fetches:
        fetch.start()
    at = [jnp.bitwise_xor(row, 2 * far[0]) for row in range(NU)]
    to = lax.broadcasted_iota(jnp.int32, (256, 256), 0)
    of = lax.broadcasted_iota(jnp.int32, (256, 256), 1)
    wanted = (to % 32) * (2 * NU) + jnp.bitwise_xor(to // 32, 2 * far[0])
    regroup = jnp.where(of == wanted, 1.0, 0.0).astype(BF16)
    for block in range(NZ // 32):
        planes = slice(block * 32, (block + 1) * 32)
        values = dot(regroup, spectrum[planes].reshape(256, WIDE)).astype(BF16)
        for c in range(2):
            for row in range(NU):
                start = (c * NU + row) * 32
                for j in range(3):
                    to, group = (rhs[row], j) if row < 3 else (rhs[j], 3)
                    to[group, planes, c * LANE : (c + 1) * LANE] = values[start : start + 32, j * LANE : (j + 1) * LANE]
    first = lax.broadcasted_iota(jnp.int32, (NZ, 2 * LANE), 1) % LANE == 0
    for j in range(KYB):
        swapped[j] = jnp.where(first, rhs[2][SWAP[j]], rhs[2][j])
    first = first[:PART]
    sends = []
    for part in range(2):
        planes = slice(part * PART, (part + 1) * PART)
        for row in range(3):
            if part == 0:
                fetches[row].wait()
            m = [dot(green[row, BLOCK[j], planes, :], rhs[row][j]) for j in range(KYB)]
            if row == 2:
                if part == 0:
                    fetches[3].wait()
                other = [dot(green[3, MIRROR[j], planes, :], swapped[j]) for j in range(KYB)]
                m = [m[j] + jnp.where(first, other[SWAP.index(j)], other[j]) for j in range(KYB)]
            s2 = jnp.where(first, m[3], m[2])
            s3 = jnp.where(first, m[2], m[3])
            t0 = m[0] + jnp.where(first, 0.0, s2)
            d0 = jnp.where(first, 0.0, m[0]) - s2
            t1 = m[1] + s3
            d1 = m[1] - s3
            groups = (
                (t0[:, :LANE], t0[:, LANE:]),
                (t1[:, :LANE], t1[:, LANE:]),
                (-d0[:, LANE:], d0[:, :LANE]),
                (-d1[:, LANE:], d1[:, :LANE]),
            )
            for j, group in enumerate(groups):
                for c in range(2):
                    to, slot = (j, row) if j < 3 else (row, 3)
                    sums[to, pl.ds(c * NU + at[slot], PART, stride=2 * NU), :] = group[c]
        for j in range(3):
            out[planes, :, j * LANE : (j + 1) * LANE] = sums[j].astype(BF16).reshape(PART, 2 * NU, LANE)
        send = pltpu.make_async_copy(out.at[planes], out_hbm.at[planes], out_sem.at[part])
        send.start()
        sends.append(send)
    for send in sends:
        send.wait()


def mix(pencil, green, mirror):
    vmem = pl.BlockSpec(memory_space=pltpu.VMEM)
    hbm = pl.BlockSpec(memory_space=pltpu.HBM)
    return pl.pallas_call(
        green_kernel,
        out_shape=pltpu.HBM((NZ, 2 * NU, WIDE), BF16),
        in_specs=[pl.BlockSpec(memory_space=pltpu.SMEM), vmem, hbm, hbm],
        out_specs=hbm,
        compiler_params=pltpu.CompilerParams(vmem_limit_bytes=36 << 20),
        scratch_shapes=[
            pltpu.VMEM((NU, KYB, NZ, NZ), BF16),
            pltpu.VMEM((NZ, 2 * NU, WIDE), BF16),
            pltpu.VMEM((3, PART * 2 * NU, LANE), F32),
            pltpu.VMEM((KYB, NZ, 2 * LANE), BF16),
            pltpu.SemaphoreType.DMA((NU,)),
            pltpu.SemaphoreType.DMA((2,)),
        ]
        + [pltpu.VMEM((KYB, NZ, 2 * LANE), BF16)] * 3,
        name="mix",
    )(lax.axis_index("zg").astype(jnp.int32).reshape(1), pencil.reshape(NZ, 2 * NU, WIDE), *in_hbm(green, mirror))


def back_kernel(mixed, x_hbm, y_hbm, out_hbm, along_x, along_y, out, rest, tab_sem, out_sem):
    fetches = [
        pltpu.make_async_copy(x_hbm.at[pl.ds(0, HALF)], along_x.at[pl.ds(0, HALF)], tab_sem.at[0]),
        pltpu.make_async_copy(y_hbm, along_y, tab_sem.at[1]),
        pltpu.make_async_copy(x_hbm.at[pl.ds(HALF, HALF)], along_x.at[pl.ds(HALF, HALF)], tab_sem.at[2]),
    ]
    for fetch in fetches:
        fetch.start()
    row_of_tile = lax.broadcasted_iota(jnp.int32, (DEV // 2, 2 * NU, LANE), 1) % NU
    sends = []
    for z in range(ZD):
        for side in range(2):
            devices = slice(side * (DEV // 2), (side + 1) * (DEV // 2))
            spare = 3 - 2 * side
            last = None
            for j in range(3):
                group = mixed[devices, z, :, j * LANE : (j + 1) * LANE].astype(F32)
                moved = pltpu.roll(group, ((j ^ 2 * side) - spare) % 8, 1)
                last = moved if last is None else jnp.where(row_of_tile == (j ^ 2 * side), moved, last)
            rest[devices, :, LANE:] = last.astype(BF16)
        rest[:, :, :LANE] = mixed[:, z, :, 2 * LANE :]
        for h in range(2):
            rows = pl.ds(h * HALF, HALF)
            if z == 0:
                fetches[2 * h].wait()
            front = dot(along_x[rows, :], mixed[:, z, :, : 2 * LANE].reshape(2 * NX, 2 * LANE)).astype(BF16)
            tail = dot(along_x[rows, :], rest[...].reshape(2 * NX, 2 * LANE)).astype(BF16)
            if z == 0 and h == 0:
                fetches[1].wait()
            out[z, rows, :] = dot(front, along_y[: 2 * LANE, :]) + dot(tail, along_y[2 * LANE :, :])
            send = pltpu.make_async_copy(out.at[z, rows], out_hbm.at[z, rows], out_sem.at[2 * z + h])
            send.start()
            sends.append(send)
    for send in sends:
        send.wait()


def back(returned, inverse_x, inverse_y):
    vmem = pl.BlockSpec(memory_space=pltpu.VMEM)
    hbm = pl.BlockSpec(memory_space=pltpu.HBM)
    return pl.pallas_call(
        back_kernel,
        out_shape=jax.ShapeDtypeStruct((ZD, NX, NY), F32),
        in_specs=[vmem, hbm, hbm],
        out_specs=hbm,
        compiler_params=pltpu.CompilerParams(vmem_limit_bytes=24 << 20),
        scratch_shapes=[
            pltpu.VMEM((NX, 2 * NX), BF16),
            pltpu.VMEM((NY, NY), BF16),
            pltpu.VMEM((ZD, NX, NY), F32),
            pltpu.VMEM((DEV, 2 * NU, 2 * LANE), BF16),
            pltpu.SemaphoreType.DMA((3,)),
            pltpu.SemaphoreType.DMA((2 * ZD,)),
        ],
        name="back",
    )(returned, *in_hbm(inverse_x, inverse_y))


def steps(charges, cells, splines, counts, green):
    forward = tuple(jnp.asarray(t) for t in forward_tables())
    inverse_x, inverse_y = inverse_tables()
    mirror = lax.ppermute(green[NU - 1], AXES, [(d, DEV - 1 - d) for d in range(DEV)])
    spectrum = front(charges, cells, splines, counts, forward)
    pencil = lax.all_to_all(spectrum, AXES, split_axis=0, concat_axis=0, tiled=True)
    mixed = mix(pencil, green, mirror).reshape(DEV, ZD, 2 * NU, WIDE)
    returned = lax.all_to_all(mixed, AXES, split_axis=0, concat_axis=0, tiled=True)
    return back(returned, inverse_x, inverse_y)


def solution(mesh):
    in_specs = (
        P(AXES),
        P(None, AXES),
        P(None, AXES),
        P(AXES),
        P(AXES, None, None, None),
    )
    return jax.shard_map(steps, mesh=mesh, in_specs=in_specs, out_specs=P(AXES, None, None), check_vma=False)
```

```python
import jax
import jax.numpy as jnp
import numpy as np
from jax import lax
from jax.experimental import pallas as pl
from jax.experimental.pallas import tpu as pltpu
from jax.sharding import PartitionSpec as P

NX = 512
NY = 512
NZ = 384
KYB = 4
AXES = ("zg", "xy")
DEV = 128
ZD = 3
NU = NX // DEV
HALF = NY // 2
LANE = 128
WIDE = 3 * LANE
SLOTS = 2048
SPREAD = 8
TILES = SLOTS // LANE
ROWS = ZD * NX * NY // LANE
F32 = jnp.float32
BF16 = jnp.bfloat16


def split(table):
    high = table.astype(BF16)
    return high, (table - high.astype(np.float64)).astype(BF16)


def angles(left, right):
    return (np.outer(left, right) % NX) * (2.0 * np.pi / NX)


def waves():
    device = np.arange(DEV)[:, None]
    offset = np.array([[0, 2, 1, -1], [1, -1, 0, 2]])[device[:, 0] // (DEV // 2)]
    return np.where(offset < 0, -1, device * NU + offset)


def forward_tables():
    y = np.arange(NY)
    v = np.arange(HALF)
    along_y = np.concatenate([np.cos(angles(y, v)), -np.sin(angles(y, v))], axis=1)
    along_y[:, HALF] = np.where(y % 2 == 0, 1.0, -1.0)
    x = np.arange(NX // 2)
    near, far = waves()[: DEV // 2], waves()[DEV // 2 :]
    out = [*split(along_y / 512.0)]
    for wave in (np.concatenate([near[:, :2], far[:, 2:]], axis=1), np.concatenate([far[:, :2], near[:, 2:]], axis=1)):
        a = angles(wave.reshape(-1), x).reshape(DEV // 2, NU, NX // 2)
        used = (wave >= 0)[:, :, None]
        out += split(np.stack([np.cos(a) * used, -np.sin(a) * used], axis=1).reshape(NX, NX // 2))
    return tuple(out)


def inverse_table():
    wave = waves()[:, None, :]
    a = angles(np.arange(NX // 2), wave.reshape(-1)).reshape(NX // 2, DEV, 1, NU)
    table = np.concatenate([np.cos(a), -np.sin(a)], axis=2) * (wave >= 0)
    return table.reshape(NX // 2, 2 * NX).astype(BF16)


def in_hbm(*arrays):
    return tuple(pltpu.with_memory_space_constraint(a, pltpu.HBM) for a in arrays)


def dot(a, b):
    return jnp.dot(a, b, preferred_element_type=F32)


def dot_nt(a, b):
    return lax.dot_general(a, b, (((1,), (1,)), ((), ())), preferred_element_type=F32)


def turn(q):
    whole = q.reshape(-1, 2 * NU, q.shape[1])
    real = lax.broadcasted_iota(jnp.int32, whole.shape, 1) < NU
    swapped = pltpu.roll(whole, NU, 1)
    return jnp.where(real, -swapped, swapped).reshape(q.shape)


def front_kernel(
    rows_hbm, cells_hbm, splines_hbm, charges_hbm, counts, yh_hbm, yl_hbm, eh_hbm, el_hbm, oh_hbm, ol_hbm, out_hbm, *scratch
):
    bins = scratch[:SPREAD]
    spikes = scratch[8:10]
    lanes, values, dens_hi, dens_lo, fold_hi, fold_lo = scratch[10:16]
    tabs = scratch[16:22]
    out, cells, splines, charges, row_sem, tab_sem, out_sem, slot_sem = scratch[22:30]
    row_of = scratch[30:]
    slot_copies = [
        pltpu.make_async_copy(s, d, slot_sem.at[i])
        for i, (s, d) in enumerate(((cells_hbm, cells), (splines_hbm, splines), (charges_hbm, charges)))
    ]
    for copy in slot_copies:
        copy.start()
    row_copies = [
        pltpu.make_async_copy(rows_hbm.at[pl.ds(t * 1024, 1024)], row_of[t], row_sem.at[t]) for t in range(TILES)
    ]
    for copy in row_copies:
        copy.start()
    sources = (yh_hbm, yl_hbm, eh_hbm, el_hbm, oh_hbm, ol_hbm)
    tab_copies = [pltpu.make_async_copy(s, d, tab_sem.at[i]) for i, (s, d) in enumerate(zip(sources, tabs))]
    for copy in tab_copies:
        copy.start()
    zeros = jnp.zeros((256, LANE), F32)

    def clear(i, carry):
        for b in bins:
            b[pl.ds(i * 256, 256), :] = zeros
        return carry

    lax.fori_loop(0, ROWS // 256, clear, 0)
    for copy in slot_copies:
        copy.wait()
    slot = lax.broadcasted_iota(jnp.int32, (1, SLOTS), 1)
    live = (slot < counts[0]).astype(F32)
    value = splines[...] * (charges[...] * live)
    lane_of = cells[...] & (LANE - 1)
    for t in range(TILES):
        lanes[t] = lane_of[:, t * LANE : (t + 1) * LANE]
        values[t] = value[:, t * LANE : (t + 1) * LANE]
    lane = lax.broadcasted_iota(jnp.int32, (SPREAD, LANE), 1)

    def build(spike, g):
        pick = jnp.full((SPREAD, LANE), g, jnp.int32)
        for t in range(TILES):
            at = jnp.take_along_axis(lanes[t], pick, axis=1)
            amount = jnp.take_along_axis(values[t], pick, axis=1)
            spike[t * SPREAD : (t + 1) * SPREAD, :] = jnp.where(lane == at, amount, 0.0)

    def apply(spike, g):
        for t in range(TILES):
            rows = [row_of[t][g + k * LANE] for k in range(SPREAD)]
            sums = [bins[k][pl.ds(rows[k], 1), :] + spike[pl.ds(t * SPREAD + k, 1), :] for k in range(SPREAD)]
            for k in range(SPREAD):
                bins[k][pl.ds(rows[k], 1), :] = sums[k]

    build(spikes[0], 0)
    for copy in row_copies:
        copy.wait()

    def body(h, carry):
        build(spikes[1], 2 * h + 1)
        apply(spikes[0], 2 * h)
        build(spikes[0], jnp.minimum(2 * h + 2, LANE - 1))
        apply(spikes[1], 2 * h + 1)
        return carry

    lax.fori_loop(0, LANE // 2, body, 0)
    for copy in tab_copies:
        copy.wait()
    yh, yl, *along_x = tabs
    first = lax.broadcasted_iota(jnp.int32, (NX, LANE), 1) == 0
    lower = lax.broadcasted_iota(jnp.int32, (NX, LANE), 0) % NU < 2
    row_of_tile = lax.broadcasted_iota(jnp.int32, (DEV // 2, 2 * NU, LANE), 1) % NU

    def plane(z, carry):
        for j in range(NY // LANE):
            for q in range(4):
                at = pl.ds(z * (NX * 4) + q * 512 + j, 128, stride=4)
                total = bins[0][at, :]
                for b in bins[1:]:
                    total = total + b[at, :]
                high = total.astype(BF16)
                dens_hi[q * 128 : (q + 1) * 128, j * LANE : (j + 1) * LANE] = high
                dens_lo[q * 128 : (q + 1) * 128, j * LANE : (j + 1) * LANE] = (total - high.astype(F32)).astype(BF16)
        along = dot(dens_hi[...], yh[...]) + dot(dens_lo[...], yh[...]) + dot(dens_hi[...], yl[...])
        near, far = along[: NX // 2], along[NX // 2 :]
        parts = []
        for h, folded in enumerate((near + far, near - far)):
            high = folded.astype(BF16)
            fold_hi[h] = high
            fold_lo[h] = (folded - high.astype(F32)).astype(BF16)
            tab_hi, tab_lo = along_x[2 * h], along_x[2 * h + 1]
            p, q = (
                dot(tab_hi[...], fold_hi[h, :, c]) + dot(tab_hi[...], fold_lo[h, :, c]) + dot(tab_lo[...], fold_hi[h, :, c])
                for c in (slice(0, HALF), slice(HALF, NY))
            )
            q = turn(q)
            p0, p1, q0, q1 = p[:, :LANE], p[:, LANE:], q[:, :LANE], q[:, LANE:]
            minus0 = jnp.where(first, 0.0, p0) - q0
            minus1 = p1 - q1
            parts.append(
                (
                    p0 + jnp.where(first, 0.0, q0),
                    p1 + q1,
                    jnp.where(first, minus1, minus0),
                    jnp.where(first, minus0, minus1),
                )
            )
        near = [jnp.where(lower, even, odd) for even, odd in zip(*parts)]
        far = [jnp.where(lower, odd, even) for even, odd in zip(*parts)]
        for side, (groups, spare) in enumerate(((near, 3), (far, 1))):
            shape = (DEV // 2, 2 * NU, LANE)
            last = groups[3].reshape(shape)
            for j in range(3):
                moved = pltpu.roll(last, (spare - (j ^ 2 * side)) % 8, 1)
                out[z, side * (DEV // 2) : (side + 1) * (DEV // 2), :, j * LANE : (j + 1) * LANE] = jnp.where(
                    row_of_tile == spare, moved, groups[j].reshape(shape)
                ).astype(BF16)
        pltpu.make_async_copy(out.at[z], out_hbm.at[:, z], out_sem.at[z]).start()
        return carry

    lax.fori_loop(0, ZD, plane, 0)
    for z in range(ZD):
        pltpu.make_async_copy(out.at[z], out_hbm.at[:, z], out_sem.at[z]).wait()


def front(charges, cells, splines, counts, tabs):
    smem = pl.BlockSpec(memory_space=pltpu.SMEM)
    hbm = pl.BlockSpec(memory_space=pltpu.HBM)
    rows = lax.shift_right_logical(cells, 7).reshape(SPREAD, TILES, LANE).transpose(1, 0, 2).reshape(-1)
    return pl.pallas_call(
        front_kernel,
        out_shape=pltpu.HBM((DEV, ZD, 2 * NU, WIDE), BF16),
        in_specs=[hbm] * 4 + [smem] + [hbm] * 6,
        out_specs=hbm,
        scratch_shapes=[pltpu.VMEM((ROWS, LANE), F32)] * SPREAD
        + [pltpu.VMEM((LANE, LANE), F32)] * 2
        + [pltpu.VMEM((TILES, SPREAD, LANE), jnp.int32), pltpu.VMEM((TILES, SPREAD, LANE), F32)]
        + [pltpu.VMEM((NX, NY), BF16)] * 2
        + [pltpu.VMEM((2, NX // 2, NY), BF16)] * 2
        + [pltpu.VMEM(t.shape, BF16) for t in tabs]
        + [pltpu.VMEM((ZD, DEV, 2 * NU, WIDE), BF16)]
        + [pltpu.VMEM((SPREAD, SLOTS), jnp.int32), pltpu.VMEM((SPREAD, SLOTS), F32), pltpu.VMEM((1, SLOTS), F32)]
        + [pltpu.SemaphoreType.DMA((n,)) for n in (TILES, 6, ZD, 3)]
        + [pltpu.SMEM((SPREAD * LANE,), jnp.int32)] * TILES,
        compiler_params=pltpu.CompilerParams(vmem_limit_bytes=44 << 20),
        name="front",
    )(*in_hbm(rows, cells, splines, charges.reshape(1, SLOTS)), counts, *in_hbm(*tabs))


WAVE = (0, 2, 1)
BLOCK = (0, 1, 3, 2)
MIRROR = (3, 2, 0, 1)
SWAP = (1, 3, 0, 2)
PART = NZ // 2


def green_kernel(far, spectrum, green_hbm, mirror_hbm, out, green, flat, sums, swapped, green_sem, *rhs):
    sources = [green_hbm.at[w] for w in WAVE] + [mirror_hbm]
    fetches = [pltpu.make_async_copy(s, green.at[i], green_sem.at[i]) for i, s in enumerate(sources)]
    for fetch in fetches:
        fetch.start()
    at = [jnp.bitwise_xor(row, 2 * far[0]) for row in range(NU)]
    for j in range(3):
        flat[...] = spectrum[:, :, j * LANE : (j + 1) * LANE].astype(F32).reshape(NZ * 2 * NU, LANE)
        for row in range(NU):
            for c in range(2):
                values = flat[pl.ds(c * NU + at[row], NZ, stride=2 * NU), :].astype(BF16)
                to, group = (rhs[row], j) if row < 3 else (rhs[j], 3)
                to[group, :, c * LANE : (c + 1) * LANE] = values
    first = lax.broadcasted_iota(jnp.int32, (NZ, 2 * LANE), 1) % LANE == 0
    for j in range(KYB):
        swapped[j] = jnp.where(first, rhs[2][SWAP[j]], rhs[2][j])
    first = first[:PART]
    for part in range(2):
        planes = slice(part * PART, (part + 1) * PART)
        for row in range(3):
            if part == 0:
                fetches[row].wait()
            m = [dot(green[row, BLOCK[j], planes, :], rhs[row][j]) for j in range(KYB)]
            if row == 2:
                if part == 0:
                    fetches[3].wait()
                other = [dot(green[3, MIRROR[j], planes, :], swapped[j]) for j in range(KYB)]
                m = [m[j] + jnp.where(first, other[SWAP.index(j)], other[j]) for j in range(KYB)]
            s2 = jnp.where(first, m[3], m[2])
            s3 = jnp.where(first, m[2], m[3])
            t0 = m[0] + jnp.where(first, 0.0, s2)
            d0 = jnp.where(first, 0.0, m[0]) - s2
            t1 = m[1] + s3
            d1 = m[1] - s3
            groups = (
                (t0[:, :LANE], t0[:, LANE:]),
                (t1[:, :LANE], t1[:, LANE:]),
                (d0[:, LANE:], -d0[:, :LANE]),
                (d1[:, LANE:], -d1[:, :LANE]),
            )
            for j, group in enumerate(groups):
                for c in range(2):
                    to, slot = (j, row) if j < 3 else (row, 3)
                    sums[to, pl.ds(c * NU + at[slot], PART, stride=2 * NU), :] = group[c]
        for j in range(3):
            out[planes, :, j * LANE : (j + 1) * LANE] = sums[j].astype(BF16).reshape(PART, 2 * NU, LANE)


def mix(pencil, green, mirror):
    vmem = pl.BlockSpec(memory_space=pltpu.VMEM)
    hbm = pl.BlockSpec(memory_space=pltpu.HBM)
    return pl.pallas_call(
        green_kernel,
        out_shape=pltpu.VMEM((NZ, 2 * NU, WIDE), BF16),
        in_specs=[pl.BlockSpec(memory_space=pltpu.SMEM), vmem, hbm, hbm],
        out_specs=vmem,
        compiler_params=pltpu.CompilerParams(vmem_limit_bytes=36 << 20),
        scratch_shapes=[
            pltpu.VMEM((NU, KYB, NZ, NZ), BF16),
            pltpu.VMEM((NZ * 2 * NU, LANE), F32),
            pltpu.VMEM((3, PART * 2 * NU, LANE), F32),
            pltpu.VMEM((KYB, NZ, 2 * LANE), BF16),
            pltpu.SemaphoreType.DMA((NU,)),
        ]
        + [pltpu.VMEM((KYB, NZ, 2 * LANE), BF16)] * 3,
        name="mix",
    )(lax.axis_index("zg").astype(jnp.int32).reshape(1), pencil.reshape(NZ, 2 * NU, WIDE), *in_hbm(green, mirror))


def back_kernel(mixed, x_hbm, y_hbm, out_hbm, along_x, along_y, out, rest, tab_sem, out_sem):
    fetches = [
        pltpu.make_async_copy(x_hbm, along_x.at[pl.ds(0, HALF)], tab_sem.at[0]),
        pltpu.make_async_copy(y_hbm, along_y, tab_sem.at[1]),
    ]
    for fetch in fetches:
        fetch.start()
    row_of_tile = lax.broadcasted_iota(jnp.int32, (DEV // 2, 2 * NU, LANE), 1) % NU
    sends = []
    for z in range(ZD):
        for side in range(2):
            devices = slice(side * (DEV // 2), (side + 1) * (DEV // 2))
            spare = 3 - 2 * side
            last = None
            for j in range(3):
                group = mixed[devices, z, :, j * LANE : (j + 1) * LANE].astype(F32)
                moved = pltpu.roll(group, ((j ^ 2 * side) - spare) % 8, 1)
                last = moved if last is None else jnp.where(row_of_tile == (j ^ 2 * side), moved, last)
            rest[devices, :, LANE:] = last.astype(BF16)
        rest[:, :, :LANE] = mixed[:, z, :, 2 * LANE :]
        for h in range(2):
            rows = pl.ds(h * HALF, HALF)
            if z == 0 and h == 0:
                fetches[0].wait()
            elif z == 0:
                place = lax.broadcasted_iota(jnp.int32, (1, 2 * NX), 1)
                sign = jnp.where(place % NU == jnp.where(place < NX, 2, 0), -1.0, 1.0).astype(BF16)
                along_x[HALF:, :] = along_x[:HALF, :] * sign
            front = dot(along_x[rows, :], mixed[:, z, :, : 2 * LANE].reshape(2 * NX, 2 * LANE)).astype(BF16)
            tail = dot(along_x[rows, :], rest[...].reshape(2 * NX, 2 * LANE)).astype(BF16)
            if z == 0 and h == 0:
                fetches[1].wait()
            out[z, rows, :] = dot_nt(front, along_y[:, : 2 * LANE]) + dot_nt(tail, along_y[:, 2 * LANE :])
            send = pltpu.make_async_copy(out.at[z, rows], out_hbm.at[z, rows], out_sem.at[2 * z + h])
            send.start()
            sends.append(send)
    for send in sends:
        send.wait()


def back(returned, inverse_x, inverse_y):
    vmem = pl.BlockSpec(memory_space=pltpu.VMEM)
    hbm = pl.BlockSpec(memory_space=pltpu.HBM)
    return pl.pallas_call(
        back_kernel,
        out_shape=jax.ShapeDtypeStruct((ZD, NX, NY), F32),
        in_specs=[vmem, hbm, hbm],
        out_specs=hbm,
        compiler_params=pltpu.CompilerParams(vmem_limit_bytes=24 << 20),
        scratch_shapes=[
            pltpu.VMEM((NX, 2 * NX), BF16),
            pltpu.VMEM((NY, NY), BF16),
            pltpu.VMEM((ZD, NX, NY), F32),
            pltpu.VMEM((DEV, 2 * NU, 2 * LANE), BF16),
            pltpu.SemaphoreType.DMA((2,)),
            pltpu.SemaphoreType.DMA((2 * ZD,)),
        ],
        name="back",
    )(returned, *in_hbm(inverse_x, inverse_y))


def steps(charges, cells, splines, counts, green):
    forward = tuple(jnp.asarray(t) for t in forward_tables())
    mirror = lax.ppermute(green[NU - 1], AXES, [(d, DEV - 1 - d) for d in range(DEV)])
    spectrum = front(charges, cells, splines, counts, forward)
    pencil = lax.all_to_all(spectrum, AXES, split_axis=0, concat_axis=0, tiled=True)
    mixed = mix(pencil, green, mirror).reshape(DEV, ZD, 2 * NU, WIDE)
    returned = lax.all_to_all(mixed, AXES, split_axis=0, concat_axis=0, tiled=True)
    return back(returned, jnp.asarray(inverse_table()), forward[0])


def solution(mesh):
    in_specs = (
        P(AXES),
        P(None, AXES),
        P(None, AXES),
        P(AXES),
        P(AXES, None, None, None),
    )
    return jax.shard_map(steps, mesh=mesh, in_specs=in_specs, out_specs=P(AXES, None, None), check_vma=False)
```

```python
import jax
import jax.numpy as jnp
import numpy as np
from jax import lax
from jax.experimental import pallas as pl
from jax.experimental.pallas import tpu as pltpu
from jax.sharding import PartitionSpec as P

NX = 512
NY = 512
NZ = 384
KYB = 4
AXES = ("zg", "xy")
DEV = 128
ZD = 3
NU = NX // DEV
HALF = NY // 2
LANE = 128
WIDE = 3 * LANE
SLOTS = 2048
SPREAD = 8
TILES = SLOTS // LANE
ROWS = ZD * NX * NY // LANE
F32 = jnp.float32
BF16 = jnp.bfloat16


def split(table):
    high = table.astype(BF16)
    return high, (table - high.astype(np.float64)).astype(BF16)


def angles(left, right):
    return (np.outer(left, right) % NX) * (2.0 * np.pi / NX)


def waves():
    device = np.arange(DEV)[:, None]
    offset = np.array([[0, 2, 1, -1], [1, -1, 0, 2]])[device[:, 0] // (DEV // 2)]
    return np.where(offset < 0, -1, device * NU + offset)


def forward_tables():
    y = np.arange(NY)
    v = np.arange(HALF)
    along_y = np.concatenate([np.cos(angles(y, v)), -np.sin(angles(y, v))], axis=1)
    along_y[:, HALF] = np.where(y % 2 == 0, 1.0, -1.0)
    x = np.arange(NX // 2)
    near, far = waves()[: DEV // 2], waves()[DEV // 2 :]
    out = [*split(along_y / 512.0)]
    for wave in (np.concatenate([near[:, :2], far[:, 2:]], axis=1), np.concatenate([far[:, :2], near[:, 2:]], axis=1)):
        a = angles(wave.reshape(-1), x).reshape(DEV // 2, NU, NX // 2)
        used = (wave >= 0)[:, :, None]
        out += split(np.stack([np.cos(a) * used, -np.sin(a) * used], axis=1).reshape(NX, NX // 2))
    return tuple(out)


def inverse_table():
    wave = waves()[:, None, :]
    a = angles(np.arange(NX // 2), wave.reshape(-1)).reshape(NX // 2, DEV, 1, NU)
    table = np.concatenate([np.cos(a), -np.sin(a)], axis=2) * (wave >= 0)
    return table.reshape(NX // 2, 2 * NX).astype(BF16)


def in_hbm(*arrays):
    return tuple(pltpu.with_memory_space_constraint(a, pltpu.HBM) for a in arrays)


def dot(a, b):
    return jnp.dot(a, b, preferred_element_type=F32)


def dot_nt(a, b):
    return lax.dot_general(a, b, (((1,), (1,)), ((), ())), preferred_element_type=F32)


def turn(q):
    whole = q.reshape(-1, 2 * NU, q.shape[1])
    real = lax.broadcasted_iota(jnp.int32, whole.shape, 1) < NU
    swapped = pltpu.roll(whole, NU, 1)
    return jnp.where(real, -swapped, swapped).reshape(q.shape)


def front_kernel(
    rows_hbm, cells_hbm, splines_hbm, charges_hbm, counts, yh_hbm, yl_hbm, eh_hbm, el_hbm, oh_hbm, ol_hbm, out_hbm, *scratch
):
    bins = scratch[:SPREAD]
    spikes = scratch[8:10]
    lanes, values, dens_hi, dens_lo, fold_hi, fold_lo = scratch[10:16]
    tabs = scratch[16:22]
    out, cells, splines, charges, row_sem, tab_sem, out_sem, slot_sem = scratch[22:30]
    row_of = scratch[30:]
    slot_copies = [
        pltpu.make_async_copy(s, d, slot_sem.at[i])
        for i, (s, d) in enumerate(((cells_hbm, cells), (splines_hbm, splines), (charges_hbm, charges)))
    ]
    for copy in slot_copies:
        copy.start()
    row_copies = [
        pltpu.make_async_copy(rows_hbm.at[pl.ds(t * 1024, 1024)], row_of[t], row_sem.at[t]) for t in range(TILES)
    ]
    for copy in row_copies:
        copy.start()
    sources = (yh_hbm, yl_hbm, eh_hbm, el_hbm, oh_hbm, ol_hbm)
    tab_copies = [pltpu.make_async_copy(s, d, tab_sem.at[i]) for i, (s, d) in enumerate(zip(sources, tabs))]
    for copy in tab_copies:
        copy.start()
    zeros = jnp.zeros((256, LANE), F32)

    def clear(i, carry):
        for b in bins:
            b[pl.ds(i * 256, 256), :] = zeros
        return carry

    lax.fori_loop(0, ROWS // 256, clear, 0)
    for copy in slot_copies:
        copy.wait()
    slot = lax.broadcasted_iota(jnp.int32, (1, SLOTS), 1)
    live = (slot < counts[0]).astype(F32)
    value = splines[...] * (charges[...] * live)
    lane_of = cells[...] & (LANE - 1)
    for t in range(TILES):
        lanes[t] = lane_of[:, t * LANE : (t + 1) * LANE]
        values[t] = value[:, t * LANE : (t + 1) * LANE]
    lane = lax.broadcasted_iota(jnp.int32, (SPREAD, LANE), 1)

    def build(spike, g):
        pick = jnp.full((SPREAD, LANE), g, jnp.int32)
        for t in range(TILES):
            at = jnp.take_along_axis(lanes[t], pick, axis=1)
            amount = jnp.take_along_axis(values[t], pick, axis=1)
            spike[t * SPREAD : (t + 1) * SPREAD, :] = jnp.where(lane == at, amount, 0.0)

    def apply(spike, g):
        for t in range(TILES):
            rows = [row_of[t][g + k * LANE] for k in range(SPREAD)]
            sums = [bins[k][pl.ds(rows[k], 1), :] + spike[pl.ds(t * SPREAD + k, 1), :] for k in range(SPREAD)]
            for k in range(SPREAD):
                bins[k][pl.ds(rows[k], 1), :] = sums[k]

    build(spikes[0], 0)
    for copy in row_copies:
        copy.wait()

    def body(h, carry):
        build(spikes[1], 2 * h + 1)
        apply(spikes[0], 2 * h)
        build(spikes[0], jnp.minimum(2 * h + 2, LANE - 1))
        apply(spikes[1], 2 * h + 1)
        return carry

    lax.fori_loop(0, LANE // 2, body, 0)
    for copy in tab_copies:
        copy.wait()
    yh, yl, *along_x = tabs
    first = lax.broadcasted_iota(jnp.int32, (NX, LANE), 1) == 0
    lower = lax.broadcasted_iota(jnp.int32, (NX, LANE), 0) % NU < 2
    row_of_tile = lax.broadcasted_iota(jnp.int32, (DEV // 2, 2 * NU, LANE), 1) % NU

    def plane(z, carry):
        for j in range(NY // LANE):
            for q in range(4):
                at = pl.ds(z * (NX * 4) + q * 512 + j, 128, stride=4)
                total = bins[0][at, :]
                for b in bins[1:]:
                    total = total + b[at, :]
                high = total.astype(BF16)
                dens_hi[q * 128 : (q + 1) * 128, j * LANE : (j + 1) * LANE] = high
                dens_lo[q * 128 : (q + 1) * 128, j * LANE : (j + 1) * LANE] = (total - high.astype(F32)).astype(BF16)
        along = dot(dens_hi[...], yh[...]) + dot(dens_lo[...], yh[...]) + dot(dens_hi[...], yl[...])
        near, far = along[: NX // 2], along[NX // 2 :]
        parts = []
        for h, folded in enumerate((near + far, near - far)):
            high = folded.astype(BF16)
            fold_hi[h] = high
            fold_lo[h] = (folded - high.astype(F32)).astype(BF16)
            tab_hi, tab_lo = along_x[2 * h], along_x[2 * h + 1]
            p, q = (
                dot(tab_hi[...], fold_hi[h, :, c]) + dot(tab_hi[...], fold_lo[h, :, c]) + dot(tab_lo[...], fold_hi[h, :, c])
                for c in (slice(0, HALF), slice(HALF, NY))
            )
            q = turn(q)
            p0, p1, q0, q1 = p[:, :LANE], p[:, LANE:], q[:, :LANE], q[:, LANE:]
            minus0 = jnp.where(first, 0.0, p0) - q0
            minus1 = p1 - q1
            parts.append(
                (
                    p0 + jnp.where(first, 0.0, q0),
                    p1 + q1,
                    jnp.where(first, minus1, minus0),
                    jnp.where(first, minus0, minus1),
                )
            )
        near = [jnp.where(lower, even, odd) for even, odd in zip(*parts)]
        far = [jnp.where(lower, odd, even) for even, odd in zip(*parts)]
        for side, (groups, spare) in enumerate(((near, 3), (far, 1))):
            shape = (DEV // 2, 2 * NU, LANE)
            last = groups[3].reshape(shape)
            for j in range(3):
                moved = pltpu.roll(last, (spare - (j ^ 2 * side)) % 8, 1)
                out[z, side * (DEV // 2) : (side + 1) * (DEV // 2), :, j * LANE : (j + 1) * LANE] = jnp.where(
                    row_of_tile == spare, moved, groups[j].reshape(shape)
                ).astype(BF16)
        pltpu.make_async_copy(out.at[z], out_hbm.at[:, z], out_sem.at[z]).start()
        return carry

    lax.fori_loop(0, ZD, plane, 0)
    for z in range(ZD):
        pltpu.make_async_copy(out.at[z], out_hbm.at[:, z], out_sem.at[z]).wait()


def front(charges, cells, splines, counts, tabs):
    smem = pl.BlockSpec(memory_space=pltpu.SMEM)
    hbm = pl.BlockSpec(memory_space=pltpu.HBM)
    rows = lax.shift_right_logical(cells, 7).reshape(SPREAD, TILES, LANE).transpose(1, 0, 2).reshape(-1)
    return pl.pallas_call(
        front_kernel,
        out_shape=pltpu.HBM((DEV, ZD, 2 * NU, WIDE), BF16),
        in_specs=[hbm] * 4 + [smem] + [hbm] * 6,
        out_specs=hbm,
        scratch_shapes=[pltpu.VMEM((ROWS, LANE), F32)] * SPREAD
        + [pltpu.VMEM((LANE, LANE), F32)] * 2
        + [pltpu.VMEM((TILES, SPREAD, LANE), jnp.int32), pltpu.VMEM((TILES, SPREAD, LANE), F32)]
        + [pltpu.VMEM((NX, NY), BF16)] * 2
        + [pltpu.VMEM((2, NX // 2, NY), BF16)] * 2
        + [pltpu.VMEM(t.shape, BF16) for t in tabs]
        + [pltpu.VMEM((ZD, DEV, 2 * NU, WIDE), BF16)]
        + [pltpu.VMEM((SPREAD, SLOTS), jnp.int32), pltpu.VMEM((SPREAD, SLOTS), F32), pltpu.VMEM((1, SLOTS), F32)]
        + [pltpu.SemaphoreType.DMA((n,)) for n in (TILES, 6, ZD, 3)]
        + [pltpu.SMEM((SPREAD * LANE,), jnp.int32)] * TILES,
        compiler_params=pltpu.CompilerParams(vmem_limit_bytes=44 << 20),
        name="front",
    )(*in_hbm(rows, cells, splines, charges.reshape(1, SLOTS)), counts, *in_hbm(*tabs))


WAVE = (0, 2, 1)
BLOCK = (0, 1, 3, 2)
MIRROR = (3, 2, 0, 1)
SWAP = (1, 3, 0, 2)
PART = NZ // 2


def green_kernel(
    far, spectrum, green_hbm, mirror_hbm, x_hbm, y_hbm, out, x_out, y_out, green, flat, sums, swapped, green_sem, *rhs
):
    sources = [green_hbm.at[w] for w in WAVE] + [mirror_hbm]
    fetches = [pltpu.make_async_copy(s, green.at[i], green_sem.at[i]) for i, s in enumerate(sources)]
    fetches.append(pltpu.make_async_copy(x_hbm, x_out, green_sem.at[4]))
    fetches.append(pltpu.make_async_copy(y_hbm, y_out, green_sem.at[5]))
    for fetch in fetches:
        fetch.start()
    at = [jnp.bitwise_xor(row, 2 * far[0]) for row in range(NU)]
    for j in range(3):
        flat[...] = spectrum[:, :, j * LANE : (j + 1) * LANE].astype(F32).reshape(NZ * 2 * NU, LANE)
        for row in range(NU):
            for c in range(2):
                values = flat[pl.ds(c * NU + at[row], NZ, stride=2 * NU), :].astype(BF16)
                to, group = (rhs[row], j) if row < 3 else (rhs[j], 3)
                to[group, :, c * LANE : (c + 1) * LANE] = values
    first = lax.broadcasted_iota(jnp.int32, (NZ, 2 * LANE), 1) % LANE == 0
    for j in range(KYB):
        swapped[j] = jnp.where(first, rhs[2][SWAP[j]], rhs[2][j])
    first = first[:PART]
    for part in range(2):
        planes = slice(part * PART, (part + 1) * PART)
        for row in range(3):
            if part == 0:
                fetches[row].wait()
            m = [dot(green[row, BLOCK[j], planes, :], rhs[row][j]) for j in range(KYB)]
            if row == 2:
                if part == 0:
                    fetches[3].wait()
                other = [dot(green[3, MIRROR[j], planes, :], swapped[j]) for j in range(KYB)]
                m = [m[j] + jnp.where(first, other[SWAP.index(j)], other[j]) for j in range(KYB)]
            s2 = jnp.where(first, m[3], m[2])
            s3 = jnp.where(first, m[2], m[3])
            t0 = m[0] + jnp.where(first, 0.0, s2)
            d0 = jnp.where(first, 0.0, m[0]) - s2
            t1 = m[1] + s3
            d1 = m[1] - s3
            groups = (
                (t0[:, :LANE], t0[:, LANE:]),
                (t1[:, :LANE], t1[:, LANE:]),
                (d0[:, LANE:], -d0[:, :LANE]),
                (d1[:, LANE:], -d1[:, :LANE]),
            )
            for j, group in enumerate(groups):
                for c in range(2):
                    to, slot = (j, row) if j < 3 else (row, 3)
                    sums[to, pl.ds(c * NU + at[slot], PART, stride=2 * NU), :] = group[c]
        for j in range(3):
            out[planes, :, j * LANE : (j + 1) * LANE] = sums[j].astype(BF16).reshape(PART, 2 * NU, LANE)
    for fetch in fetches[4:]:
        fetch.wait()


def mix(pencil, green, mirror, *tabs):
    vmem = pl.BlockSpec(memory_space=pltpu.VMEM)
    hbm = pl.BlockSpec(memory_space=pltpu.HBM)
    return pl.pallas_call(
        green_kernel,
        out_shape=(pltpu.VMEM((NZ, 2 * NU, WIDE), BF16), *(pltpu.VMEM(t.shape, BF16) for t in tabs)),
        in_specs=[pl.BlockSpec(memory_space=pltpu.SMEM), vmem, hbm, hbm, hbm, hbm],
        out_specs=(vmem, vmem, vmem),
        compiler_params=pltpu.CompilerParams(vmem_limit_bytes=36 << 20),
        scratch_shapes=[
            pltpu.VMEM((NU, KYB, NZ, NZ), BF16),
            pltpu.VMEM((NZ * 2 * NU, LANE), F32),
            pltpu.VMEM((3, PART * 2 * NU, LANE), F32),
            pltpu.VMEM((KYB, NZ, 2 * LANE), BF16),
            pltpu.SemaphoreType.DMA((6,)),
        ]
        + [pltpu.VMEM((KYB, NZ, 2 * LANE), BF16)] * 3,
        name="mix",
    )(lax.axis_index("zg").astype(jnp.int32).reshape(1), pencil.reshape(NZ, 2 * NU, WIDE), *in_hbm(green, mirror, *tabs))


def back_kernel(mixed, half_x, along_y, out_hbm, far_x, out, rest, out_sem):
    row_of_tile = lax.broadcasted_iota(jnp.int32, (DEV // 2, 2 * NU, LANE), 1) % NU
    sends = []
    for z in range(ZD):
        for side in range(2):
            devices = slice(side * (DEV // 2), (side + 1) * (DEV // 2))
            spare = 3 - 2 * side
            last = None
            for j in range(3):
                group = mixed[devices, z, :, j * LANE : (j + 1) * LANE].astype(F32)
                moved = pltpu.roll(group, ((j ^ 2 * side) - spare) % 8, 1)
                last = moved if last is None else jnp.where(row_of_tile == (j ^ 2 * side), moved, last)
            rest[devices, :, LANE:] = last.astype(BF16)
        rest[:, :, :LANE] = mixed[:, z, :, 2 * LANE :]
        for h in range(2):
            rows = pl.ds(h * HALF, HALF)
            if z == 0 and h == 1:
                place = lax.broadcasted_iota(jnp.int32, (1, 2 * NX), 1)
                sign = jnp.where(place % NU == jnp.where(place < NX, 2, 0), -1.0, 1.0).astype(BF16)
                far_x[...] = half_x[...] * sign
            along_x = (half_x, far_x)[h]
            front = dot(along_x[...], mixed[:, z, :, : 2 * LANE].reshape(2 * NX, 2 * LANE)).astype(BF16)
            tail = dot(along_x[...], rest[...].reshape(2 * NX, 2 * LANE)).astype(BF16)
            out[z, rows, :] = dot_nt(front, along_y[:, : 2 * LANE]) + dot_nt(tail, along_y[:, 2 * LANE :])
            send = pltpu.make_async_copy(out.at[z, rows], out_hbm.at[z, rows], out_sem.at[2 * z + h])
            send.start()
            sends.append(send)
    for send in sends:
        send.wait()


def back(returned, inverse_x, inverse_y):
    vmem = pl.BlockSpec(memory_space=pltpu.VMEM)
    hbm = pl.BlockSpec(memory_space=pltpu.HBM)
    return pl.pallas_call(
        back_kernel,
        out_shape=jax.ShapeDtypeStruct((ZD, NX, NY), F32),
        in_specs=[vmem, vmem, vmem],
        out_specs=hbm,
        compiler_params=pltpu.CompilerParams(vmem_limit_bytes=24 << 20),
        scratch_shapes=[
            pltpu.VMEM((NX // 2, 2 * NX), BF16),
            pltpu.VMEM((ZD, NX, NY), F32),
            pltpu.VMEM((DEV, 2 * NU, 2 * LANE), BF16),
            pltpu.SemaphoreType.DMA((2 * ZD,)),
        ],
        name="back",
    )(returned, inverse_x, inverse_y)


def steps(charges, cells, splines, counts, green):
    forward = tuple(jnp.asarray(t) for t in forward_tables())
    mirror = lax.ppermute(green[NU - 1], AXES, [(d, DEV - 1 - d) for d in range(DEV)])
    spectrum = front(charges, cells, splines, counts, forward)
    pencil = lax.all_to_all(spectrum, AXES, split_axis=0, concat_axis=0, tiled=True)
    mixed, *along = mix(pencil, green, mirror, jnp.asarray(inverse_table()), forward[0])
    mixed = mixed.reshape(DEV, ZD, 2 * NU, WIDE)
    returned = lax.all_to_all(mixed, AXES, split_axis=0, concat_axis=0, tiled=True)
    return back(returned, *along)


def solution(mesh):
    in_specs = (
        P(AXES),
        P(None, AXES),
        P(None, AXES),
        P(AXES),
        P(AXES, None, None, None),
    )
    return jax.shard_map(steps, mesh=mesh, in_specs=in_specs, out_specs=P(AXES, None, None), check_vma=False)
```

```python
import jax
import jax.numpy as jnp
import numpy as np
from jax import lax
from jax.experimental import pallas as pl
from jax.experimental.pallas import tpu as pltpu
from jax.sharding import PartitionSpec as P

NX = 512
NY = 512
NZ = 384
KYB = 4
AXES = ("zg", "xy")
DEV = 128
ZD = 3
NU = NX // DEV
HALF = NY // 2
LANE = 128
WIDE = 3 * LANE
SLOTS = 2048
SPREAD = 8
TILES = SLOTS // LANE
ROWS = ZD * NX * NY // LANE
F32 = jnp.float32
BF16 = jnp.bfloat16


def split(table):
    high = table.astype(BF16)
    return high, (table - high.astype(np.float64)).astype(BF16)


def angles(left, right):
    return (np.outer(left, right) % NX) * (2.0 * np.pi / NX)


def waves():
    device = np.arange(DEV)[:, None]
    offset = np.array([[0, 2, 1, -1], [1, -1, 0, 2]])[device[:, 0] // (DEV // 2)]
    return np.where(offset < 0, -1, device * NU + offset)


def forward_tables():
    y = np.arange(NY)
    v = np.arange(HALF)
    along_y = np.concatenate([np.cos(angles(y, v)), -np.sin(angles(y, v))], axis=1)
    along_y[:, HALF] = np.where(y % 2 == 0, 1.0, -1.0)
    x = np.arange(NX // 2)
    near, far = waves()[: DEV // 2], waves()[DEV // 2 :]
    out = [*split(along_y / 512.0)]
    for wave in (np.concatenate([near[:, :2], far[:, 2:]], axis=1), np.concatenate([far[:, :2], near[:, 2:]], axis=1)):
        a = angles(wave.reshape(-1), x).reshape(DEV // 2, NU, NX // 2)
        used = (wave >= 0)[:, :, None]
        out += split(np.stack([np.cos(a) * used, -np.sin(a) * used], axis=1).reshape(NX, NX // 2))
    return tuple(out)


def inverse_table():
    wave = waves()[:, None, :]
    a = angles(np.arange(NX // 2), wave.reshape(-1)).reshape(NX // 2, DEV, 1, NU)
    table = np.concatenate([np.cos(a), -np.sin(a)], axis=2) * (wave >= 0)
    return table.reshape(NX // 2, 2 * NX).astype(BF16)


def in_hbm(*arrays):
    return tuple(pltpu.with_memory_space_constraint(a, pltpu.HBM) for a in arrays)


def dot(a, b):
    return jnp.dot(a, b, preferred_element_type=F32)


def dot_nt(a, b):
    return lax.dot_general(a, b, (((1,), (1,)), ((), ())), preferred_element_type=F32)


def turn(q):
    whole = q.reshape(-1, 2 * NU, q.shape[1])
    real = lax.broadcasted_iota(jnp.int32, whole.shape, 1) < NU
    swapped = pltpu.roll(whole, NU, 1)
    return jnp.where(real, -swapped, swapped).reshape(q.shape)


def front_kernel(
    row_table, cells_hbm, splines_hbm, charges_hbm, counts, yh_hbm, yl_hbm, eh_hbm, el_hbm, oh_hbm, ol_hbm, out_hbm, *scratch
):
    bins = scratch[:SPREAD]
    spikes = scratch[8:10]
    lanes, values, dens_hi, dens_lo, fold_hi, fold_lo = scratch[10:16]
    tabs = scratch[16:22]
    out, cells, splines, charges, row_sem, tab_sem, out_sem, slot_sem = scratch[22:30]
    row_of = scratch[30:]
    slot_copies = [
        pltpu.make_async_copy(s, d, slot_sem.at[i])
        for i, (s, d) in enumerate(((cells_hbm, cells), (splines_hbm, splines), (charges_hbm, charges)))
    ]
    for copy in slot_copies:
        copy.start()
    row_copies = [pltpu.make_async_copy(row_table.at[t], row_of[t], row_sem.at[t]) for t in range(TILES)]
    for copy in row_copies:
        copy.start()
    sources = (yh_hbm, yl_hbm, eh_hbm, el_hbm, oh_hbm, ol_hbm)
    tab_copies = [pltpu.make_async_copy(s, d, tab_sem.at[i]) for i, (s, d) in enumerate(zip(sources, tabs))]
    for copy in tab_copies:
        copy.start()
    zeros = jnp.zeros((256, LANE), F32)

    def clear(i, carry):
        for b in bins:
            b[pl.ds(i * 256, 256), :] = zeros
        return carry

    lax.fori_loop(0, ROWS // 256, clear, 0)
    for copy in slot_copies:
        copy.wait()
    slot = lax.broadcasted_iota(jnp.int32, (1, SLOTS), 1)
    live = (slot < counts[0]).astype(F32)
    value = splines[...] * (charges[...] * live)
    lane_of = cells[...] & (LANE - 1)
    for t in range(TILES):
        lanes[t] = lane_of[:, t * LANE : (t + 1) * LANE]
        values[t] = value[:, t * LANE : (t + 1) * LANE]
    lane = lax.broadcasted_iota(jnp.int32, (SPREAD, LANE), 1)

    def build(spike, g):
        pick = jnp.full((SPREAD, LANE), g, jnp.int32)
        for t in range(TILES):
            at = jnp.take_along_axis(lanes[t], pick, axis=1)
            amount = jnp.take_along_axis(values[t], pick, axis=1)
            spike[t * SPREAD : (t + 1) * SPREAD, :] = jnp.where(lane == at, amount, 0.0)

    def apply(spike, g):
        for t in range(TILES):
            rows = [row_of[t][k, g] for k in range(SPREAD)]
            sums = [bins[k][pl.ds(rows[k], 1), :] + spike[pl.ds(t * SPREAD + k, 1), :] for k in range(SPREAD)]
            for k in range(SPREAD):
                bins[k][pl.ds(rows[k], 1), :] = sums[k]

    build(spikes[0], 0)
    for copy in row_copies:
        copy.wait()

    def body(h, carry):
        build(spikes[1], 2 * h + 1)
        apply(spikes[0], 2 * h)
        build(spikes[0], jnp.minimum(2 * h + 2, LANE - 1))
        apply(spikes[1], 2 * h + 1)
        return carry

    lax.fori_loop(0, LANE // 2, body, 0)
    for copy in tab_copies:
        copy.wait()
    yh, yl, *along_x = tabs
    first = lax.broadcasted_iota(jnp.int32, (NX, LANE), 1) == 0
    lower = lax.broadcasted_iota(jnp.int32, (NX, LANE), 0) % NU < 2
    row_of_tile = lax.broadcasted_iota(jnp.int32, (DEV // 2, 2 * NU, LANE), 1) % NU

    def plane(z, carry):
        for j in range(NY // LANE):
            for q in range(4):
                at = pl.ds(z * (NX * 4) + q * 512 + j, 128, stride=4)
                total = bins[0][at, :]
                for b in bins[1:]:
                    total = total + b[at, :]
                high = total.astype(BF16)
                dens_hi[q * 128 : (q + 1) * 128, j * LANE : (j + 1) * LANE] = high
                dens_lo[q * 128 : (q + 1) * 128, j * LANE : (j + 1) * LANE] = (total - high.astype(F32)).astype(BF16)
        along = dot(dens_hi[...], yh[...]) + dot(dens_lo[...], yh[...]) + dot(dens_hi[...], yl[...])
        near, far = along[: NX // 2], along[NX // 2 :]
        parts = []
        for h, folded in enumerate((near + far, near - far)):
            high = folded.astype(BF16)
            fold_hi[h] = high
            fold_lo[h] = (folded - high.astype(F32)).astype(BF16)
            tab_hi, tab_lo = along_x[2 * h], along_x[2 * h + 1]
            p, q = (
                dot(tab_hi[...], fold_hi[h, :, c]) + dot(tab_hi[...], fold_lo[h, :, c]) + dot(tab_lo[...], fold_hi[h, :, c])
                for c in (slice(0, HALF), slice(HALF, NY))
            )
            q = turn(q)
            p0, p1, q0, q1 = p[:, :LANE], p[:, LANE:], q[:, :LANE], q[:, LANE:]
            minus0 = jnp.where(first, 0.0, p0) - q0
            minus1 = p1 - q1
            parts.append(
                (
                    p0 + jnp.where(first, 0.0, q0),
                    p1 + q1,
                    jnp.where(first, minus1, minus0),
                    jnp.where(first, minus0, minus1),
                )
            )
        near = [jnp.where(lower, even, odd) for even, odd in zip(*parts)]
        far = [jnp.where(lower, odd, even) for even, odd in zip(*parts)]
        for side, (groups, spare) in enumerate(((near, 3), (far, 1))):
            shape = (DEV // 2, 2 * NU, LANE)
            last = groups[3].reshape(shape)
            for j in range(3):
                moved = pltpu.roll(last, (spare - (j ^ 2 * side)) % 8, 1)
                out[z, side * (DEV // 2) : (side + 1) * (DEV // 2), :, j * LANE : (j + 1) * LANE] = jnp.where(
                    row_of_tile == spare, moved, groups[j].reshape(shape)
                ).astype(BF16)
        pltpu.make_async_copy(out.at[z], out_hbm.at[:, z], out_sem.at[z]).start()
        return carry

    lax.fori_loop(0, ZD, plane, 0)
    for z in range(ZD):
        pltpu.make_async_copy(out.at[z], out_hbm.at[:, z], out_sem.at[z]).wait()


def prepare_kernel(green_hbm, cells_hbm, piece, rows, cells, sem):
    copies = [
        pltpu.make_async_copy(cells_hbm, cells, sem.at[0]),
        pltpu.make_async_copy(green_hbm.at[NU - 1], piece, sem.at[1]),
    ]
    for copy in copies:
        copy.start()
    copies[0].wait()
    for t in range(TILES):
        rows[t] = lax.shift_right_logical(cells[:, t * LANE : (t + 1) * LANE], 7)
    copies[1].wait()


def prepare(green, cells):
    hbm = pl.BlockSpec(memory_space=pltpu.HBM)
    vmem = pl.BlockSpec(memory_space=pltpu.VMEM)
    return pl.pallas_call(
        prepare_kernel,
        out_shape=(pltpu.VMEM(green.shape[1:], BF16), pltpu.VMEM((TILES, SPREAD, LANE), jnp.int32)),
        in_specs=[hbm, hbm],
        out_specs=(vmem, vmem),
        scratch_shapes=[pltpu.VMEM((SPREAD, SLOTS), jnp.int32), pltpu.SemaphoreType.DMA((2,))],
        compiler_params=pltpu.CompilerParams(vmem_limit_bytes=8 << 20),
        name="prepare",
    )(*in_hbm(green, cells))


def front(rows, charges, cells, splines, counts, tabs):
    smem = pl.BlockSpec(memory_space=pltpu.SMEM)
    hbm = pl.BlockSpec(memory_space=pltpu.HBM)
    return pl.pallas_call(
        front_kernel,
        out_shape=pltpu.HBM((DEV, ZD, 2 * NU, WIDE), BF16),
        in_specs=[pl.BlockSpec(memory_space=pltpu.VMEM)] + [hbm] * 3 + [smem] + [hbm] * 6,
        out_specs=hbm,
        scratch_shapes=[pltpu.VMEM((ROWS, LANE), F32)] * SPREAD
        + [pltpu.VMEM((LANE, LANE), F32)] * 2
        + [pltpu.VMEM((TILES, SPREAD, LANE), jnp.int32), pltpu.VMEM((TILES, SPREAD, LANE), F32)]
        + [pltpu.VMEM((NX, NY), BF16)] * 2
        + [pltpu.VMEM((2, NX // 2, NY), BF16)] * 2
        + [pltpu.VMEM(t.shape, BF16) for t in tabs]
        + [pltpu.VMEM((ZD, DEV, 2 * NU, WIDE), BF16)]
        + [pltpu.VMEM((SPREAD, SLOTS), jnp.int32), pltpu.VMEM((SPREAD, SLOTS), F32), pltpu.VMEM((1, SLOTS), F32)]
        + [pltpu.SemaphoreType.DMA((n,)) for n in (TILES, 6, ZD, 3)]
        + [pltpu.SMEM((SPREAD, LANE), jnp.int32)] * TILES,
        compiler_params=pltpu.CompilerParams(vmem_limit_bytes=44 << 20),
        name="front",
    )(rows, *in_hbm(cells, splines, charges.reshape(1, SLOTS)), counts, *in_hbm(*tabs))


WAVE = (0, 2, 1)
BLOCK = (0, 1, 3, 2)
MIRROR = (3, 2, 0, 1)
SWAP = (1, 3, 0, 2)
PART = NZ // 2


def green_kernel(
    far, spectrum, green_hbm, mirror_hbm, x_hbm, y_hbm, out, x_out, y_out, green, flat, sums, swapped, green_sem, *rhs
):
    sources = [green_hbm.at[w] for w in WAVE] + [mirror_hbm]
    fetches = [pltpu.make_async_copy(s, green.at[i], green_sem.at[i]) for i, s in enumerate(sources)]
    fetches.append(pltpu.make_async_copy(x_hbm, x_out, green_sem.at[4]))
    fetches.append(pltpu.make_async_copy(y_hbm, y_out, green_sem.at[5]))
    for fetch in fetches:
        fetch.start()
    at = [jnp.bitwise_xor(row, 2 * far[0]) for row in range(NU)]
    for j in range(3):
        flat[...] = spectrum[:, :, j * LANE : (j + 1) * LANE].astype(F32).reshape(NZ * 2 * NU, LANE)
        for row in range(NU):
            for c in range(2):
                values = flat[pl.ds(c * NU + at[row], NZ, stride=2 * NU), :].astype(BF16)
                to, group = (rhs[row], j) if row < 3 else (rhs[j], 3)
                to[group, :, c * LANE : (c + 1) * LANE] = values
    first = lax.broadcasted_iota(jnp.int32, (NZ, 2 * LANE), 1) % LANE == 0
    for j in range(KYB):
        swapped[j] = jnp.where(first, rhs[2][SWAP[j]], rhs[2][j])
    first = first[:PART]
    for part in range(2):
        planes = slice(part * PART, (part + 1) * PART)
        for row in range(3):
            if part == 0:
                fetches[row].wait()
            m = [dot(green[row, BLOCK[j], planes, :], rhs[row][j]) for j in range(KYB)]
            if row == 2:
                if part == 0:
                    fetches[3].wait()
                other = [dot(green[3, MIRROR[j], planes, :], swapped[j]) for j in range(KYB)]
                m = [m[j] + jnp.where(first, other[SWAP.index(j)], other[j]) for j in range(KYB)]
            s2 = jnp.where(first, m[3], m[2])
            s3 = jnp.where(first, m[2], m[3])
            t0 = m[0] + jnp.where(first, 0.0, s2)
            d0 = jnp.where(first, 0.0, m[0]) - s2
            t1 = m[1] + s3
            d1 = m[1] - s3
            groups = (
                (t0[:, :LANE], t0[:, LANE:]),
                (t1[:, :LANE], t1[:, LANE:]),
                (d0[:, LANE:], -d0[:, :LANE]),
                (d1[:, LANE:], -d1[:, :LANE]),
            )
            for j, group in enumerate(groups):
                for c in range(2):
                    to, slot = (j, row) if j < 3 else (row, 3)
                    sums[to, pl.ds(c * NU + at[slot], PART, stride=2 * NU), :] = group[c]
        for j in range(3):
            out[planes, :, j * LANE : (j + 1) * LANE] = sums[j].astype(BF16).reshape(PART, 2 * NU, LANE)
    for fetch in fetches[4:]:
        fetch.wait()


def mix(pencil, green, mirror, *tabs):
    vmem = pl.BlockSpec(memory_space=pltpu.VMEM)
    hbm = pl.BlockSpec(memory_space=pltpu.HBM)
    return pl.pallas_call(
        green_kernel,
        out_shape=(pltpu.VMEM((NZ, 2 * NU, WIDE), BF16), *(pltpu.VMEM(t.shape, BF16) for t in tabs)),
        in_specs=[pl.BlockSpec(memory_space=pltpu.SMEM), vmem, hbm, hbm, hbm, hbm],
        out_specs=(vmem, vmem, vmem),
        compiler_params=pltpu.CompilerParams(vmem_limit_bytes=36 << 20),
        scratch_shapes=[
            pltpu.VMEM((NU, KYB, NZ, NZ), BF16),
            pltpu.VMEM((NZ * 2 * NU, LANE), F32),
            pltpu.VMEM((3, PART * 2 * NU, LANE), F32),
            pltpu.VMEM((KYB, NZ, 2 * LANE), BF16),
            pltpu.SemaphoreType.DMA((6,)),
        ]
        + [pltpu.VMEM((KYB, NZ, 2 * LANE), BF16)] * 3,
        name="mix",
    )(lax.axis_index("zg").astype(jnp.int32).reshape(1), pencil.reshape(NZ, 2 * NU, WIDE), *in_hbm(green, mirror, *tabs))


def back_kernel(mixed, half_x, along_y, out_hbm, far_x, out, rest, out_sem):
    row_of_tile = lax.broadcasted_iota(jnp.int32, (DEV // 2, 2 * NU, LANE), 1) % NU
    sends = []
    for z in range(ZD):
        for side in range(2):
            devices = slice(side * (DEV // 2), (side + 1) * (DEV // 2))
            spare = 3 - 2 * side
            last = None
            for j in range(3):
                group = mixed[devices, z, :, j * LANE : (j + 1) * LANE].astype(F32)
                moved = pltpu.roll(group, ((j ^ 2 * side) - spare) % 8, 1)
                last = moved if last is None else jnp.where(row_of_tile == (j ^ 2 * side), moved, last)
            rest[devices, :, LANE:] = last.astype(BF16)
        rest[:, :, :LANE] = mixed[:, z, :, 2 * LANE :]
        for h in range(2):
            rows = pl.ds(h * HALF, HALF)
            if z == 0 and h == 1:
                place = lax.broadcasted_iota(jnp.int32, (1, 2 * NX), 1)
                sign = jnp.where(place % NU == jnp.where(place < NX, 2, 0), -1.0, 1.0).astype(BF16)
                far_x[...] = half_x[...] * sign
            along_x = (half_x, far_x)[h]
            front = dot(along_x[...], mixed[:, z, :, : 2 * LANE].reshape(2 * NX, 2 * LANE)).astype(BF16)
            tail = dot(along_x[...], rest[...].reshape(2 * NX, 2 * LANE)).astype(BF16)
            out[z, rows, :] = dot_nt(front, along_y[:, : 2 * LANE]) + dot_nt(tail, along_y[:, 2 * LANE :])
            send = pltpu.make_async_copy(out.at[z, rows], out_hbm.at[z, rows], out_sem.at[2 * z + h])
            send.start()
            sends.append(send)
    for send in sends:
        send.wait()


def back(returned, inverse_x, inverse_y):
    vmem = pl.BlockSpec(memory_space=pltpu.VMEM)
    hbm = pl.BlockSpec(memory_space=pltpu.HBM)
    return pl.pallas_call(
        back_kernel,
        out_shape=jax.ShapeDtypeStruct((ZD, NX, NY), F32),
        in_specs=[vmem, vmem, vmem],
        out_specs=hbm,
        compiler_params=pltpu.CompilerParams(vmem_limit_bytes=24 << 20),
        scratch_shapes=[
            pltpu.VMEM((NX // 2, 2 * NX), BF16),
            pltpu.VMEM((ZD, NX, NY), F32),
            pltpu.VMEM((DEV, 2 * NU, 2 * LANE), BF16),
            pltpu.SemaphoreType.DMA((2 * ZD,)),
        ],
        name="back",
    )(returned, inverse_x, inverse_y)


def steps(charges, cells, splines, counts, green):
    forward = tuple(jnp.asarray(t) for t in forward_tables())
    piece, rows = prepare(green, cells)
    mirror = lax.ppermute(piece, AXES, [(d, DEV - 1 - d) for d in range(DEV)])
    spectrum = front(rows, charges, cells, splines, counts, forward)
    pencil = lax.all_to_all(spectrum, AXES, split_axis=0, concat_axis=0, tiled=True)
    mixed, *along = mix(pencil, green, mirror, jnp.asarray(inverse_table()), forward[0])
    mixed = mixed.reshape(DEV, ZD, 2 * NU, WIDE)
    returned = lax.all_to_all(mixed, AXES, split_axis=0, concat_axis=0, tiled=True)
    return back(returned, *along)


def solution(mesh):
    in_specs = (
        P(AXES),
        P(None, AXES),
        P(None, AXES),
        P(AXES),
        P(AXES, None, None, None),
    )
    return jax.shard_map(steps, mesh=mesh, in_specs=in_specs, out_specs=P(AXES, None, None), check_vma=False)
```

```python
import jax
import jax.numpy as jnp
import numpy as np
from jax import lax
from jax.experimental import pallas as pl
from jax.experimental.pallas import tpu as pltpu
from jax.sharding import PartitionSpec as P

NX = 512
NY = 512
NZ = 384
KYB = 4
AXES = ("zg", "xy")
DEV = 128
ZD = 3
NU = NX // DEV
HALF = NY // 2
LANE = 128
WIDE = 3 * LANE
SLOTS = 2048
SPREAD = 8
TILES = SLOTS // LANE
ROWS = ZD * NX * NY // LANE
F32 = jnp.float32
BF16 = jnp.bfloat16


def split(table):
    high = table.astype(BF16)
    return high, (table - high.astype(np.float64)).astype(BF16)


def angles(left, right):
    return (np.outer(left, right) % NX) * (2.0 * np.pi / NX)


def waves():
    device = np.arange(DEV)[:, None]
    offset = np.array([[0, 2, 1, -1], [1, -1, 0, 2]])[device[:, 0] // (DEV // 2)]
    return np.where(offset < 0, -1, device * NU + offset)


def forward_tables():
    y = np.arange(NY)
    v = np.arange(HALF)
    along_y = np.concatenate([np.cos(angles(y, v)), -np.sin(angles(y, v))], axis=1)
    along_y[:, HALF] = np.where(y % 2 == 0, 1.0, -1.0)
    x = np.arange(NX // 2)
    near, far = waves()[: DEV // 2], waves()[DEV // 2 :]
    out = [*split(along_y / 512.0)]
    for wave in (np.concatenate([near[:, :2], far[:, 2:]], axis=1), np.concatenate([far[:, :2], near[:, 2:]], axis=1)):
        a = angles(wave.reshape(-1), x).reshape(DEV // 2, NU, NX // 2)
        used = (wave >= 0)[:, :, None]
        out += split(np.stack([np.cos(a) * used, -np.sin(a) * used], axis=1).reshape(NX, NX // 2))
    return tuple(out)


def inverse_table():
    wave = waves()[:, None, :]
    a = angles(np.arange(NX // 2), wave.reshape(-1)).reshape(NX // 2, DEV, 1, NU)
    table = np.concatenate([np.cos(a), -np.sin(a)], axis=2) * (wave >= 0)
    return table.reshape(NX // 2, 2 * NX).astype(BF16)


def in_hbm(*arrays):
    return tuple(pltpu.with_memory_space_constraint(a, pltpu.HBM) for a in arrays)


def dot(a, b):
    return jnp.dot(a, b, preferred_element_type=F32)


def dot_nt(a, b):
    return lax.dot_general(a, b, (((1,), (1,)), ((), ())), preferred_element_type=F32)


def turn(q):
    whole = q.reshape(-1, 2 * NU, q.shape[1])
    real = lax.broadcasted_iota(jnp.int32, whole.shape, 1) < NU
    swapped = pltpu.roll(whole, NU, 1)
    return jnp.where(real, -swapped, swapped).reshape(q.shape)


def front_kernel(
    row_table, cells_hbm, splines_hbm, charges_hbm, counts, yh_hbm, yl_hbm, eh_hbm, el_hbm, oh_hbm, ol_hbm, out_hbm, *scratch
):
    bins = scratch[:SPREAD]
    spikes = scratch[8:10]
    lanes, values, dens_hi, dens_lo, fold_hi, fold_lo = scratch[10:16]
    tabs = scratch[16:22]
    out, cells, splines, charges, row_sem, tab_sem, out_sem, slot_sem = scratch[22:30]
    row_of = scratch[30:]
    slot_copies = [
        pltpu.make_async_copy(s, d, slot_sem.at[i])
        for i, (s, d) in enumerate(((cells_hbm, cells), (splines_hbm, splines), (charges_hbm, charges)))
    ]
    for copy in slot_copies:
        copy.start()
    row_copies = [pltpu.make_async_copy(row_table.at[t], row_of[t], row_sem.at[t]) for t in range(TILES)]
    for copy in row_copies:
        copy.start()
    sources = (yh_hbm, yl_hbm, eh_hbm, el_hbm, oh_hbm, ol_hbm)
    tab_copies = [pltpu.make_async_copy(s, d, tab_sem.at[i]) for i, (s, d) in enumerate(zip(sources, tabs))]
    for copy in tab_copies:
        copy.start()
    zeros = jnp.zeros((256, LANE), F32)

    def clear(i, carry):
        for b in bins:
            b[pl.ds(i * 256, 256), :] = zeros
        return carry

    lax.fori_loop(0, ROWS // 256, clear, 0)
    for copy in slot_copies:
        copy.wait()
    slot = lax.broadcasted_iota(jnp.int32, (1, SLOTS), 1)
    live = (slot < counts[0]).astype(F32)
    value = splines[...] * (charges[...] * live)
    lane_of = cells[...] & (LANE - 1)
    for t in range(TILES):
        lanes[t] = lane_of[:, t * LANE : (t + 1) * LANE]
        values[t] = value[:, t * LANE : (t + 1) * LANE]
    lane = lax.broadcasted_iota(jnp.int32, (SPREAD, LANE), 1)

    def build(spike, g):
        pick = jnp.full((SPREAD, LANE), g, jnp.int32)
        for t in range(TILES):
            at = jnp.take_along_axis(lanes[t], pick, axis=1)
            amount = jnp.take_along_axis(values[t], pick, axis=1)
            spike[t * SPREAD : (t + 1) * SPREAD, :] = jnp.where(lane == at, amount, 0.0)

    def apply(spike, g):
        for t in range(TILES):
            rows = [row_of[t][k, g] for k in range(SPREAD)]
            sums = [bins[k][pl.ds(rows[k], 1), :] + spike[pl.ds(t * SPREAD + k, 1), :] for k in range(SPREAD)]
            for k in range(SPREAD):
                bins[k][pl.ds(rows[k], 1), :] = sums[k]

    build(spikes[0], 0)
    for copy in row_copies:
        copy.wait()

    def body(h, carry):
        build(spikes[1], 2 * h + 1)
        apply(spikes[0], 2 * h)
        build(spikes[0], jnp.minimum(2 * h + 2, LANE - 1))
        apply(spikes[1], 2 * h + 1)
        return carry

    lax.fori_loop(0, LANE // 2, body, 0)
    for copy in tab_copies:
        copy.wait()
    yh, yl, *along_x = tabs
    first = lax.broadcasted_iota(jnp.int32, (NX, LANE), 1) == 0
    lower = lax.broadcasted_iota(jnp.int32, (NX, LANE), 0) % NU < 2
    row_of_tile = lax.broadcasted_iota(jnp.int32, (DEV // 2, 2 * NU, LANE), 1) % NU

    def plane(z, carry):
        for j in range(NY // LANE):
            for q in range(4):
                at = pl.ds(j * (ROWS // 4) + z * NX + q * 128, 128)
                total = bins[0][at, :]
                for b in bins[1:]:
                    total = total + b[at, :]
                high = total.astype(BF16)
                dens_hi[q * 128 : (q + 1) * 128, j * LANE : (j + 1) * LANE] = high
                dens_lo[q * 128 : (q + 1) * 128, j * LANE : (j + 1) * LANE] = (total - high.astype(F32)).astype(BF16)
        along = dot(dens_hi[...], yh[...]) + dot(dens_lo[...], yh[...]) + dot(dens_hi[...], yl[...])
        near, far = along[: NX // 2], along[NX // 2 :]
        parts = []
        for h, folded in enumerate((near + far, near - far)):
            high = folded.astype(BF16)
            fold_hi[h] = high
            fold_lo[h] = (folded - high.astype(F32)).astype(BF16)
            tab_hi, tab_lo = along_x[2 * h], along_x[2 * h + 1]
            p, q = (
                dot(tab_hi[...], fold_hi[h, :, c]) + dot(tab_hi[...], fold_lo[h, :, c]) + dot(tab_lo[...], fold_hi[h, :, c])
                for c in (slice(0, HALF), slice(HALF, NY))
            )
            q = turn(q)
            p0, p1, q0, q1 = p[:, :LANE], p[:, LANE:], q[:, :LANE], q[:, LANE:]
            minus0 = jnp.where(first, 0.0, p0) - q0
            minus1 = p1 - q1
            parts.append(
                (
                    p0 + jnp.where(first, 0.0, q0),
                    p1 + q1,
                    jnp.where(first, minus1, minus0),
                    jnp.where(first, minus0, minus1),
                )
            )
        near = [jnp.where(lower, even, odd) for even, odd in zip(*parts)]
        far = [jnp.where(lower, odd, even) for even, odd in zip(*parts)]
        for side, (groups, spare) in enumerate(((near, 3), (far, 1))):
            shape = (DEV // 2, 2 * NU, LANE)
            last = groups[3].reshape(shape)
            for j in range(3):
                moved = pltpu.roll(last, (spare - (j ^ 2 * side)) % 8, 1)
                out[z, side * (DEV // 2) : (side + 1) * (DEV // 2), :, j * LANE : (j + 1) * LANE] = jnp.where(
                    row_of_tile == spare, moved, groups[j].reshape(shape)
                ).astype(BF16)
        pltpu.make_async_copy(out.at[z], out_hbm.at[:, z], out_sem.at[z]).start()
        return carry

    lax.fori_loop(0, ZD, plane, 0)
    for z in range(ZD):
        pltpu.make_async_copy(out.at[z], out_hbm.at[:, z], out_sem.at[z]).wait()


def prepare_kernel(green_hbm, cells_hbm, piece, rows, cells, sem):
    copies = [
        pltpu.make_async_copy(cells_hbm, cells, sem.at[0]),
        pltpu.make_async_copy(green_hbm.at[NU - 1], piece, sem.at[1]),
    ]
    for copy in copies:
        copy.start()
    copies[0].wait()
    for t in range(TILES):
        row = lax.shift_right_logical(cells[:, t * LANE : (t + 1) * LANE], 7)
        rows[t] = (row & 3) * (ROWS // 4) + lax.shift_right_logical(row, 2)
    copies[1].wait()


def prepare(green, cells):
    hbm = pl.BlockSpec(memory_space=pltpu.HBM)
    vmem = pl.BlockSpec(memory_space=pltpu.VMEM)
    return pl.pallas_call(
        prepare_kernel,
        out_shape=(pltpu.VMEM(green.shape[1:], BF16), pltpu.VMEM((TILES, SPREAD, LANE), jnp.int32)),
        in_specs=[hbm, hbm],
        out_specs=(vmem, vmem),
        scratch_shapes=[pltpu.VMEM((SPREAD, SLOTS), jnp.int32), pltpu.SemaphoreType.DMA((2,))],
        compiler_params=pltpu.CompilerParams(vmem_limit_bytes=8 << 20),
        name="prepare",
    )(*in_hbm(green, cells))


def front(rows, charges, cells, splines, counts, tabs):
    smem = pl.BlockSpec(memory_space=pltpu.SMEM)
    hbm = pl.BlockSpec(memory_space=pltpu.HBM)
    return pl.pallas_call(
        front_kernel,
        out_shape=pltpu.HBM((DEV, ZD, 2 * NU, WIDE), BF16),
        in_specs=[pl.BlockSpec(memory_space=pltpu.VMEM)] + [hbm] * 3 + [smem] + [hbm] * 6,
        out_specs=hbm,
        scratch_shapes=[pltpu.VMEM((ROWS, LANE), F32)] * SPREAD
        + [pltpu.VMEM((LANE, LANE), F32)] * 2
        + [pltpu.VMEM((TILES, SPREAD, LANE), jnp.int32), pltpu.VMEM((TILES, SPREAD, LANE), F32)]
        + [pltpu.VMEM((NX, NY), BF16)] * 2
        + [pltpu.VMEM((2, NX // 2, NY), BF16)] * 2
        + [pltpu.VMEM(t.shape, BF16) for t in tabs]
        + [pltpu.VMEM((ZD, DEV, 2 * NU, WIDE), BF16)]
        + [pltpu.VMEM((SPREAD, SLOTS), jnp.int32), pltpu.VMEM((SPREAD, SLOTS), F32), pltpu.VMEM((1, SLOTS), F32)]
        + [pltpu.SemaphoreType.DMA((n,)) for n in (TILES, 6, ZD, 3)]
        + [pltpu.SMEM((SPREAD, LANE), jnp.int32)] * TILES,
        compiler_params=pltpu.CompilerParams(vmem_limit_bytes=44 << 20),
        name="front",
    )(rows, *in_hbm(cells, splines, charges.reshape(1, SLOTS)), counts, *in_hbm(*tabs))


WAVE = (0, 2, 1)
BLOCK = (0, 1, 3, 2)
MIRROR = (3, 2, 0, 1)
SWAP = (1, 3, 0, 2)
PART = NZ // 2


def green_kernel(
    far, spectrum, green_hbm, mirror_hbm, x_hbm, y_hbm, out, x_out, y_out, green, flat, sums, swapped, green_sem, *rhs
):
    sources = [green_hbm.at[w] for w in WAVE] + [mirror_hbm]
    fetches = [pltpu.make_async_copy(s, green.at[i], green_sem.at[i]) for i, s in enumerate(sources)]
    fetches.append(pltpu.make_async_copy(x_hbm, x_out, green_sem.at[4]))
    fetches.append(pltpu.make_async_copy(y_hbm, y_out, green_sem.at[5]))
    for fetch in fetches:
        fetch.start()
    at = [jnp.bitwise_xor(row, 2 * far[0]) for row in range(NU)]
    for j in range(3):
        flat[...] = spectrum[:, :, j * LANE : (j + 1) * LANE].astype(F32).reshape(NZ * 2 * NU, LANE)
        for row in range(NU):
            for c in range(2):
                values = flat[pl.ds(c * NU + at[row], NZ, stride=2 * NU), :].astype(BF16)
                to, group = (rhs[row], j) if row < 3 else (rhs[j], 3)
                to[group, :, c * LANE : (c + 1) * LANE] = values
    first = lax.broadcasted_iota(jnp.int32, (NZ, 2 * LANE), 1) % LANE == 0
    for j in range(KYB):
        swapped[j] = jnp.where(first, rhs[2][SWAP[j]], rhs[2][j])
    first = first[:PART]
    for part in range(2):
        planes = slice(part * PART, (part + 1) * PART)
        for row in range(3):
            if part == 0:
                fetches[row].wait()
            m = [dot(green[row, BLOCK[j], planes, :], rhs[row][j]) for j in range(KYB)]
            if row == 2:
                if part == 0:
                    fetches[3].wait()
                other = [dot(green[3, MIRROR[j], planes, :], swapped[j]) for j in range(KYB)]
                m = [m[j] + jnp.where(first, other[SWAP.index(j)], other[j]) for j in range(KYB)]
            s2 = jnp.where(first, m[3], m[2])
            s3 = jnp.where(first, m[2], m[3])
            t0 = m[0] + jnp.where(first, 0.0, s2)
            d0 = jnp.where(first, 0.0, m[0]) - s2
            t1 = m[1] + s3
            d1 = m[1] - s3
            groups = (
                (t0[:, :LANE], t0[:, LANE:]),
                (t1[:, :LANE], t1[:, LANE:]),
                (d0[:, LANE:], -d0[:, :LANE]),
                (d1[:, LANE:], -d1[:, :LANE]),
            )
            for j, group in enumerate(groups):
                for c in range(2):
                    to, slot = (j, row) if j < 3 else (row, 3)
                    sums[to, pl.ds(c * NU + at[slot], PART, stride=2 * NU), :] = group[c]
        for j in range(3):
            out[planes, :, j * LANE : (j + 1) * LANE] = sums[j].astype(BF16).reshape(PART, 2 * NU, LANE)
    for fetch in fetches[4:]:
        fetch.wait()


def mix(pencil, green, mirror, *tabs):
    vmem = pl.BlockSpec(memory_space=pltpu.VMEM)
    hbm = pl.BlockSpec(memory_space=pltpu.HBM)
    return pl.pallas_call(
        green_kernel,
        out_shape=(pltpu.VMEM((NZ, 2 * NU, WIDE), BF16), *(pltpu.VMEM(t.shape, BF16) for t in tabs)),
        in_specs=[pl.BlockSpec(memory_space=pltpu.SMEM), vmem, hbm, hbm, hbm, hbm],
        out_specs=(vmem, vmem, vmem),
        compiler_params=pltpu.CompilerParams(vmem_limit_bytes=36 << 20),
        scratch_shapes=[
            pltpu.VMEM((NU, KYB, NZ, NZ), BF16),
            pltpu.VMEM((NZ * 2 * NU, LANE), F32),
            pltpu.VMEM((3, PART * 2 * NU, LANE), F32),
            pltpu.VMEM((KYB, NZ, 2 * LANE), BF16),
            pltpu.SemaphoreType.DMA((6,)),
        ]
        + [pltpu.VMEM((KYB, NZ, 2 * LANE), BF16)] * 3,
        name="mix",
    )(lax.axis_index("zg").astype(jnp.int32).reshape(1), pencil.reshape(NZ, 2 * NU, WIDE), *in_hbm(green, mirror, *tabs))


def back_kernel(mixed, half_x, along_y, out_hbm, far_x, out, rest, out_sem):
    row_of_tile = lax.broadcasted_iota(jnp.int32, (DEV // 2, 2 * NU, LANE), 1) % NU
    sends = []
    for z in range(ZD):
        for side in range(2):
            devices = slice(side * (DEV // 2), (side + 1) * (DEV // 2))
            spare = 3 - 2 * side
            last = None
            for j in range(3):
                group = mixed[devices, z, :, j * LANE : (j + 1) * LANE].astype(F32)
                moved = pltpu.roll(group, ((j ^ 2 * side) - spare) % 8, 1)
                last = moved if last is None else jnp.where(row_of_tile == (j ^ 2 * side), moved, last)
            rest[devices, :, LANE:] = last.astype(BF16)
        rest[:, :, :LANE] = mixed[:, z, :, 2 * LANE :]
        for h in range(2):
            rows = pl.ds(h * HALF, HALF)
            if z == 0 and h == 1:
                place = lax.broadcasted_iota(jnp.int32, (1, 2 * NX), 1)
                sign = jnp.where(place % NU == jnp.where(place < NX, 2, 0), -1.0, 1.0).astype(BF16)
                far_x[...] = half_x[...] * sign
            along_x = (half_x, far_x)[h]
            front = dot(along_x[...], mixed[:, z, :, : 2 * LANE].reshape(2 * NX, 2 * LANE)).astype(BF16)
            tail = dot(along_x[...], rest[...].reshape(2 * NX, 2 * LANE)).astype(BF16)
            out[z, rows, :] = dot_nt(front, along_y[:, : 2 * LANE]) + dot_nt(tail, along_y[:, 2 * LANE :])
            send = pltpu.make_async_copy(out.at[z, rows], out_hbm.at[z, rows], out_sem.at[2 * z + h])
            send.start()
            sends.append(send)
    for send in sends:
        send.wait()


def back(returned, inverse_x, inverse_y):
    vmem = pl.BlockSpec(memory_space=pltpu.VMEM)
    hbm = pl.BlockSpec(memory_space=pltpu.HBM)
    return pl.pallas_call(
        back_kernel,
        out_shape=jax.ShapeDtypeStruct((ZD, NX, NY), F32),
        in_specs=[vmem, vmem, vmem],
        out_specs=hbm,
        compiler_params=pltpu.CompilerParams(vmem_limit_bytes=24 << 20),
        scratch_shapes=[
            pltpu.VMEM((NX // 2, 2 * NX), BF16),
            pltpu.VMEM((ZD, NX, NY), F32),
            pltpu.VMEM((DEV, 2 * NU, 2 * LANE), BF16),
            pltpu.SemaphoreType.DMA((2 * ZD,)),
        ],
        name="back",
    )(returned, inverse_x, inverse_y)


def steps(charges, cells, splines, counts, green):
    forward = tuple(jnp.asarray(t) for t in forward_tables())
    piece, rows = prepare(green, cells)
    mirror = lax.ppermute(piece, AXES, [(d, DEV - 1 - d) for d in range(DEV)])
    spectrum = front(rows, charges, cells, splines, counts, forward)
    pencil = lax.all_to_all(spectrum, AXES, split_axis=0, concat_axis=0, tiled=True)
    mixed, *along = mix(pencil, green, mirror, jnp.asarray(inverse_table()), forward[0])
    mixed = mixed.reshape(DEV, ZD, 2 * NU, WIDE)
    returned = lax.all_to_all(mixed, AXES, split_axis=0, concat_axis=0, tiled=True)
    return back(returned, *along)


def solution(mesh):
    in_specs = (
        P(AXES),
        P(None, AXES),
        P(None, AXES),
        P(AXES),
        P(AXES, None, None, None),
    )
    return jax.shard_map(steps, mesh=mesh, in_specs=in_specs, out_specs=P(AXES, None, None), check_vma=False)
```

```python
import jax
import jax.numpy as jnp
import numpy as np
from jax import lax
from jax.experimental import pallas as pl
from jax.experimental.pallas import tpu as pltpu
from jax.sharding import PartitionSpec as P

NX = 512
NY = 512
NZ = 384
KYB = 4
AXES = ("zg", "xy")
DEV = 128
ZD = 3
NU = NX // DEV
HALF = NY // 2
LANE = 128
WIDE = 3 * LANE
SLOTS = 2048
SPREAD = 8
TILES = SLOTS // LANE
ROWS = ZD * NX * NY // LANE
F32 = jnp.float32
BF16 = jnp.bfloat16


def split(table):
    high = table.astype(BF16)
    return high, (table - high.astype(np.float64)).astype(BF16)


def angles(left, right):
    return (np.outer(left, right) % NX) * (2.0 * np.pi / NX)


def waves():
    device = np.arange(DEV)[:, None]
    offset = np.array([[0, 2, 1, -1], [1, -1, 0, 2]])[device[:, 0] // (DEV // 2)]
    return np.where(offset < 0, -1, device * NU + offset)


def forward_tables():
    y = np.arange(NY)
    v = np.arange(HALF)
    along_y = np.concatenate([np.cos(angles(y, v)), -np.sin(angles(y, v))], axis=1)
    along_y[:, HALF] = np.where(y % 2 == 0, 1.0, -1.0)
    x = np.arange(NX // 2)
    near, far = waves()[: DEV // 2], waves()[DEV // 2 :]
    out = [*split(along_y / 512.0)]
    for wave in (np.concatenate([near[:, :2], far[:, 2:]], axis=1), np.concatenate([far[:, :2], near[:, 2:]], axis=1)):
        a = angles(wave.reshape(-1), x).reshape(DEV // 2, NU, NX // 2)
        used = (wave >= 0)[:, :, None]
        out += split(np.stack([np.cos(a) * used, -np.sin(a) * used], axis=1).reshape(NX, NX // 2))
    return tuple(out)


def inverse_table():
    wave = waves()[:, None, :]
    a = angles(np.arange(NX // 2), wave.reshape(-1)).reshape(NX // 2, DEV, 1, NU)
    table = np.concatenate([np.cos(a), -np.sin(a)], axis=2) * (wave >= 0)
    return table.reshape(NX // 2, 2 * NX).astype(BF16)


def in_hbm(*arrays):
    return tuple(pltpu.with_memory_space_constraint(a, pltpu.HBM) for a in arrays)


def dot(a, b):
    return jnp.dot(a, b, preferred_element_type=F32)


def dot_nt(a, b):
    return lax.dot_general(a, b, (((1,), (1,)), ((), ())), preferred_element_type=F32)


def turn(q):
    whole = q.reshape(-1, 2 * NU, q.shape[1])
    real = lax.broadcasted_iota(jnp.int32, whole.shape, 1) < NU
    swapped = pltpu.roll(whole, NU, 1)
    return jnp.where(real, -swapped, swapped).reshape(q.shape)


def front_kernel(
    row_table, cells_hbm, splines_hbm, charges_hbm, counts, yh_hbm, yl_hbm, eh_hbm, el_hbm, oh_hbm, ol_hbm, out_hbm, *scratch
):
    bins = scratch[:SPREAD]
    spikes = scratch[8:10]
    lanes, values, dens_hi, dens_lo, fold_hi, fold_lo = scratch[10:16]
    tabs = scratch[16:22]
    out, cells, splines, charges, row_sem, tab_sem, out_sem, slot_sem = scratch[22:30]
    row_of = scratch[30:]
    slot_copies = [
        pltpu.make_async_copy(s, d, slot_sem.at[i])
        for i, (s, d) in enumerate(((cells_hbm, cells), (splines_hbm, splines), (charges_hbm, charges)))
    ]
    for copy in slot_copies:
        copy.start()
    row_copies = [pltpu.make_async_copy(row_table.at[t], row_of[t], row_sem.at[t]) for t in range(TILES)]
    for copy in row_copies:
        copy.start()
    sources = (yh_hbm, yl_hbm, eh_hbm, el_hbm, oh_hbm, ol_hbm)
    tab_copies = [pltpu.make_async_copy(s, d, tab_sem.at[i]) for i, (s, d) in enumerate(zip(sources, tabs))]
    for copy in tab_copies:
        copy.start()
    zeros = jnp.zeros((256, LANE), F32)

    def clear(i, carry):
        for b in bins:
            b[pl.ds(i * 256, 256), :] = zeros
        return carry

    lax.fori_loop(0, ROWS // 256, clear, 0)
    for copy in slot_copies:
        copy.wait()
    slot = lax.broadcasted_iota(jnp.int32, (1, SLOTS), 1)
    live = (slot < counts[0]).astype(F32)
    value = splines[...] * (charges[...] * live)
    lane_of = cells[...] & (LANE - 1)
    for t in range(TILES):
        lanes[t] = lane_of[:, t * LANE : (t + 1) * LANE]
        values[t] = value[:, t * LANE : (t + 1) * LANE]
    lane = lax.broadcasted_iota(jnp.int32, (SPREAD, LANE), 1)

    def build(spike, g):
        pick = jnp.full((SPREAD, LANE), g, jnp.int32)
        for t in range(TILES):
            at = jnp.take_along_axis(lanes[t], pick, axis=1)
            amount = jnp.take_along_axis(values[t], pick, axis=1)
            spike[t * SPREAD : (t + 1) * SPREAD, :] = jnp.where(lane == at, amount, 0.0)

    def apply(spike, g):
        for t in range(TILES):
            rows = [row_of[t][k, g] for k in range(SPREAD)]
            sums = [bins[k][pl.ds(rows[k], 1), :] + spike[pl.ds(t * SPREAD + k, 1), :] for k in range(SPREAD)]
            for k in range(SPREAD):
                bins[k][pl.ds(rows[k], 1), :] = sums[k]

    build(spikes[0], 0)
    for copy in row_copies:
        copy.wait()

    def body(h, carry):
        build(spikes[1], 2 * h + 1)
        apply(spikes[0], 2 * h)
        build(spikes[0], jnp.minimum(2 * h + 2, LANE - 1))
        apply(spikes[1], 2 * h + 1)
        return carry

    lax.fori_loop(0, LANE // 2, body, 0)
    for copy in tab_copies:
        copy.wait()
    yh, yl, *along_x = tabs
    first = lax.broadcasted_iota(jnp.int32, (NX, LANE), 1) == 0
    lower = lax.broadcasted_iota(jnp.int32, (NX, LANE), 0) % NU < 2
    row_of_tile = lax.broadcasted_iota(jnp.int32, (DEV // 2, 2 * NU, LANE), 1) % NU

    def plane(z, carry):
        for j in range(NY // LANE):
            for q in range(4):
                at = pl.ds(j * (ROWS // 4) + z * NX + q * 128, 128)
                total = bins[0][at, :]
                for b in bins[1:]:
                    total = total + b[at, :]
                high = total.astype(BF16)
                dens_hi[q * 128 : (q + 1) * 128, j * LANE : (j + 1) * LANE] = high
                dens_lo[q * 128 : (q + 1) * 128, j * LANE : (j + 1) * LANE] = (total - high.astype(F32)).astype(BF16)
        along = dot(dens_hi[...], yh[...]) + dot(dens_lo[...], yh[...]) + dot(dens_hi[...], yl[...])
        near, far = along[: NX // 2], along[NX // 2 :]
        parts = []
        for h, folded in enumerate((near + far, near - far)):
            high = folded.astype(BF16)
            fold_hi[h] = high
            fold_lo[h] = (folded - high.astype(F32)).astype(BF16)
            tab_hi, tab_lo = along_x[2 * h], along_x[2 * h + 1]
            p, q = (
                dot(tab_hi[...], fold_hi[h, :, c]) + dot(tab_hi[...], fold_lo[h, :, c]) + dot(tab_lo[...], fold_hi[h, :, c])
                for c in (slice(0, HALF), slice(HALF, NY))
            )
            q = turn(q)
            p0, p1, q0, q1 = p[:, :LANE], p[:, LANE:], q[:, :LANE], q[:, LANE:]
            minus0 = jnp.where(first, 0.0, p0) - q0
            minus1 = p1 - q1
            parts.append(
                (
                    p0 + jnp.where(first, 0.0, q0),
                    p1 + q1,
                    jnp.where(first, minus1, minus0),
                    jnp.where(first, minus0, minus1),
                )
            )
        near = [jnp.where(lower, even, odd) for even, odd in zip(*parts)]
        far = [jnp.where(lower, odd, even) for even, odd in zip(*parts)]
        for side, (groups, spare) in enumerate(((near, 3), (far, 1))):
            shape = (DEV // 2, 2 * NU, LANE)
            last = groups[3].reshape(shape)
            for j in range(3):
                moved = pltpu.roll(last, (spare - (j ^ 2 * side)) % 8, 1)
                out[z, side * (DEV // 2) : (side + 1) * (DEV // 2), :, j * LANE : (j + 1) * LANE] = jnp.where(
                    row_of_tile == spare, moved, groups[j].reshape(shape)
                ).astype(BF16)
        pltpu.make_async_copy(out.at[z], out_hbm.at[:, z], out_sem.at[z]).start()
        return carry

    lax.fori_loop(0, ZD, plane, 0)
    for z in range(ZD):
        pltpu.make_async_copy(out.at[z], out_hbm.at[:, z], out_sem.at[z]).wait()


def prepare_kernel(green_hbm, cells_hbm, piece, rows, cells, sem):
    copies = [
        pltpu.make_async_copy(cells_hbm, cells, sem.at[0]),
        pltpu.make_async_copy(green_hbm.at[NU - 1], piece, sem.at[1]),
    ]
    for copy in copies:
        copy.start()
    copies[0].wait()
    for t in range(TILES):
        row = lax.shift_right_logical(cells[:, t * LANE : (t + 1) * LANE], 7)
        rows[t] = (row & 3) * (ROWS // 4) + lax.shift_right_logical(row, 2)
    copies[1].wait()


def prepare(green, cells):
    hbm = pl.BlockSpec(memory_space=pltpu.HBM)
    vmem = pl.BlockSpec(memory_space=pltpu.VMEM)
    return pl.pallas_call(
        prepare_kernel,
        out_shape=(pltpu.VMEM(green.shape[1:], BF16), pltpu.VMEM((TILES, SPREAD, LANE), jnp.int32)),
        in_specs=[hbm, hbm],
        out_specs=(vmem, vmem),
        scratch_shapes=[pltpu.VMEM((SPREAD, SLOTS), jnp.int32), pltpu.SemaphoreType.DMA((2,))],
        compiler_params=pltpu.CompilerParams(vmem_limit_bytes=8 << 20),
        name="prepare",
    )(*in_hbm(green, cells))


def front(rows, charges, cells, splines, counts, tabs):
    smem = pl.BlockSpec(memory_space=pltpu.SMEM)
    hbm = pl.BlockSpec(memory_space=pltpu.HBM)
    return pl.pallas_call(
        front_kernel,
        out_shape=pltpu.HBM((DEV, ZD, 2 * NU, WIDE), BF16),
        in_specs=[pl.BlockSpec(memory_space=pltpu.VMEM)] + [hbm] * 3 + [smem] + [hbm] * 6,
        out_specs=hbm,
        scratch_shapes=[pltpu.VMEM((ROWS, LANE), F32)] * SPREAD
        + [pltpu.VMEM((LANE, LANE), F32)] * 2
        + [pltpu.VMEM((TILES, SPREAD, LANE), jnp.int32), pltpu.VMEM((TILES, SPREAD, LANE), F32)]
        + [pltpu.VMEM((NX, NY), BF16)] * 2
        + [pltpu.VMEM((2, NX // 2, NY), BF16)] * 2
        + [pltpu.VMEM(t.shape, BF16) for t in tabs]
        + [pltpu.VMEM((ZD, DEV, 2 * NU, WIDE), BF16)]
        + [pltpu.VMEM((SPREAD, SLOTS), jnp.int32), pltpu.VMEM((SPREAD, SLOTS), F32), pltpu.VMEM((1, SLOTS), F32)]
        + [pltpu.SemaphoreType.DMA((n,)) for n in (TILES, 6, ZD, 3)]
        + [pltpu.SMEM((SPREAD, LANE), jnp.int32)] * TILES,
        compiler_params=pltpu.CompilerParams(vmem_limit_bytes=44 << 20),
        name="front",
    )(rows, *in_hbm(cells, splines, charges.reshape(1, SLOTS)), counts, *in_hbm(*tabs))


WAVE = (0, 2, 1)
BLOCK = (0, 1, 3, 2)
MIRROR = (3, 2, 0, 1)
SWAP = (1, 3, 0, 2)
PART = NZ // 2


def green_kernel(
    spectrum, green_hbm, mirror_hbm, x_hbm, y_hbm, out, x_out, y_out, green, flat, sums, swapped, green_sem, *rhs
):
    sources = [green_hbm.at[w] for w in WAVE] + [mirror_hbm]
    fetches = [pltpu.make_async_copy(s, green.at[i], green_sem.at[i]) for i, s in enumerate(sources)]
    fetches.append(pltpu.make_async_copy(x_hbm, x_out, green_sem.at[4]))
    fetches.append(pltpu.make_async_copy(y_hbm, y_out, green_sem.at[5]))
    for fetch in fetches:
        fetch.start()
    far = lax.axis_index("zg")
    at = [jnp.bitwise_xor(row, 2 * far) for row in range(NU)]
    for j in range(3):
        flat[...] = spectrum[:, :, j * LANE : (j + 1) * LANE].astype(F32).reshape(NZ * 2 * NU, LANE)
        for row in range(NU):
            for c in range(2):
                values = flat[pl.ds(c * NU + at[row], NZ, stride=2 * NU), :].astype(BF16)
                to, group = (rhs[row], j) if row < 3 else (rhs[j], 3)
                to[group, :, c * LANE : (c + 1) * LANE] = values
    first = lax.broadcasted_iota(jnp.int32, (NZ, 2 * LANE), 1) % LANE == 0
    for j in range(KYB):
        swapped[j] = jnp.where(first, rhs[2][SWAP[j]], rhs[2][j])
    first = first[:PART]
    for part in range(2):
        planes = slice(part * PART, (part + 1) * PART)
        for row in range(3):
            if part == 0:
                fetches[row].wait()
            m = [dot(green[row, BLOCK[j], planes, :], rhs[row][j]) for j in range(KYB)]
            if row == 2:
                if part == 0:
                    fetches[3].wait()
                other = [dot(green[3, MIRROR[j], planes, :], swapped[j]) for j in range(KYB)]
                m = [m[j] + jnp.where(first, other[SWAP.index(j)], other[j]) for j in range(KYB)]
            s2 = jnp.where(first, m[3], m[2])
            s3 = jnp.where(first, m[2], m[3])
            t0 = m[0] + jnp.where(first, 0.0, s2)
            d0 = jnp.where(first, 0.0, m[0]) - s2
            t1 = m[1] + s3
            d1 = m[1] - s3
            groups = (
                (t0[:, :LANE], t0[:, LANE:]),
                (t1[:, :LANE], t1[:, LANE:]),
                (d0[:, LANE:], -d0[:, :LANE]),
                (d1[:, LANE:], -d1[:, :LANE]),
            )
            for j, group in enumerate(groups):
                for c in range(2):
                    to, slot = (j, row) if j < 3 else (row, 3)
                    sums[to, pl.ds(c * NU + at[slot], PART, stride=2 * NU), :] = group[c]
        for j in range(3):
            out[planes, :, j * LANE : (j + 1) * LANE] = sums[j].astype(BF16).reshape(PART, 2 * NU, LANE)
    for fetch in fetches[4:]:
        fetch.wait()


def mix(pencil, green, mirror, *tabs):
    vmem = pl.BlockSpec(memory_space=pltpu.VMEM)
    hbm = pl.BlockSpec(memory_space=pltpu.HBM)
    return pl.pallas_call(
        green_kernel,
        out_shape=(pltpu.VMEM((NZ, 2 * NU, WIDE), BF16), *(pltpu.VMEM(t.shape, BF16) for t in tabs)),
        in_specs=[vmem, hbm, hbm, hbm, hbm],
        out_specs=(vmem, vmem, vmem),
        compiler_params=pltpu.CompilerParams(vmem_limit_bytes=36 << 20),
        scratch_shapes=[
            pltpu.VMEM((NU, KYB, NZ, NZ), BF16),
            pltpu.VMEM((NZ * 2 * NU, LANE), F32),
            pltpu.VMEM((3, PART * 2 * NU, LANE), F32),
            pltpu.VMEM((KYB, NZ, 2 * LANE), BF16),
            pltpu.SemaphoreType.DMA((6,)),
        ]
        + [pltpu.VMEM((KYB, NZ, 2 * LANE), BF16)] * 3,
        name="mix",
    )(pencil.reshape(NZ, 2 * NU, WIDE), *in_hbm(green, mirror, *tabs))


def back_kernel(mixed, half_x, along_y, out_hbm, far_x, out, rest, out_sem):
    row_of_tile = lax.broadcasted_iota(jnp.int32, (DEV // 2, 2 * NU, LANE), 1) % NU
    sends = []
    for z in range(ZD):
        for side in range(2):
            devices = slice(side * (DEV // 2), (side + 1) * (DEV // 2))
            spare = 3 - 2 * side
            last = None
            for j in range(3):
                group = mixed[devices, z, :, j * LANE : (j + 1) * LANE].astype(F32)
                moved = pltpu.roll(group, ((j ^ 2 * side) - spare) % 8, 1)
                last = moved if last is None else jnp.where(row_of_tile == (j ^ 2 * side), moved, last)
            rest[devices, :, LANE:] = last.astype(BF16)
        rest[:, :, :LANE] = mixed[:, z, :, 2 * LANE :]
        for h in range(2):
            rows = pl.ds(h * HALF, HALF)
            if z == 0 and h == 1:
                place = lax.broadcasted_iota(jnp.int32, (1, 2 * NX), 1)
                sign = jnp.where(place % NU == jnp.where(place < NX, 2, 0), -1.0, 1.0).astype(BF16)
                far_x[...] = half_x[...] * sign
            along_x = (half_x, far_x)[h]
            front = dot(along_x[...], mixed[:, z, :, : 2 * LANE].reshape(2 * NX, 2 * LANE)).astype(BF16)
            tail = dot(along_x[...], rest[...].reshape(2 * NX, 2 * LANE)).astype(BF16)
            out[z, rows, :] = dot_nt(front, along_y[:, : 2 * LANE]) + dot_nt(tail, along_y[:, 2 * LANE :])
            send = pltpu.make_async_copy(out.at[z, rows], out_hbm.at[z, rows], out_sem.at[2 * z + h])
            send.start()
            sends.append(send)
    for send in sends:
        send.wait()


def back(returned, inverse_x, inverse_y):
    vmem = pl.BlockSpec(memory_space=pltpu.VMEM)
    hbm = pl.BlockSpec(memory_space=pltpu.HBM)
    return pl.pallas_call(
        back_kernel,
        out_shape=jax.ShapeDtypeStruct((ZD, NX, NY), F32),
        in_specs=[vmem, vmem, vmem],
        out_specs=hbm,
        compiler_params=pltpu.CompilerParams(vmem_limit_bytes=24 << 20),
        scratch_shapes=[
            pltpu.VMEM((NX // 2, 2 * NX), BF16),
            pltpu.VMEM((ZD, NX, NY), F32),
            pltpu.VMEM((DEV, 2 * NU, 2 * LANE), BF16),
            pltpu.SemaphoreType.DMA((2 * ZD,)),
        ],
        name="back",
    )(returned, inverse_x, inverse_y)


def steps(charges, cells, splines, counts, green):
    forward = tuple(jnp.asarray(t) for t in forward_tables())
    piece, rows = prepare(green, cells)
    mirror = lax.ppermute(piece, AXES, [(d, DEV - 1 - d) for d in range(DEV)])
    spectrum = front(rows, charges, cells, splines, counts, forward)
    pencil = lax.all_to_all(spectrum, AXES, split_axis=0, concat_axis=0, tiled=True)
    mixed, *along = mix(pencil, green, mirror, jnp.asarray(inverse_table()), forward[0])
    mixed = mixed.reshape(DEV, ZD, 2 * NU, WIDE)
    returned = lax.all_to_all(mixed, AXES, split_axis=0, concat_axis=0, tiled=True)
    return back(returned, *along)


def solution(mesh):
    in_specs = (
        P(AXES),
        P(None, AXES),
        P(None, AXES),
        P(AXES),
        P(AXES, None, None, None),
    )
    return jax.shard_map(steps, mesh=mesh, in_specs=in_specs, out_specs=P(AXES, None, None), check_vma=False)
```

```python
import jax
import jax.numpy as jnp
import numpy as np
from jax import lax
from jax.experimental import pallas as pl
from jax.experimental.pallas import tpu as pltpu
from jax.sharding import PartitionSpec as P

NX = 512
NY = 512
NZ = 384
KYB = 4
AXES = ("zg", "xy")
DEV = 128
ZD = 3
NU = NX // DEV
HALF = NY // 2
LANE = 128
WIDE = 3 * LANE
SLOTS = 2048
SPREAD = 8
TILES = SLOTS // LANE
ROWS = ZD * NX * NY // LANE
F32 = jnp.float32
BF16 = jnp.bfloat16


def split(table):
    high = table.astype(BF16)
    return high, (table - high.astype(np.float64)).astype(BF16)


def angles(left, right):
    return (np.outer(left, right) % NX) * (2.0 * np.pi / NX)


def waves():
    device = np.arange(DEV)[:, None]
    offset = np.array([[0, 2, 1, -1], [1, -1, 0, 2]])[device[:, 0] // (DEV // 2)]
    return np.where(offset < 0, -1, device * NU + offset)


def forward_tables():
    y = np.arange(NY)
    v = np.arange(HALF)
    along_y = np.concatenate([np.cos(angles(y, v)), -np.sin(angles(y, v))], axis=1)
    along_y[:, HALF] = np.where(y % 2 == 0, 1.0, -1.0)
    x = np.arange(NX // 2)
    near, far = waves()[: DEV // 2], waves()[DEV // 2 :]
    out = [*split(along_y / 512.0)]
    for wave in (np.concatenate([near[:, :2], far[:, 2:]], axis=1), np.concatenate([far[:, :2], near[:, 2:]], axis=1)):
        a = angles(wave.reshape(-1), x).reshape(DEV // 2, NU, NX // 2)
        used = (wave >= 0)[:, :, None]
        out += split(np.stack([np.cos(a) * used, -np.sin(a) * used], axis=1).reshape(NX, NX // 2))
    return tuple(out)


def inverse_table():
    wave = waves()[:, None, :]
    a = angles(np.arange(NX // 2), wave.reshape(-1)).reshape(NX // 2, DEV, 1, NU)
    table = np.concatenate([np.cos(a), -np.sin(a)], axis=2) * (wave >= 0)
    return table.reshape(NX // 2, 2 * NX).astype(BF16)


def in_hbm(*arrays):
    return tuple(pltpu.with_memory_space_constraint(a, pltpu.HBM) for a in arrays)


def dot(a, b):
    return jnp.dot(a, b, preferred_element_type=F32)


def dot_nt(a, b):
    return lax.dot_general(a, b, (((1,), (1,)), ((), ())), preferred_element_type=F32)


def turn(q):
    whole = q.reshape(-1, 2 * NU, q.shape[1])
    real = lax.broadcasted_iota(jnp.int32, whole.shape, 1) < NU
    swapped = pltpu.roll(whole, NU, 1)
    return jnp.where(real, -swapped, swapped).reshape(q.shape)


def front_kernel(
    row_table, cells_hbm, splines_hbm, charges_hbm, counts, yh_hbm, yl_hbm, eh_hbm, el_hbm, oh_hbm, ol_hbm, out_hbm, *scratch
):
    bins = scratch[:SPREAD]
    spikes = scratch[8:10]
    lanes, values, dens_hi, dens_lo, fold_hi, fold_lo = scratch[10:16]
    tabs = scratch[16:22]
    out, cells, splines, charges, row_sem, tab_sem, out_sem, slot_sem = scratch[22:30]
    row_of = scratch[30:]
    slot_copies = [
        pltpu.make_async_copy(s, d, slot_sem.at[i])
        for i, (s, d) in enumerate(((cells_hbm, cells), (splines_hbm, splines), (charges_hbm, charges)))
    ]
    for copy in slot_copies:
        copy.start()
    row_copies = [pltpu.make_async_copy(row_table.at[t], row_of[t], row_sem.at[t]) for t in range(TILES)]
    for copy in row_copies:
        copy.start()
    sources = (yh_hbm, yl_hbm, eh_hbm, el_hbm, oh_hbm, ol_hbm)
    tab_copies = [pltpu.make_async_copy(s, d, tab_sem.at[i]) for i, (s, d) in enumerate(zip(sources, tabs))]
    for copy in tab_copies:
        copy.start()
    zeros = jnp.zeros((256, LANE), F32)

    def clear(i, carry):
        for b in bins:
            b[pl.ds(i * 256, 256), :] = zeros
        return carry

    lax.fori_loop(0, ROWS // 256, clear, 0)
    for copy in slot_copies:
        copy.wait()
    slot = lax.broadcasted_iota(jnp.int32, (1, SLOTS), 1)
    live = (slot < counts[0]).astype(F32)
    value = splines[...] * (charges[...] * live)
    lane_of = cells[...] & (LANE - 1)
    for t in range(TILES):
        lanes[t] = lane_of[:, t * LANE : (t + 1) * LANE]
        values[t] = value[:, t * LANE : (t + 1) * LANE]
    lane = lax.broadcasted_iota(jnp.int32, (SPREAD, LANE), 1)

    def build(spike, g):
        pick = jnp.full((SPREAD, LANE), g, jnp.int32)
        for t in range(TILES):
            at = jnp.take_along_axis(lanes[t], pick, axis=1)
            amount = jnp.take_along_axis(values[t], pick, axis=1)
            spike[t * SPREAD : (t + 1) * SPREAD, :] = jnp.where(lane == at, amount, 0.0)

    def apply(spike, g):
        for t in range(TILES):
            rows = [row_of[t][k, g] for k in range(SPREAD)]
            sums = [bins[k][pl.ds(rows[k], 1), :] + spike[pl.ds(t * SPREAD + k, 1), :] for k in range(SPREAD)]
            for k in range(SPREAD):
                bins[k][pl.ds(rows[k], 1), :] = sums[k]

    build(spikes[0], 0)
    for copy in row_copies:
        copy.wait()

    def body(h, carry):
        build(spikes[1], 2 * h + 1)
        apply(spikes[0], 2 * h)
        build(spikes[0], jnp.minimum(2 * h + 2, LANE - 1))
        apply(spikes[1], 2 * h + 1)
        return carry

    lax.fori_loop(0, LANE // 2, body, 0)
    for copy in tab_copies:
        copy.wait()
    yh, yl, *along_x = tabs
    first = lax.broadcasted_iota(jnp.int32, (NX, LANE), 1) == 0
    lower = lax.broadcasted_iota(jnp.int32, (NX, LANE), 0) % NU < 2
    row_of_tile = lax.broadcasted_iota(jnp.int32, (DEV // 2, 2 * NU, LANE), 1) % NU

    def send(z, side):
        devices = pl.ds(side * (DEV // 2), DEV // 2)
        return pltpu.make_async_copy(out.at[z, devices], out_hbm.at[devices, z], out_sem.at[2 * z + side])

    def plane(z, carry):
        for j in range(NY // LANE):
            for q in range(4):
                at = pl.ds(j * (ROWS // 4) + z * NX + q * 128, 128)
                total = bins[0][at, :]
                for b in bins[1:]:
                    total = total + b[at, :]
                high = total.astype(BF16)
                dens_hi[q * 128 : (q + 1) * 128, j * LANE : (j + 1) * LANE] = high
                dens_lo[q * 128 : (q + 1) * 128, j * LANE : (j + 1) * LANE] = (total - high.astype(F32)).astype(BF16)
        along = dot(dens_hi[...], yh[...]) + dot(dens_lo[...], yh[...]) + dot(dens_hi[...], yl[...])
        near, far = along[: NX // 2], along[NX // 2 :]
        parts = []
        for h, folded in enumerate((near + far, near - far)):
            high = folded.astype(BF16)
            fold_hi[h] = high
            fold_lo[h] = (folded - high.astype(F32)).astype(BF16)
            tab_hi, tab_lo = along_x[2 * h], along_x[2 * h + 1]
            p, q = (
                dot(tab_hi[...], fold_hi[h, :, c]) + dot(tab_hi[...], fold_lo[h, :, c]) + dot(tab_lo[...], fold_hi[h, :, c])
                for c in (slice(0, HALF), slice(HALF, NY))
            )
            q = turn(q)
            p0, p1, q0, q1 = p[:, :LANE], p[:, LANE:], q[:, :LANE], q[:, LANE:]
            minus0 = jnp.where(first, 0.0, p0) - q0
            minus1 = p1 - q1
            parts.append(
                (
                    p0 + jnp.where(first, 0.0, q0),
                    p1 + q1,
                    jnp.where(first, minus1, minus0),
                    jnp.where(first, minus0, minus1),
                )
            )
        near = [jnp.where(lower, even, odd) for even, odd in zip(*parts)]
        far = [jnp.where(lower, odd, even) for even, odd in zip(*parts)]
        for side, (groups, spare) in enumerate(((near, 3), (far, 1))):
            shape = (DEV // 2, 2 * NU, LANE)
            last = groups[3].reshape(shape)
            for j in range(3):
                moved = pltpu.roll(last, (spare - (j ^ 2 * side)) % 8, 1)
                out[z, side * (DEV // 2) : (side + 1) * (DEV // 2), :, j * LANE : (j + 1) * LANE] = jnp.where(
                    row_of_tile == spare, moved, groups[j].reshape(shape)
                ).astype(BF16)
            send(z, side).start()
        return carry

    lax.fori_loop(0, ZD, plane, 0)
    for z in range(ZD):
        for side in range(2):
            send(z, side).wait()


def prepare_kernel(green_hbm, cells_hbm, piece, rows, cells, sem):
    copies = [
        pltpu.make_async_copy(cells_hbm, cells, sem.at[0]),
        pltpu.make_async_copy(green_hbm.at[NU - 1], piece, sem.at[1]),
    ]
    for copy in copies:
        copy.start()
    copies[0].wait()
    for t in range(TILES):
        row = lax.shift_right_logical(cells[:, t * LANE : (t + 1) * LANE], 7)
        rows[t] = (row & 3) * (ROWS // 4) + lax.shift_right_logical(row, 2)
    copies[1].wait()


def prepare(green, cells):
    hbm = pl.BlockSpec(memory_space=pltpu.HBM)
    vmem = pl.BlockSpec(memory_space=pltpu.VMEM)
    return pl.pallas_call(
        prepare_kernel,
        out_shape=(pltpu.VMEM(green.shape[1:], BF16), pltpu.VMEM((TILES, SPREAD, LANE), jnp.int32)),
        in_specs=[hbm, hbm],
        out_specs=(vmem, vmem),
        scratch_shapes=[pltpu.VMEM((SPREAD, SLOTS), jnp.int32), pltpu.SemaphoreType.DMA((2,))],
        compiler_params=pltpu.CompilerParams(vmem_limit_bytes=8 << 20),
        name="prepare",
    )(*in_hbm(green, cells))


def front(rows, charges, cells, splines, counts, tabs):
    smem = pl.BlockSpec(memory_space=pltpu.SMEM)
    hbm = pl.BlockSpec(memory_space=pltpu.HBM)
    return pl.pallas_call(
        front_kernel,
        out_shape=pltpu.HBM((DEV, ZD, 2 * NU, WIDE), BF16),
        in_specs=[pl.BlockSpec(memory_space=pltpu.VMEM)] + [hbm] * 3 + [smem] + [hbm] * 6,
        out_specs=hbm,
        scratch_shapes=[pltpu.VMEM((ROWS, LANE), F32)] * SPREAD
        + [pltpu.VMEM((LANE, LANE), F32)] * 2
        + [pltpu.VMEM((TILES, SPREAD, LANE), jnp.int32), pltpu.VMEM((TILES, SPREAD, LANE), F32)]
        + [pltpu.VMEM((NX, NY), BF16)] * 2
        + [pltpu.VMEM((2, NX // 2, NY), BF16)] * 2
        + [pltpu.VMEM(t.shape, BF16) for t in tabs]
        + [pltpu.VMEM((ZD, DEV, 2 * NU, WIDE), BF16)]
        + [pltpu.VMEM((SPREAD, SLOTS), jnp.int32), pltpu.VMEM((SPREAD, SLOTS), F32), pltpu.VMEM((1, SLOTS), F32)]
        + [pltpu.SemaphoreType.DMA((n,)) for n in (TILES, 6, 2 * ZD, 3)]
        + [pltpu.SMEM((SPREAD, LANE), jnp.int32)] * TILES,
        compiler_params=pltpu.CompilerParams(vmem_limit_bytes=44 << 20),
        name="front",
    )(rows, *in_hbm(cells, splines, charges.reshape(1, SLOTS)), counts, *in_hbm(*tabs))


WAVE = (0, 2, 1)
BLOCK = (0, 1, 3, 2)
MIRROR = (3, 2, 0, 1)
SWAP = (1, 3, 0, 2)
PART = NZ // 2


def green_kernel(
    spectrum, green_hbm, mirror_hbm, x_hbm, y_hbm, out, x_out, y_out, green, flat, sums, swapped, green_sem, *rhs
):
    sources = [green_hbm.at[w] for w in WAVE] + [mirror_hbm]
    fetches = [pltpu.make_async_copy(s, green.at[i], green_sem.at[i]) for i, s in enumerate(sources)]
    fetches.append(pltpu.make_async_copy(x_hbm, x_out, green_sem.at[4]))
    fetches.append(pltpu.make_async_copy(y_hbm, y_out, green_sem.at[5]))
    for fetch in fetches:
        fetch.start()
    far = lax.axis_index("zg")
    at = [jnp.bitwise_xor(row, 2 * far) for row in range(NU)]
    for j in range(3):
        flat[...] = spectrum[:, :, j * LANE : (j + 1) * LANE].astype(F32).reshape(NZ * 2 * NU, LANE)
        for row in range(NU):
            for c in range(2):
                values = flat[pl.ds(c * NU + at[row], NZ, stride=2 * NU), :].astype(BF16)
                to, group = (rhs[row], j) if row < 3 else (rhs[j], 3)
                to[group, :, c * LANE : (c + 1) * LANE] = values
    first = lax.broadcasted_iota(jnp.int32, (NZ, 2 * LANE), 1) % LANE == 0
    for j in range(KYB):
        swapped[j] = jnp.where(first, rhs[2][SWAP[j]], rhs[2][j])
    first = first[:PART]
    for part in range(2):
        planes = slice(part * PART, (part + 1) * PART)
        for row in range(3):
            if part == 0:
                fetches[row].wait()
            m = [dot(green[row, BLOCK[j], planes, :], rhs[row][j]) for j in range(KYB)]
            if row == 2:
                if part == 0:
                    fetches[3].wait()
                other = [dot(green[3, MIRROR[j], planes, :], swapped[j]) for j in range(KYB)]
                m = [m[j] + jnp.where(first, other[SWAP.index(j)], other[j]) for j in range(KYB)]
            s2 = jnp.where(first, m[3], m[2])
            s3 = jnp.where(first, m[2], m[3])
            t0 = m[0] + jnp.where(first, 0.0, s2)
            d0 = jnp.where(first, 0.0, m[0]) - s2
            t1 = m[1] + s3
            d1 = m[1] - s3
            groups = (
                (t0[:, :LANE], t0[:, LANE:]),
                (t1[:, :LANE], t1[:, LANE:]),
                (d0[:, LANE:], -d0[:, :LANE]),
                (d1[:, LANE:], -d1[:, :LANE]),
            )
            for j, group in enumerate(groups):
                for c in range(2):
                    to, slot = (j, row) if j < 3 else (row, 3)
                    sums[to, pl.ds(c * NU + at[slot], PART, stride=2 * NU), :] = group[c]
        for j in range(3):
            out[planes, :, j * LANE : (j + 1) * LANE] = sums[j].astype(BF16).reshape(PART, 2 * NU, LANE)
    for fetch in fetches[4:]:
        fetch.wait()


def mix(pencil, green, mirror, *tabs):
    vmem = pl.BlockSpec(memory_space=pltpu.VMEM)
    hbm = pl.BlockSpec(memory_space=pltpu.HBM)
    return pl.pallas_call(
        green_kernel,
        out_shape=(pltpu.VMEM((NZ, 2 * NU, WIDE), BF16), *(pltpu.VMEM(t.shape, BF16) for t in tabs)),
        in_specs=[vmem, hbm, hbm, hbm, hbm],
        out_specs=(vmem, vmem, vmem),
        compiler_params=pltpu.CompilerParams(vmem_limit_bytes=36 << 20),
        scratch_shapes=[
            pltpu.VMEM((NU, KYB, NZ, NZ), BF16),
            pltpu.VMEM((NZ * 2 * NU, LANE), F32),
            pltpu.VMEM((3, PART * 2 * NU, LANE), F32),
            pltpu.VMEM((KYB, NZ, 2 * LANE), BF16),
            pltpu.SemaphoreType.DMA((6,)),
        ]
        + [pltpu.VMEM((KYB, NZ, 2 * LANE), BF16)] * 3,
        name="mix",
    )(pencil.reshape(NZ, 2 * NU, WIDE), *in_hbm(green, mirror, *tabs))


def back_kernel(mixed, half_x, along_y, out_hbm, far_x, out, rest, out_sem):
    row_of_tile = lax.broadcasted_iota(jnp.int32, (DEV // 2, 2 * NU, LANE), 1) % NU
    sends = []
    for z in range(ZD):
        for side in range(2):
            devices = slice(side * (DEV // 2), (side + 1) * (DEV // 2))
            spare = 3 - 2 * side
            last = None
            for j in range(3):
                group = mixed[devices, z, :, j * LANE : (j + 1) * LANE].astype(F32)
                moved = pltpu.roll(group, ((j ^ 2 * side) - spare) % 8, 1)
                last = moved if last is None else jnp.where(row_of_tile == (j ^ 2 * side), moved, last)
            rest[devices, :, LANE:] = last.astype(BF16)
        rest[:, :, :LANE] = mixed[:, z, :, 2 * LANE :]
        for h in range(2):
            rows = pl.ds(h * HALF, HALF)
            if z == 0 and h == 1:
                place = lax.broadcasted_iota(jnp.int32, (1, 2 * NX), 1)
                sign = jnp.where(place % NU == jnp.where(place < NX, 2, 0), -1.0, 1.0).astype(BF16)
                far_x[...] = half_x[...] * sign
            along_x = (half_x, far_x)[h]
            front = dot(along_x[...], mixed[:, z, :, : 2 * LANE].reshape(2 * NX, 2 * LANE)).astype(BF16)
            tail = dot(along_x[...], rest[...].reshape(2 * NX, 2 * LANE)).astype(BF16)
            out[z, rows, :] = dot_nt(front, along_y[:, : 2 * LANE]) + dot_nt(tail, along_y[:, 2 * LANE :])
            send = pltpu.make_async_copy(out.at[z, rows], out_hbm.at[z, rows], out_sem.at[2 * z + h])
            send.start()
            sends.append(send)
    for send in sends:
        send.wait()


def back(returned, inverse_x, inverse_y):
    vmem = pl.BlockSpec(memory_space=pltpu.VMEM)
    hbm = pl.BlockSpec(memory_space=pltpu.HBM)
    return pl.pallas_call(
        back_kernel,
        out_shape=jax.ShapeDtypeStruct((ZD, NX, NY), F32),
        in_specs=[vmem, vmem, vmem],
        out_specs=hbm,
        compiler_params=pltpu.CompilerParams(vmem_limit_bytes=24 << 20),
        scratch_shapes=[
            pltpu.VMEM((NX // 2, 2 * NX), BF16),
            pltpu.VMEM((ZD, NX, NY), F32),
            pltpu.VMEM((DEV, 2 * NU, 2 * LANE), BF16),
            pltpu.SemaphoreType.DMA((2 * ZD,)),
        ],
        name="back",
    )(returned, inverse_x, inverse_y)


def steps(charges, cells, splines, counts, green):
    forward = tuple(jnp.asarray(t) for t in forward_tables())
    piece, rows = prepare(green, cells)
    mirror = lax.ppermute(piece, AXES, [(d, DEV - 1 - d) for d in range(DEV)])
    spectrum = front(rows, charges, cells, splines, counts, forward)
    pencil = lax.all_to_all(spectrum, AXES, split_axis=0, concat_axis=0, tiled=True)
    mixed, *along = mix(pencil, green, mirror, jnp.asarray(inverse_table()), forward[0])
    mixed = mixed.reshape(DEV, ZD, 2 * NU, WIDE)
    returned = lax.all_to_all(mixed, AXES, split_axis=0, concat_axis=0, tiled=True)
    return back(returned, *along)


def solution(mesh):
    in_specs = (
        P(AXES),
        P(None, AXES),
        P(None, AXES),
        P(AXES),
        P(AXES, None, None, None),
    )
    return jax.shard_map(steps, mesh=mesh, in_specs=in_specs, out_specs=P(AXES, None, None), check_vma=False)
```
